32 devices in a mesh: slab: 8 (over z, y), sub: 4 (over x, core).
Axes of the slice: x: 2, y: 2, z: 4, core: 2. Of those that a mesh axis runs over, the one named last changes fastest.
Arguments:
- populations: float32 [19, 8, 128, 128], P(None, 'slab', 'sub'), may hold values from 0.5 to 1.5
- marker_cell: int32 [8, 4, 256, 128], P('slab', 'sub'), may hold values from 0 to 4095
- marker_count: int32 [8, 4, 256], P('slab', 'sub'), may hold values from 1 to 128
- particle_count: int32 [8, 4], P('slab', 'sub'), may hold values from 32 to 256, as said below
- particle_id: int32 [8, 4, 256], P('slab', 'sub'), may hold values from 0 to 2047, as said below
- owner_table: int32 [4, 8], P('sub'), may hold values from 0 to 7, as said below
- particle_velocity: float32 [8, 4, 3, 256], P('slab', 'sub'), may hold values from -0.3 to 0.3
- pair_list: int32 [8, 4, 256, 4], P('slab', 'sub'), may hold values from 0 to 255, as said below
- pair_gap: float32 [8, 4, 256, 4], P('slab', 'sub'), may hold values from 0.25 to 4
- self_coupling: bfloat16 [128, 128], replicated, may hold values from -2 to 16
- pair_coupling: bfloat16 [128, 128], replicated, may hold values from -1 to 6
Outputs:
- read: float32 [19, 8, 128, 128], P(None, 'slab', 'sub')
- marker_force: bfloat16 [8, 4, 256, 3, 128], P('slab', 'sub')
The draws below stay inside these ranges and needn't reach their ends.
Inputs may be any that keep to these rules, and one draw needn't show every extreme that they name: `particle_count`: A holder's live particles fill its first slots; in every sub index some holder has 256 live particles. `particle_id`: live slots of one sub index hold distinct ids; a live slot's particle is owned by slab index owner_table[j, id // 256] of the same sub index j. At most 32 live particles of one holder belong to one owner, and in every draw some holder sends exactly 32 to every owner. Dead slots hold arbitrary ids. `owner_table`: each row is a permutation of the slab indices. `pair_list`: A spot never names itself.
All inputs are finite; a program needn't handle non-finite values.
Results may differ from the reference program's by a relative error of at most 0.0053.
Values may be sent and summed in bfloat16 or wider, within the bound.
No kernel may reach another device: no remote copies, remote signals or barrier semaphores. Data moves between devices by JAX's collectives and lax.ppermute only.
A program may use at most 64 MiB of HBM per device.

```python
import math
from functools import partial
import jax
import jax.numpy as jnp
from jax import lax

CX = 1
CY = 32
CZ = 128
PCAP = 256
MK = 128
NPAIR = 4
NX = 8
NY = 128
NZ = 128
N_SLAB = 8
N_SUB = 4


def ordering(key, array_shape):
    length = array_shape[-1]
    scores = jax.random.randint(key, array_shape, 0, 1 << 20) * length + jnp.arange(length, dtype=jnp.int32)
    return jnp.argsort(scores, axis=-1).astype(jnp.int32)


def routing(key):
    base_key = jax.random.fold_in(key, 7)
    key_list = jax.random.split(base_key, 6)
    levels = jax.random.randint(key_list[0], (N_SLAB, N_SUB), 0, 4)
    counts = PCAP // jnp.left_shift(jnp.int32(1), levels.astype(jnp.int32))
    busiest = jax.random.randint(key_list[1], (N_SUB,), 0, N_SLAB)
    counts = jnp.where(jnp.arange(N_SLAB)[:, None] == busiest[None, :], PCAP, counts).astype(jnp.int32)
    table = ordering(key_list[2], (N_SUB, N_SLAB))
    inverse = jnp.argsort(table, axis=1).astype(jnp.int32)
    destinations = ordering(key_list[3], (N_SLAB, N_SUB, N_SLAB))
    spots = ordering(key_list[4], (N_SLAB, N_SUB, PCAP))
    slot_index = jnp.arange(PCAP, dtype=jnp.int32)
    capacity = PCAP // N_SLAB
    owner_slab = destinations[:, :, slot_index % N_SLAB]
    turn_index = (slot_index // N_SLAB)[None, None, :]
    source_index = jnp.arange(N_SLAB, dtype=jnp.int32)[:, None, None]
    column_index = jnp.arange(N_SUB, dtype=jnp.int32)[None, :, None]
    owner_spot = spots[owner_slab, column_index, source_index * capacity + turn_index]
    block_index = inverse[column_index, owner_slab]
    identities = block_index * PCAP + owner_spot
    filler = jax.random.randint(key_list[5], (N_SLAB, N_SUB, PCAP), 0, N_SLAB * PCAP)
    identities = jnp.where(slot_index[None, None, :] < counts[:, :, None], identities, filler)
    return (counts, table, identities.astype(jnp.int32))


def draw_particle_count(key, part):
    return routing(key)[0]


def draw_owner_table(key, part):
    return routing(key)[1]


def draw_particle_id(key, part):
    return routing(key)[2]


def draw_pair_list(key, part):
    pair_key = jax.random.fold_in(key, 11)
    offsets = jax.random.randint(pair_key, (N_SLAB, N_SUB, PCAP, NPAIR), 0, PCAP - 1)
    spot_index = jnp.arange(PCAP, dtype=jnp.int32)[None, None, :, None]
    return ((spot_index + 1 + offsets) % PCAP).astype(jnp.int32)


def coupling_matrix(key, low_diag, high_diag, spread_scale, spread_bound):
    diag_key, spread_key = jax.random.split(key)
    diagonal = jax.random.uniform(diag_key, (MK,), jnp.float32, low_diag, high_diag)
    spread = jnp.clip(spread_scale * jax.random.normal(spread_key, (MK, MK), jnp.float32), -spread_bound, spread_bound)
    identity = jnp.eye(MK, dtype=jnp.float32)
    return (spread * (1.0 - identity) + jnp.diag(diagonal)).astype(jnp.bfloat16)


def draw_self_coupling(key, part):
    return coupling_matrix(jax.random.fold_in(key, 13), 8.0, 16.0, 0.5, 2.0)


def draw_pair_coupling(key, part):
    return coupling_matrix(jax.random.fold_in(key, 17), 2.0, 6.0, 0.25, 1.0)


def place_ends(values, key, smallest, high):
    longest = values.shape.index(max(values.shape))
    spots = []
    for shift in (0, 1):
        where = [jax.random.randint(jax.random.fold_in(key, axis), (), 0, length) for axis, length in enumerate(values.shape)]
        where[longest] = (where[longest] + shift) % values.shape[longest]
        spots.append(tuple(where))
    return values.at[spots[0]].set(smallest).at[spots[1]].set(high)


def steps_of(stream_key, extent, cuts, low, largest):
    def one(axis_at, shards_of):
        draws = jax.random.uniform(jax.random.fold_in(jax.random.fold_in(stream_key, 6), axis_at), (shards_of,), jnp.float32, low / len(cuts), largest / len(cuts))
        return jnp.repeat(jnp.exp(draws), extent[axis_at] // shards_of).reshape((-1,) + (1,) * (len(extent) - axis_at - 1))

    gain = one(*cuts[0])
    for cut in cuts[1:]:
        gain = gain * one(*cut)
    return gain


def scatter_about(own_key, extent, width, reach, pieces=(), kind=jnp.bfloat16):
    values = width * jax.random.normal(own_key, extent, jnp.float32)
    if pieces:
        values = values * steps_of(own_key, extent, pieces, -0.22, 0.18)
    return jnp.clip(values, -reach, reach).astype(kind)


def setup_inputs(seed: int = 0) -> dict:
    splits = jax.random.split(jax.random.key(seed), 12)
    return {
        "populations": jnp.clip(0.5 + 1.0 * jax.random.uniform(splits[0], (19, NX, NY, NZ), jnp.float32) ** steps_of(splits[0], (19, NX, NY, NZ), ((1, 8), (2, 4)), -0.2, 0.2), 0.5, 1.5),
        "marker_cell": place_ends(jax.random.randint(splits[1], (N_SLAB, N_SUB, PCAP, MK), 0, CX * CY * CZ), jax.random.fold_in(splits[1], 1), 0, (CX * CY * CZ) - 1).astype(jnp.int32),
        "marker_count": place_ends(jax.random.randint(splits[2], (N_SLAB, N_SUB, PCAP), 1, MK + 1), jax.random.fold_in(splits[2], 1), 1, MK).astype(jnp.int32),
        "particle_count": draw_particle_count(jax.random.fold_in(splits[11], 71), 0),
        "particle_id": draw_particle_id(jax.random.fold_in(splits[11], 71), 0),
        "owner_table": draw_owner_table(jax.random.fold_in(splits[11], 71), 0),
        "particle_velocity": scatter_about(splits[6], (N_SLAB, N_SUB, 3, PCAP), 0.05, 0.3, ((0, 8), (1, 4)), jnp.float32),
        "pair_list": draw_pair_list(jax.random.fold_in(splits[11], 71), 0),
        "pair_gap": jnp.clip(jnp.exp(math.log(4.0) - 2.7725887 * jax.random.uniform(splits[8], (N_SLAB, N_SUB, PCAP, NPAIR), jnp.float32) ** steps_of(splits[8], (N_SLAB, N_SUB, PCAP, NPAIR), ((0, 8), (1, 4)), -0.2, 0.2)), 0.25, 4.0),
        "self_coupling": draw_self_coupling(jax.random.fold_in(splits[11], 71), 0),
        "pair_coupling": draw_pair_coupling(jax.random.fold_in(splits[11], 71), 0),
    }


lattice_dirs = [(0, 0, 0), (1, 0, 0), (-1, 0, 0), (0, 1, 0), (0, -1, 0), (0, 0, 1), (0, 0, -1),
                (1, 1, 0), (-1, -1, 0), (1, -1, 0), (-1, 1, 0), (1, 0, 1), (-1, 0, -1),
                (1, 0, -1), (-1, 0, 1), (0, 1, 1), (0, -1, -1), (0, 1, -1), (0, -1, 1)]
lattice_weights = [1.0 / 3.0] + [1.0 / 18.0] * 6 + [1.0 / 36.0] * 12
opposite_of = [0, 2, 1, 4, 3, 6, 5, 8, 7, 10, 9, 12, 11, 14, 13, 16, 15, 18, 17]
relax_rate = 1.25


def moments(populations):
    dirs_table = jnp.array(lattice_dirs, jnp.float32)
    density = jnp.sum(populations, axis=0)
    moment = jnp.einsum("ic,i...->c...", dirs_table, populations, precision=lax.Precision.HIGHEST)
    return density, moment


def collide(populations, density, moment, body_force):
    dirs_table = jnp.array(lattice_dirs, jnp.float32)
    weight_col = jnp.array(lattice_weights, jnp.float32).reshape((19,) + (1,) * (populations.ndim - 1))
    velocity = (moment + 0.5 * body_force) / density
    along = jnp.einsum("ic,c...->i...", dirs_table, velocity, precision=lax.Precision.HIGHEST)
    push = jnp.einsum("ic,c...->i...", dirs_table, body_force, precision=lax.Precision.HIGHEST)
    speed_sq = jnp.sum(velocity * velocity, axis=0)
    work_rate = jnp.sum(velocity * body_force, axis=0)
    equilibrium = weight_col * density * (1.0 + 3.0 * along + 4.5 * along * along - 1.5 * speed_sq)
    source = (1.0 - 0.5 * relax_rate) * weight_col * (3.0 * (push - work_rate) + 9.0 * along * push)
    return populations - relax_rate * (populations - equilibrium) + source


def collide_plane(operands):
    plane_pops, plane_force = operands
    density, moment = moments(plane_pops)
    return collide(plane_pops, density, moment, plane_force)


def lubricate(owned, partner_index, partner_gap, self_coupling, pair_coupling):
    marker_width = owned.shape[-1]
    partners = owned[partner_index]
    weighted = jnp.sum(partners.astype(jnp.float32) / partner_gap[:, :, None, None], axis=1).astype(jnp.bfloat16)
    direct = jnp.dot(owned.reshape(-1, marker_width), self_coupling, preferred_element_type=jnp.float32)
    coupled = jnp.dot(weighted.reshape(-1, marker_width), pair_coupling, preferred_element_type=jnp.float32)
    return (direct + coupled).astype(jnp.bfloat16).reshape(owned.shape)


def lubricate_slab(operands, self_coupling, pair_coupling):
    owned, partner_index, partner_gap = operands
    column_fn = partial(lubricate, self_coupling=self_coupling, pair_coupling=pair_coupling)
    return jax.vmap(column_fn)(owned, partner_index, partner_gap)


def stream_one(collided, number, width_y):
    step_x, step_y, step_z = lattice_dirs[number]
    moved = jnp.roll(collided[number], (step_x, step_z), axis=(0, 2))
    if step_y == 0:
        return moved
    padded = jnp.pad(moved, ((0, 0), (1, 1), (0, 0)))
    moved = padded[:, 1 - step_y: 1 - step_y + width_y, :]
    edge_row = 0 if step_y == 1 else width_y - 1
    at_wall = (jnp.arange(width_y) == edge_row)[None, :, None]
    return jnp.where(at_wall, collided[opposite_of[number]], moved)


def reference(populations, marker_cell, marker_count, particle_count, particle_id, owner_table,
              particle_velocity, pair_list, pair_gap, self_coupling, pair_coupling):
    width_y = CY * N_SUB
    density, moment = moments(populations)
    fluid_flow = (moment / density).reshape(3, -1)
    slab_index = jnp.arange(N_SLAB, dtype=jnp.int32)[:, None, None, None]
    sub_index = jnp.arange(N_SUB, dtype=jnp.int32)[None, :, None, None]
    cell_x = slab_index * CX + marker_cell // (CY * CZ)
    cell_y = sub_index * CY + (marker_cell // CZ) % CY
    cell_z = marker_cell % CZ
    flat_cell = ((cell_x * width_y + cell_y) * CZ + cell_z).reshape(-1).astype(jnp.int32)
    sampled = jnp.take(fluid_flow, flat_cell, axis=1).reshape(3, N_SLAB, N_SUB, PCAP, MK)
    sampled = jnp.transpose(sampled, (1, 2, 3, 0, 4))
    slot_index = jnp.arange(PCAP, dtype=jnp.int32)
    alive_slot = slot_index[None, None, :] < particle_count[:, :, None]
    marker_index = jnp.arange(MK, dtype=jnp.int32)[None, None, None, :]
    live_marker = alive_slot[..., None] & (marker_index < marker_count[..., None])
    target_speed = jnp.transpose(particle_velocity, (0, 1, 3, 2))[..., None]
    slip_value = jnp.where(live_marker[:, :, :, None, :], target_speed - sampled, 0.0).astype(jnp.bfloat16)
    column_index = sub_index[..., 0]
    owner_slab = owner_table[column_index, particle_id // PCAP]
    owner_spot = particle_id % PCAP
    total_slots = N_SLAB * N_SUB * PCAP
    target_row = jnp.where(alive_slot, (owner_slab * N_SUB + column_index) * PCAP + owner_spot, total_slots)
    target_row = target_row.reshape(-1).astype(jnp.int32)
    gathered = jnp.zeros((total_slots, 3, MK), jnp.bfloat16).at[target_row].set(
        slip_value.reshape(total_slots, 3, MK), mode="drop")
    gathered = gathered.reshape(N_SLAB, N_SUB, PCAP, 3, MK)
    slab_fn = partial(lubricate_slab, self_coupling=self_coupling, pair_coupling=pair_coupling)
    correction = lax.map(slab_fn, (gathered, pair_list, pair_gap)).reshape(total_slots, 3, MK)
    returned = correction[jnp.minimum(target_row, total_slots - 1)].reshape(N_SLAB, N_SUB, PCAP, 3, MK)
    marker_force = jnp.where(live_marker[:, :, :, None, :], returned, 0.0).astype(jnp.bfloat16)
    spread_terms = jnp.transpose(marker_force.astype(jnp.float32), (3, 0, 1, 2, 4)).reshape(3, -1)
    body_force = jnp.zeros((3, N_SLAB * CX * width_y * CZ), jnp.float32).at[:, flat_cell].add(spread_terms)
    body_force = body_force.reshape(3, N_SLAB * CX, width_y, CZ)
    collided = lax.map(collide_plane, (jnp.moveaxis(populations, 1, 0), jnp.moveaxis(body_force, 1, 0)))
    collided = jnp.moveaxis(collided, 0, 1)
    read = jnp.stack([stream_one(collided, number, width_y) for number in range(19)])
    return read, marker_force
```

```python
import functools

import jax
import jax.numpy as jnp
from jax import lax
from jax.experimental import pallas as pl
from jax.experimental.pallas import tpu as pltpu
from jax.sharding import PartitionSpec as P

lattice_dirs = [
    (0, 0, 0),
    (1, 0, 0),
    (-1, 0, 0),
    (0, 1, 0),
    (0, -1, 0),
    (0, 0, 1),
    (0, 0, -1),
    (1, 1, 0),
    (-1, -1, 0),
    (1, -1, 0),
    (-1, 1, 0),
    (1, 0, 1),
    (-1, 0, -1),
    (1, 0, -1),
    (-1, 0, 1),
    (0, 1, 1),
    (0, -1, -1),
    (0, 1, -1),
    (0, -1, 1),
]
lattice_weights = [1.0 / 3.0] + [1.0 / 18.0] * 6 + [1.0 / 36.0] * 12
opposite_of = [0, 2, 1, 4, 3, 6, 5, 8, 7, 10, 9, 12, 11, 14, 13, 16, 15, 18, 17]
relax_rate = 1.25
forward_x = [1, 7, 9, 11, 13]
backward_x = [2, 8, 10, 12, 14]
upward_y = [3, 15, 17, 7, 10]
downward_y = [4, 16, 18, 9, 8]
BF = jnp.bfloat16
F32 = jnp.float32


def iota(shape, dim, dtype=F32):
    value = lax.broadcasted_iota(jnp.int32, shape, dim)
    return value if dtype == jnp.int32 else value.astype(F32).astype(dtype)


def dot_nt(a, b):
    return lax.dot_general(a, b, (((1,), (1,)), ((), ())), preferred_element_type=F32)


def dot_nn(a, b):
    return jnp.dot(a, b, preferred_element_type=F32)


def moments_of(pops):
    density = pops[0]
    moment = [None, None, None]
    for number in range(19):
        if number:
            density = density + pops[number]
        for axis in range(3):
            step = lattice_dirs[number][axis]
            if step == 0:
                continue
            if moment[axis] is None:
                moment[axis] = pops[number] if step == 1 else -pops[number]
            elif step == 1:
                moment[axis] = moment[axis] + pops[number]
            else:
                moment[axis] = moment[axis] - pops[number]
    return density, moment


def one_hot_rows(row, count, kind=BF):
    tall = jnp.broadcast_to(row, (16, row.shape[1])).astype(kind)
    one, zero = jnp.ones((), kind), jnp.zeros((), kind)
    parts = []
    for start in range(0, count, 16):
        number = iota((16, row.shape[1]), 0, F32) + float(start)
        parts.append(jnp.where(number.astype(kind) == tall, one, zero))
    return jnp.concatenate(parts, axis=0)


def sample_kernel(
    slab_count,
    packed,
    count_ref,
    table_ref,
    pops_ref,
    cell_ref,
    marker_count_ref,
    id_ref,
    velocity_ref,
    slip_ref,
    *rest,
):
    if packed:
        cols_ref, z_ref, y_ref, sampled_ref = rest
    else:
        spot_ref, cols_ref, z_ref, y_ref, sampled_ref = rest
    slots, width = cell_ref.shape
    rows, depth = pops_ref.shape[1:]
    capacity = slots // slab_count

    density, moment = moments_of([pops_ref[number] for number in range(19)])
    flow = jnp.concatenate([part / density for part in moment], axis=0)
    high = flow.astype(BF)
    low = (flow - high.astype(F32)).astype(BF)
    flow_pair = jnp.concatenate([high, low], axis=1)

    cells = cell_ref[...]
    z_ref[...] = (cells % depth).astype(F32)
    y_ref[...] = (cells // depth).astype(F32)

    group = 8

    def sample_group(step, carry):
        base = pl.multiple_of(step * group, group)
        z_rows = z_ref[pl.ds(base, group), :]
        y_rows = y_ref[pl.ds(base, group), :]
        parts = [[], [], []]
        for first in range(0, group, 2):
            picks = jnp.concatenate(
                [one_hot_rows(z_rows[s : s + 1], depth) for s in (first, first + 1)], axis=1
            )
            picked = dot_nn(flow_pair, jnp.concatenate([picks, picks], axis=0))
            for s in (first, first + 1):
                off = (s - first) * width
                mask = iota((rows, width), 0) == y_rows[s : s + 1]
                for c in range(3):
                    block = picked[c * rows : (c + 1) * rows, off : off + width]
                    parts[c].append(
                        jnp.sum(jnp.where(mask, block, 0.0), axis=0, keepdims=True)
                    )
        for c in range(3):
            sampled_ref[c, pl.ds(base, group), :] = jnp.concatenate(parts[c], axis=0)
        return carry

    lax.fori_loop(0, slots // group, sample_group, 0)

    lane = iota((1, slots), 1, jnp.int32)
    alive = lane < count_ref[0]
    identity = id_ref[...]
    block = identity // slots
    spot = (identity % slots).astype(F32)

    def look_up(b, owner):
        return jnp.where(block == b, table_ref[b], owner)

    owner = lax.fori_loop(0, slab_count, look_up, jnp.zeros((1, slots), jnp.int32))
    owner = jnp.where(alive, owner, -1)
    owner_f = owner.astype(F32)
    chosen = jnp.where(iota((slab_count, slots), 0) == owner_f, 1.0, 0.0)
    before = jnp.where(
        iota((slots, slots), 0) < iota((slots, slots), 1), 1.0, 0.0
    ).astype(BF)
    earlier = dot_nn(chosen.astype(BF), before)
    position = jnp.sum(chosen * earlier, axis=0, keepdims=True)
    send_row = jnp.where(alive, owner_f * float(capacity) + position, -1.0)

    count = jnp.where(alive, marker_count_ref[...], 0).astype(F32)
    velocity = velocity_ref[...]
    stack = jnp.concatenate(
        [velocity, count, send_row, jnp.zeros((3, slots), F32)], axis=0
    )
    cols = jnp.transpose(stack)
    cols_ref[...] = cols
    live = iota((slots, width), 1) < cols[:, 3:4]
    slips = []
    for c in range(3):
        slips.append(jnp.where(live, cols[:, c : c + 1] - sampled_ref[c], 0.0).astype(BF))
    place = jnp.where(iota((slots, slots), 0) == send_row, 1.0, 0.0).astype(BF)
    sent = dot_nn(place, jnp.concatenate(slips, axis=1)).astype(BF)
    where_to = jnp.where(iota((width, slots), 0) == position, 1.0, 0.0).astype(BF)
    if packed:
        for c in range(3):
            slip_ref[:, c * capacity : (c + 1) * capacity, :] = sent[
                :, c * width : (c + 1) * width
            ].reshape(slab_count, capacity, width)
        taken = (iota((slab_count * 16, slots), 0, jnp.int32) // 16).astype(F32) == owner_f
        marks = dot_nt(jnp.where(taken, spot + 1.0, 0.0).astype(BF), where_to)
        slip_ref[:, 3 * capacity :, :] = marks.astype(BF).reshape(slab_count, 16, width)
    else:
        for c in range(3):
            slip_ref[c] = sent[:, c * width : (c + 1) * width]
        marks = dot_nt((chosen * (spot + 1.0)).astype(BF), where_to)
        spot_ref[...] = marks.astype(BF)


def owner_kernel(
    slab_count,
    packed,
    *refs,
):
    if packed:
        got_ref, list_ref, gap_ref, self_ref, pair_ref, out_ref = refs
        width = got_ref.shape[2]
        slots = list_ref.shape[0]
        capacity = slots // slab_count
        got = jnp.concatenate(
            [
                got_ref[:, c * capacity : (c + 1) * capacity, :].reshape(slots, width)
                for c in range(3)
            ],
            axis=1,
        )
        per_tile = width // capacity
        lane = iota((8, width), 1, jnp.int32)
        tiles = []
        for start in range(0, slab_count, per_tile):
            total = jnp.zeros((8, width), F32)
            for source in range(start, min(start + per_tile, slab_count)):
                mark = got_ref[source, 3 * capacity : 3 * capacity + 16, :].astype(F32)[:8]
                off = (source - start) * capacity
                if off:
                    mark = pltpu.roll(mark, off, 1)
                mine = (lane >= off) & (lane < off + capacity)
                total = jnp.where(mine, mark, total)
            tiles.append(total)
        spots = jnp.concatenate(tiles, axis=1) - 1.0
    else:
        got_ref, spot_ref, list_ref, gap_ref, self_ref, pair_ref, out_ref = refs
        width = got_ref.shape[2]
        slots = list_ref.shape[0]
        got = jnp.concatenate([got_ref[c] for c in range(3)], axis=1)
        spots = jnp.broadcast_to(spot_ref[...].astype(F32), (8, slots)) - 1.0

    spot_row = spots[:1]
    spot_col = jnp.transpose(spots)[:, :1]
    land = jnp.where(iota((slots, slots), 0) == spot_row, 1.0, 0.0).astype(BF)
    reply = jnp.where(iota((slots, slots), 1) == spot_col, 1.0, 0.0).astype(BF)
    partner = list_ref[...].astype(F32)
    inverse = 1.0 / gap_ref[...]
    column = iota((slots, slots), 1)
    weight = jnp.zeros((slots, slots), F32)
    for k in range(list_ref.shape[1]):
        weight = weight + jnp.where(column == partner[:, k : k + 1], inverse[:, k : k + 1], 0.0)
    high = weight.astype(BF)
    low = (weight - high.astype(F32)).astype(BF)

    owned = dot_nn(land, got).astype(BF)
    near = (dot_nn(high, owned) + dot_nn(low, owned)).astype(BF)
    coupling = jnp.concatenate([self_ref[...], pair_ref[...]], axis=0)
    fixed = []
    for c in range(3):
        cut = slice(c * width, (c + 1) * width)
        both = jnp.concatenate([owned[:, cut], near[:, cut]], axis=1)
        fixed.append(dot_nn(both, coupling).astype(BF))
    replies = dot_nn(reply, jnp.concatenate(fixed, axis=1)).astype(BF)
    for c in range(3):
        cut = replies[:, c * width : (c + 1) * width]
        if packed:
            out_ref[:, c * capacity : (c + 1) * capacity, :] = cut.reshape(
                slab_count, capacity, width
            )
        else:
            out_ref[c] = cut


def spread_kernel(
    slab_count,
    packed,
    back_ref,
    cols_ref,
    cell_ref,
    pops_ref,
    force_out_ref,
    collided_ref,
    up_ref,
    down_ref,
    ahead_ref,
    behind_ref,
    z_ref,
    y_ref,
    force_ref,
):
    slots, width = cell_ref.shape
    rows, depth = pops_ref.shape[1:]
    capacity = slots // slab_count
    if packed:
        back = jnp.concatenate(
            [
                back_ref[:, c * capacity : (c + 1) * capacity, :].reshape(slots, width)
                for c in range(3)
            ],
            axis=1,
        )
    else:
        back = jnp.concatenate([back_ref[c] for c in range(3)], axis=1)
    cols = cols_ref[...]
    fetch = jnp.where(iota((slots, slots), 1) == cols[:, 4:5], 1.0, 0.0).astype(BF)
    own = dot_nn(fetch, back)
    live = iota((slots, width), 1) < cols[:, 3:4]
    for c in range(3):
        masked = jnp.where(live, own[:, c * width : (c + 1) * width], 0.0)
        force_ref[c] = masked
        force_out_ref[c] = masked.astype(BF)

    cells = cell_ref[...]
    z_ref[...] = (cells % depth).astype(F32)
    y_ref[...] = (cells // depth).astype(F32)

    group = 16

    def spread_group(step, total):
        base = pl.multiple_of(step * group, group)
        z_rows = z_ref[pl.ds(base, group), :]
        y_rows = y_ref[pl.ds(base, group), :]
        f_rows = [force_ref[c, pl.ds(base, group), :] for c in range(3)]
        picks, terms = [], []
        for s in range(group):
            picks.append(one_hot_rows(z_rows[s : s + 1], depth))
            tall = jnp.broadcast_to(y_rows[s : s + 1], (16, width)).astype(BF)
            parts = []
            for c in range(3):
                value = jnp.broadcast_to(f_rows[c][s : s + 1], (16, width)).astype(BF)
                for start in range(0, rows, 16):
                    number = (iota((16, width), 0) + float(start)).astype(BF)
                    parts.append(jnp.where(number == tall, value, jnp.zeros((), BF)))
            terms.append(jnp.concatenate(parts, axis=0))
        return total + dot_nt(jnp.concatenate(terms, axis=1), jnp.concatenate(picks, axis=1))

    total = lax.fori_loop(
        0, slots // group, spread_group, jnp.zeros((3 * rows, depth), F32)
    )

    force = [total[c * rows : (c + 1) * rows] for c in range(3)]
    pops = [pops_ref[number] for number in range(19)]
    density, moment = moments_of(pops)
    velocity = [(moment[c] + 0.5 * force[c]) / density for c in range(3)]
    speed_sq = velocity[0] * velocity[0] + velocity[1] * velocity[1] + velocity[2] * velocity[2]
    work_rate = velocity[0] * force[0] + velocity[1] * force[1] + velocity[2] * force[2]
    base_term = 1.0 - 1.5 * speed_sq
    for number in range(19):
        step = lattice_dirs[number]
        along, push = None, None
        for c in range(3):
            if step[c] == 0:
                continue
            v, f = (velocity[c], force[c]) if step[c] == 1 else (-velocity[c], -force[c])
            along = v if along is None else along + v
            push = f if push is None else push + f
        weight = lattice_weights[number]
        if along is None:
            equilibrium = weight * density * base_term
            source = ((1.0 - 0.5 * relax_rate) * weight * -3.0) * work_rate
        else:
            equilibrium = weight * density * (base_term + 3.0 * along + 4.5 * along * along)
            source = ((1.0 - 0.5 * relax_rate) * weight) * (
                3.0 * (push - work_rate) + 9.0 * along * push
            )
        value = pops[number] - relax_rate * (pops[number] - equilibrium) + source
        collided_ref[number] = value
        if number in forward_x:
            ahead_ref[forward_x.index(number)] = value.astype(BF)
        if number in backward_x:
            behind_ref[backward_x.index(number)] = value.astype(BF)
        if number in upward_y:
            at = upward_y.index(number)
            up_ref[at : at + 1, :] = value[rows - 1 :]
        if number in downward_y:
            at = downward_y.index(number)
            down_ref[at : at + 1, :] = value[:1]
    up_ref[5:, :] = jnp.zeros((3, depth), F32)
    down_ref[5:, :] = jnp.zeros((3, depth), F32)


def stream_kernel(
    sub_ref, collided_ref, low_ref, high_ref, ahead_ref, behind_ref, corner_f, corner_b, read_ref
):
    rows, depth = collided_ref.shape[1:]
    row = iota((rows, depth), 0, jnp.int32)
    at_low, at_high = sub_ref[0] == 0, sub_ref[0] == sub_ref[1] - 1
    low_wall = jnp.where(at_low, 1, 0)
    high_wall = jnp.where(at_high, 1, 0)
    for number in range(19):
        step_x, step_y, step_z = lattice_dirs[number]
        if step_x == 1:
            moved = ahead_ref[forward_x.index(number)].astype(F32)
        elif step_x == -1:
            moved = behind_ref[backward_x.index(number)].astype(F32)
        else:
            moved = collided_ref[number]
        if step_y != 0:
            rolled = pltpu.roll(moved, 1 if step_y == 1 else rows - 1, 0)
            edge_row = 0 if step_y == 1 else rows - 1
            if step_x == 0:
                at = (upward_y if step_y == 1 else downward_y).index(number)
                edge = (low_ref if step_y == 1 else high_ref)[at : at + 1, :]
            else:
                at = 0 if step_y == 1 else 1
                edge = (corner_f if step_x == 1 else corner_b)[at : at + 1, :]
            moved = jnp.where(row == edge_row, edge, rolled)
        if step_z != 0:
            moved = pltpu.roll(moved, 1 if step_z == 1 else depth - 1, 1)
        if step_y != 0:
            wall = low_wall if step_y == 1 else high_wall
            at_wall = (row == edge_row) & (wall == 1)
            moved = jnp.where(at_wall, collided_ref[opposite_of[number]], moved)
        read_ref[number] = moved


def whole(memory=pltpu.VMEM):
    return pl.BlockSpec(memory_space=memory)


def ring(value, axis, steps):
    count = lax.axis_size(axis)
    return lax.ppermute(value, axis, [(i, (i + steps) % count) for i in range(count)])


def per_device(
    populations,
    marker_cell,
    marker_count,
    particle_count,
    particle_id,
    owner_table,
    particle_velocity,
    pair_list,
    pair_gap,
    self_coupling,
    pair_coupling,
):
    slab_count = lax.axis_size("slab")
    slots, width = marker_cell.shape[2:]
    planes, rows, depth = populations.shape[1:]
    assert planes == 1 and slots <= 256 and slots % slab_count == 0
    capacity = slots // slab_count
    assert capacity <= width
    packed = capacity % 16 == 0 and width % capacity == 0
    pops = populations.reshape(19, rows, depth)
    cells = marker_cell.reshape(slots, width)
    shape = jax.ShapeDtypeStruct

    if packed:
        sample_out = [shape((slab_count, 3 * capacity + 16, width), BF)]
    else:
        sample_out = [shape((3, slots, width), BF), shape((slab_count, width), BF)]
    sample_out.append(shape((slots, 8), F32))
    results = pl.pallas_call(
        functools.partial(sample_kernel, slab_count, packed),
        out_shape=sample_out,
        in_specs=[whole(pltpu.SMEM)] * 2 + [whole()] * 5,
        out_specs=[whole()] * len(sample_out),
        scratch_shapes=[
            pltpu.VMEM((slots, width), F32),
            pltpu.VMEM((slots, width), F32),
            pltpu.VMEM((3, slots, width), F32),
        ],
        name="sample",
    )(
        particle_count.reshape(1),
        owner_table.reshape(slab_count),
        pops,
        cells,
        marker_count.reshape(1, slots),
        particle_id.reshape(1, slots),
        particle_velocity.reshape(3, slots),
    )
    cols = results[-1]

    def exchange(value):
        return lax.all_to_all(value, "slab", split_axis=0, concat_axis=0, tiled=True)

    def by_owner(value):
        value = value.reshape(3, slab_count, capacity, width)
        return jnp.transpose(value, (1, 0, 2, 3)).reshape(slab_count, 3 * capacity, width)

    def by_component(value):
        value = value.reshape(slab_count, 3, capacity, width)
        return jnp.transpose(value, (1, 0, 2, 3)).reshape(3, slots, width)

    if packed:
        arrived = [exchange(results[0])]
        reply_shape = shape((slab_count, 3 * capacity, width), BF)
    else:
        slip = jnp.concatenate([by_owner(results[0]), results[1][:, None, :]], axis=1)
        got = exchange(slip)
        arrived = [
            by_component(got[:, : 3 * capacity]),
            got[:, 3 * capacity, :capacity].reshape(1, slots),
        ]
        reply_shape = shape((3, slots, width), BF)
    reply = pl.pallas_call(
        functools.partial(owner_kernel, slab_count, packed),
        out_shape=reply_shape,
        in_specs=[whole()] * (len(arrived) + 4),
        out_specs=whole(),
        name="owner",
    )(
        *arrived,
        pair_list.reshape(slots, -1),
        pair_gap.reshape(slots, -1),
        self_coupling,
        pair_coupling,
    )
    back = exchange(reply) if packed else by_component(exchange(by_owner(reply)))

    marker_force, collided, up, down, ahead, behind = pl.pallas_call(
        functools.partial(spread_kernel, slab_count, packed),
        out_shape=[
            shape((3, slots, width), BF),
            shape((19, rows, depth), F32),
            shape((8, depth), F32),
            shape((8, depth), F32),
            shape((5, rows, depth), BF),
            shape((5, rows, depth), BF),
        ],
        in_specs=[whole()] * 4,
        out_specs=[whole()] * 6,
        scratch_shapes=[
            pltpu.VMEM((slots, width), F32),
            pltpu.VMEM((slots, width), F32),
            pltpu.VMEM((3, slots, width), F32),
        ],
        name="spread",
    )(back, cols, cells, pops)

    low = ring(up, "sub", 1)
    high = ring(down, "sub", -1)
    ahead = ring(ahead, "slab", 1)
    behind = ring(behind, "slab", -1)
    corner_f = ring(jnp.concatenate([low[3:4], high[3:4]]), "slab", 1)
    corner_b = ring(jnp.concatenate([low[4:5], high[4:5]]), "slab", -1)
    place = jnp.stack([lax.axis_index("sub"), jnp.int32(lax.axis_size("sub"))]).astype(jnp.int32)
    read = pl.pallas_call(
        stream_kernel,
        out_shape=shape((19, rows, depth), F32),
        in_specs=[whole(pltpu.SMEM)] + [whole()] * 7,
        out_specs=whole(),
        name="stream",
    )(place, collided, low, high, ahead, behind, corner_f, corner_b)
    marker_force = jnp.transpose(marker_force, (1, 0, 2))[None, None]
    return (read.reshape(19, 1, rows, depth), marker_force)


def solution(mesh):
    placed = (
        P(None, "slab", "sub", None),
        P("slab", "sub", None, None),
        P("slab", "sub", None),
        P("slab", "sub"),
        P("slab", "sub", None),
        P("sub", None),
        P("slab", "sub", None, None),
        P("slab", "sub", None, None),
        P("slab", "sub", None, None),
        P(),
        P(),
    )
    return jax.shard_map(
        per_device,
        mesh=mesh,
        in_specs=placed,
        out_specs=(P(None, "slab", "sub", None), P("slab", "sub", None, None, None)),
        check_vma=False,
    )
```

```python
import functools
import math

import jax
import jax.numpy as jnp
from jax import lax
from jax.experimental import pallas as pl
from jax.experimental.pallas import tpu as pltpu
from jax.sharding import PartitionSpec as P

lattice_dirs = [
    (0, 0, 0),
    (1, 0, 0),
    (-1, 0, 0),
    (0, 1, 0),
    (0, -1, 0),
    (0, 0, 1),
    (0, 0, -1),
    (1, 1, 0),
    (-1, -1, 0),
    (1, -1, 0),
    (-1, 1, 0),
    (1, 0, 1),
    (-1, 0, -1),
    (1, 0, -1),
    (-1, 0, 1),
    (0, 1, 1),
    (0, -1, -1),
    (0, 1, -1),
    (0, -1, 1),
]
lattice_weights = [1.0 / 3.0] + [1.0 / 18.0] * 6 + [1.0 / 36.0] * 12
opposite_of = [0, 2, 1, 4, 3, 6, 5, 8, 7, 10, 9, 12, 11, 14, 13, 16, 15, 18, 17]
relax_rate = 1.25
forward_x = [1, 7, 9, 11, 13]
backward_x = [2, 8, 10, 12, 14]
upward_y = [3, 15, 17, 7, 10]
downward_y = [4, 16, 18, 9, 8]
sample_unroll = 64
spread_unroll = 64
kernel_memory = 16 << 20
BF = jnp.bfloat16
F32 = jnp.float32


def iota(shape, dim, dtype=F32):
    value = lax.broadcasted_iota(jnp.int32, shape, dim)
    return value if dtype == jnp.int32 else value.astype(F32).astype(dtype)


def dot_nt(a, b):
    return lax.dot_general(a, b, (((1,), (1,)), ((), ())), preferred_element_type=F32)


def dot_nn(a, b):
    return jnp.dot(a, b, preferred_element_type=F32)


def moments_of(pops):
    density = pops[0]
    moment = [None, None, None]
    for number in range(19):
        if number:
            density = density + pops[number]
        for axis in range(3):
            step = lattice_dirs[number][axis]
            if step == 0:
                continue
            if moment[axis] is None:
                moment[axis] = pops[number] if step == 1 else -pops[number]
            elif step == 1:
                moment[axis] = moment[axis] + pops[number]
            else:
                moment[axis] = moment[axis] - pops[number]
    return density, moment


def one_hot_rows(row, count, kind=BF):
    tall = jnp.broadcast_to(row, (16, row.shape[1])).astype(kind)
    one, zero = jnp.ones((), kind), jnp.zeros((), kind)
    parts = []
    for start in range(0, count, 16):
        number = iota((16, row.shape[1]), 0, F32) + float(start)
        parts.append(jnp.where(number.astype(kind) == tall, one, zero))
    return jnp.concatenate(parts, axis=0)


def fold_rows(blocks):
    row = iota(blocks[0].shape, 0, jnp.int32)
    half = 4
    while half:
        merged = []
        for s in range(half):
            a, b = blocks[s], blocks[s + half]
            merged.append(
                jnp.where(
                    (row & half) == 0,
                    a + pltpu.roll(a, 8 - half, 0),
                    b + pltpu.roll(b, half, 0),
                )
            )
        blocks = merged
        half //= 2
    return blocks[0]


def sample_kernel(
    slab_count,
    packed,
    count_ref,
    table_ref,
    pops_ref,
    cell_ref,
    marker_count_ref,
    id_ref,
    velocity_ref,
    slip_ref,
    *rest,
):
    if packed:
        cols_ref, z_ref, y_ref, sampled_ref = rest
    else:
        spot_ref, cols_ref, z_ref, y_ref, sampled_ref = rest
    slots, width = cell_ref.shape
    rows, depth = pops_ref.shape[1:]
    capacity = slots // slab_count

    density, moment = moments_of([pops_ref[number] for number in range(19)])
    flow = jnp.concatenate([part / density for part in moment], axis=0)
    high = flow.astype(BF)
    low = (flow - high.astype(F32)).astype(BF)
    flow_pair = jnp.concatenate([high, low], axis=1)

    cells = cell_ref[...]
    z_ref[...] = (cells % depth).astype(F32)
    y_ref[...] = (cells // depth).astype(F32)

    group = math.gcd(slots, sample_unroll)

    def sample_group(step, carry):
        base = pl.multiple_of(step * group, group)
        for eight in range(0, group, 8):
            z_rows = z_ref[pl.ds(base + eight, 8), :]
            y_rows = y_ref[pl.ds(base + eight, 8), :]
            parts = [[], [], []]
            for first in range(0, 8, 2):
                picks = jnp.concatenate(
                    [one_hot_rows(z_rows[s : s + 1], depth) for s in (first, first + 1)], axis=1
                )
                picked = dot_nn(flow_pair, jnp.concatenate([picks, picks], axis=0))
                for s in (first, first + 1):
                    cut = slice((s - first) * width, (s - first + 1) * width)
                    tall = jnp.broadcast_to(y_rows[s : s + 1], (8, width))
                    found = [jnp.zeros((8, width), F32)] * 3
                    for start in range(0, rows, 8):
                        mask = iota((8, width), 0) + float(start) == tall
                        for c in range(3):
                            at = c * rows + start
                            found[c] = jnp.where(mask, picked[at : at + 8, cut], found[c])
                    for c in range(3):
                        parts[c].append(found[c])
            for c in range(3):
                sampled_ref[c, pl.ds(base + eight, 8), :] = fold_rows(parts[c])
        return carry

    lax.fori_loop(0, slots // group, sample_group, 0)

    lane = iota((1, slots), 1, jnp.int32)
    alive = lane < count_ref[0]
    identity = id_ref[...]
    block = identity // slots
    spot = (identity % slots).astype(F32)

    def look_up(b, owner):
        return jnp.where(block == b, table_ref[b], owner)

    owner = lax.fori_loop(0, slab_count, look_up, jnp.zeros((1, slots), jnp.int32))
    owner = jnp.where(alive, owner, -1)
    owner_f = owner.astype(F32)
    chosen = jnp.where(iota((slab_count, slots), 0) == owner_f, 1.0, 0.0)
    before = jnp.where(
        iota((slots, slots), 0) < iota((slots, slots), 1), 1.0, 0.0
    ).astype(BF)
    earlier = dot_nn(chosen.astype(BF), before)
    position = jnp.sum(chosen * earlier, axis=0, keepdims=True)
    send_row = jnp.where(alive, owner_f * float(capacity) + position, -1.0)

    count = jnp.where(alive, marker_count_ref[...], 0).astype(F32)
    velocity = jnp.concatenate([velocity_ref[c] for c in range(3)], axis=0)
    stack = jnp.concatenate(
        [velocity, count, send_row, jnp.zeros((3, slots), F32)], axis=0
    )
    cols = jnp.transpose(stack)
    cols_ref[...] = cols
    live = iota((slots, width), 1) < cols[:, 3:4]
    slips = []
    for c in range(3):
        slips.append(jnp.where(live, cols[:, c : c + 1] - sampled_ref[c], 0.0).astype(BF))
    place = jnp.where(iota((slots, slots), 0) == send_row, 1.0, 0.0).astype(BF)
    sent = dot_nn(place, jnp.concatenate(slips, axis=1)).astype(BF)
    where_to = jnp.where(iota((width, slots), 0) == position, 1.0, 0.0).astype(BF)
    if packed:
        for c in range(3):
            slip_ref[:, c * capacity : (c + 1) * capacity, :] = sent[
                :, c * width : (c + 1) * width
            ].reshape(slab_count, capacity, width)
        taken = (iota((slab_count * 16, slots), 0, jnp.int32) // 16).astype(F32) == owner_f
        marks = dot_nt(jnp.where(taken, spot + 1.0, 0.0).astype(BF), where_to)
        slip_ref[:, 3 * capacity :, :] = marks.astype(BF).reshape(slab_count, 16, width)
    else:
        for c in range(3):
            slip_ref[c] = sent[:, c * width : (c + 1) * width]
        marks = dot_nt((chosen * (spot + 1.0)).astype(BF), where_to)
        spot_ref[...] = marks.astype(BF)


def owner_kernel(
    slab_count,
    packed,
    *refs,
):
    if packed:
        got_ref, list_ref, gap_ref, self_ref, pair_ref, out_ref = refs
        width = got_ref.shape[2]
        slots = list_ref.shape[1]
        capacity = slots // slab_count
        got = jnp.concatenate(
            [
                got_ref[:, c * capacity : (c + 1) * capacity, :].reshape(slots, width)
                for c in range(3)
            ],
            axis=1,
        )
        per_tile = width // capacity
        lane = iota((8, width), 1, jnp.int32)
        tiles = []
        for start in range(0, slab_count, per_tile):
            total = jnp.zeros((8, width), F32)
            for source in range(start, min(start + per_tile, slab_count)):
                mark = got_ref[source, 3 * capacity : 3 * capacity + 16, :].astype(F32)[:8]
                off = (source - start) * capacity
                if off:
                    mark = pltpu.roll(mark, off, 1)
                mine = (lane >= off) & (lane < off + capacity)
                total = jnp.where(mine, mark, total)
            tiles.append(total)
        spots = jnp.concatenate(tiles, axis=1) - 1.0
    else:
        got_ref, spot_ref, list_ref, gap_ref, self_ref, pair_ref, out_ref = refs
        width = got_ref.shape[2]
        slots = list_ref.shape[1]
        got = jnp.concatenate([got_ref[c] for c in range(3)], axis=1)
        spots = jnp.broadcast_to(spot_ref[...].astype(F32), (8, slots)) - 1.0

    spot_row = spots[:1]
    spot_col = jnp.transpose(spots)[:, :1]
    land = jnp.where(iota((slots, slots), 0) == spot_row, 1.0, 0.0).astype(BF)
    reply = jnp.where(iota((slots, slots), 1) == spot_col, 1.0, 0.0).astype(BF)
    pairs = list_ref.shape[0]
    filler = jnp.zeros((-2 * pairs % 8, slots), F32)
    turned = jnp.transpose(
        jnp.concatenate([list_ref[...].astype(F32), 1.0 / gap_ref[...], filler][: 2 + (2 * pairs % 8 > 0)], axis=0)
    )
    partner, inverse = turned[:, :pairs], turned[:, pairs : 2 * pairs]
    column = iota((slots, slots), 1)
    weight = jnp.zeros((slots, slots), F32)
    for k in range(pairs):
        weight = weight + jnp.where(column == partner[:, k : k + 1], inverse[:, k : k + 1], 0.0)
    high = weight.astype(BF)
    low = (weight - high.astype(F32)).astype(BF)

    owned = dot_nn(land, got).astype(BF)
    near = (dot_nn(high, owned) + dot_nn(low, owned)).astype(BF)
    coupling = jnp.concatenate([self_ref[...], pair_ref[...]], axis=0)
    fixed = []
    for c in range(3):
        cut = slice(c * width, (c + 1) * width)
        both = jnp.concatenate([owned[:, cut], near[:, cut]], axis=1)
        fixed.append(dot_nn(both, coupling).astype(BF))
    replies = dot_nn(reply, jnp.concatenate(fixed, axis=1)).astype(BF)
    for c in range(3):
        cut = replies[:, c * width : (c + 1) * width]
        if packed:
            out_ref[:, c * capacity : (c + 1) * capacity, :] = cut.reshape(
                slab_count, capacity, width
            )
        else:
            out_ref[c] = cut


def spread_kernel(
    slab_count,
    packed,
    back_ref,
    cols_ref,
    cell_ref,
    pops_ref,
    force_out_ref,
    collided_ref,
    up_ref,
    down_ref,
    ahead_ref,
    behind_ref,
    z_ref,
    y_ref,
    force_ref,
):
    slots, width = cell_ref.shape
    rows, depth = pops_ref.shape[1:]
    capacity = slots // slab_count
    if packed:
        back = jnp.concatenate(
            [
                back_ref[:, c * capacity : (c + 1) * capacity, :].reshape(slots, width)
                for c in range(3)
            ],
            axis=1,
        )
    else:
        back = jnp.concatenate([back_ref[c] for c in range(3)], axis=1)
    cols = cols_ref[...]
    fetch = jnp.where(iota((slots, slots), 1) == cols[:, 4:5], 1.0, 0.0).astype(BF)
    own = dot_nn(fetch, back)
    live = iota((slots, width), 1) < cols[:, 3:4]
    for c in range(3):
        masked = jnp.where(live, own[:, c * width : (c + 1) * width], 0.0)
        force_ref[c] = masked
        force_out_ref[c] = masked.astype(BF)

    cells = cell_ref[...]
    z_ref[...] = (cells % depth).astype(F32)
    y_ref[...] = (cells // depth).astype(F32)

    group = math.gcd(slots, spread_unroll)

    def spread_group(step, total):
        base = pl.multiple_of(step * group, group)
        z_rows = z_ref[pl.ds(base, group), :]
        y_rows = y_ref[pl.ds(base, group), :]
        f_rows = [force_ref[c, pl.ds(base, group), :] for c in range(3)]
        picks, terms = [], []
        for s in range(group):
            picks.append(one_hot_rows(z_rows[s : s + 1], depth))
            tall = jnp.broadcast_to(y_rows[s : s + 1], (16, width)).astype(BF)
            parts = []
            for c in range(3):
                value = jnp.broadcast_to(f_rows[c][s : s + 1], (16, width)).astype(BF)
                for start in range(0, rows, 16):
                    number = (iota((16, width), 0) + float(start)).astype(BF)
                    parts.append(jnp.where(number == tall, value, jnp.zeros((), BF)))
            terms.append(jnp.concatenate(parts, axis=0))
        return total + dot_nt(jnp.concatenate(terms, axis=1), jnp.concatenate(picks, axis=1))

    total = lax.fori_loop(
        0, slots // group, spread_group, jnp.zeros((3 * rows, depth), F32)
    )

    force = [total[c * rows : (c + 1) * rows] for c in range(3)]
    pops = [pops_ref[number] for number in range(19)]
    density, moment = moments_of(pops)
    velocity = [(moment[c] + 0.5 * force[c]) / density for c in range(3)]
    speed_sq = velocity[0] * velocity[0] + velocity[1] * velocity[1] + velocity[2] * velocity[2]
    work_rate = velocity[0] * force[0] + velocity[1] * force[1] + velocity[2] * force[2]
    base_term = 1.0 - 1.5 * speed_sq
    for number in range(19):
        step = lattice_dirs[number]
        along, push = None, None
        for c in range(3):
            if step[c] == 0:
                continue
            v, f = (velocity[c], force[c]) if step[c] == 1 else (-velocity[c], -force[c])
            along = v if along is None else along + v
            push = f if push is None else push + f
        weight = lattice_weights[number]
        if along is None:
            equilibrium = weight * density * base_term
            source = ((1.0 - 0.5 * relax_rate) * weight * -3.0) * work_rate
        else:
            equilibrium = weight * density * (base_term + 3.0 * along + 4.5 * along * along)
            source = ((1.0 - 0.5 * relax_rate) * weight) * (
                3.0 * (push - work_rate) + 9.0 * along * push
            )
        value = pops[number] - relax_rate * (pops[number] - equilibrium) + source
        collided_ref[number] = value
        if number in forward_x:
            ahead_ref[forward_x.index(number)] = value.astype(BF)
        if number in backward_x:
            behind_ref[backward_x.index(number)] = value.astype(BF)
        if number in upward_y[:3]:
            at = upward_y.index(number)
            up_ref[at : at + 1, :] = value[rows - 1 :]
        if number in downward_y[:3]:
            at = downward_y.index(number)
            down_ref[at : at + 1, :] = value[:1]
    up_ref[3:, :] = jnp.zeros((5, depth), F32)
    down_ref[3:, :] = jnp.zeros((5, depth), F32)


def stream_kernel(
    sub_total, collided_ref, low_ref, high_ref, ahead_ref, behind_ref, read_ref
):
    rows, depth = collided_ref.shape[1:]
    row = iota((rows, depth), 0, jnp.int32)
    place = lax.axis_index("sub")
    low_wall = jnp.where(place == 0, 1, 0)
    high_wall = jnp.where(place == sub_total - 1, 1, 0)
    for number in range(19):
        step_x, step_y, step_z = lattice_dirs[number]
        if step_x == 1:
            moved = ahead_ref[forward_x.index(number)].astype(F32)
        elif step_x == -1:
            moved = behind_ref[backward_x.index(number)].astype(F32)
        else:
            moved = collided_ref[number]
        if step_y != 0:
            rolled = pltpu.roll(moved, 1 if step_y == 1 else rows - 1, 0)
            edge_row = 0 if step_y == 1 else rows - 1
            at = (upward_y if step_y == 1 else downward_y).index(number)
            edge = (low_ref if step_y == 1 else high_ref)[at : at + 1, :]
            moved = jnp.where(row == edge_row, edge, rolled)
        if step_z != 0:
            moved = pltpu.roll(moved, 1 if step_z == 1 else depth - 1, 1)
        if step_y != 0:
            wall = low_wall if step_y == 1 else high_wall
            at_wall = (row == edge_row) & (wall == 1)
            moved = jnp.where(at_wall, collided_ref[opposite_of[number]], moved)
        read_ref[number] = moved


def whole(memory=pltpu.VMEM):
    return pl.BlockSpec(memory_space=memory)


def ring(value, axis, steps):
    count = lax.axis_size(axis)
    return lax.ppermute(value, axis, [(i, (i + steps) % count) for i in range(count)])


def per_device(
    populations,
    marker_cell,
    marker_count,
    particle_count,
    particle_id,
    owner_table,
    particle_velocity,
    pair_list,
    pair_gap,
    self_coupling,
    pair_coupling,
):
    slab_count = lax.axis_size("slab")
    slots, width = marker_cell.shape[2:]
    planes, rows, depth = populations.shape[1:]
    assert planes == 1 and slots <= 256 and slots % slab_count == 0
    capacity = slots // slab_count
    assert capacity <= width
    packed = capacity % 16 == 0 and width % capacity == 0
    pops = populations.reshape(19, rows, depth)
    cells = marker_cell.reshape(slots, width)
    shape = jax.ShapeDtypeStruct
    limits = pltpu.CompilerParams(vmem_limit_bytes=kernel_memory)

    if packed:
        sample_out = [shape((slab_count, 3 * capacity + 16, width), BF)]
    else:
        sample_out = [shape((3, slots, width), BF), shape((slab_count, width), BF)]
    sample_out.append(shape((slots, 8), F32))
    results = pl.pallas_call(
        functools.partial(sample_kernel, slab_count, packed),
        out_shape=sample_out,
        in_specs=[whole(pltpu.SMEM)] * 2 + [whole()] * 5,
        out_specs=[whole()] * len(sample_out),
        scratch_shapes=[
            pltpu.VMEM((slots, width), F32),
            pltpu.VMEM((slots, width), F32),
            pltpu.VMEM((3, slots, width), F32),
        ],
        compiler_params=limits,
        name="sample",
    )(
        particle_count.reshape(1),
        owner_table.reshape(slab_count),
        pops,
        cells,
        marker_count.reshape(1, slots),
        particle_id.reshape(1, slots),
        particle_velocity.reshape(3, 1, slots),
    )
    cols = results[-1]

    def exchange(value):
        return lax.all_to_all(value, "slab", split_axis=0, concat_axis=0, tiled=True)

    def by_owner(value):
        value = value.reshape(3, slab_count, capacity, width)
        return jnp.transpose(value, (1, 0, 2, 3)).reshape(slab_count, 3 * capacity, width)

    def by_component(value):
        value = value.reshape(slab_count, 3, capacity, width)
        return jnp.transpose(value, (1, 0, 2, 3)).reshape(3, slots, width)

    if packed:
        arrived = [exchange(results[0])]
        reply_shape = shape((slab_count, 3 * capacity, width), BF)
    else:
        slip = jnp.concatenate([by_owner(results[0]), results[1][:, None, :]], axis=1)
        got = exchange(slip)
        arrived = [
            by_component(got[:, : 3 * capacity]),
            got[:, 3 * capacity, :capacity].reshape(1, slots),
        ]
        reply_shape = shape((3, slots, width), BF)
    reply = pl.pallas_call(
        functools.partial(owner_kernel, slab_count, packed),
        out_shape=reply_shape,
        in_specs=[whole()] * (len(arrived) + 4),
        out_specs=whole(),
        compiler_params=limits,
        name="owner",
    )(
        *arrived,
        jnp.transpose(pair_list.reshape(slots, -1)),
        jnp.transpose(pair_gap.reshape(slots, -1)),
        self_coupling,
        pair_coupling,
    )
    back = exchange(reply) if packed else by_component(exchange(by_owner(reply)))

    marker_force, collided, up, down, ahead, behind = pl.pallas_call(
        functools.partial(spread_kernel, slab_count, packed),
        out_shape=[
            shape((3, slots, width), BF),
            shape((19, rows, depth), F32),
            shape((8, depth), F32),
            shape((8, depth), F32),
            shape((5, rows, depth), BF),
            shape((5, rows, depth), BF),
        ],
        in_specs=[whole()] * 4,
        out_specs=[whole()] * 6,
        scratch_shapes=[
            pltpu.VMEM((slots, width), F32),
            pltpu.VMEM((slots, width), F32),
            pltpu.VMEM((3, slots, width), F32),
        ],
        compiler_params=limits,
        name="spread",
    )(back, cols, cells, pops)

    ahead = ring(ahead, "slab", 1)
    behind = ring(behind, "slab", -1)
    rise = [ahead[forward_x.index(7), rows - 1 :], behind[backward_x.index(10), rows - 1 :]]
    sink = [ahead[forward_x.index(9), :1], behind[backward_x.index(8), :1]]
    low = ring(jnp.concatenate([up[:3]] + [row.astype(F32) for row in rise]), "sub", 1)
    high = ring(jnp.concatenate([down[:3]] + [row.astype(F32) for row in sink]), "sub", -1)
    read = pl.pallas_call(
        functools.partial(stream_kernel, lax.axis_size("sub")),
        out_shape=shape((19, rows, depth), F32),
        in_specs=[whole()] * 5,
        out_specs=whole(),
        compiler_params=limits,
        name="stream",
    )(collided, low, high, ahead, behind)
    marker_force = jnp.transpose(marker_force, (1, 0, 2))[None, None]
    return (read.reshape(19, 1, rows, depth), marker_force)


def solution(mesh):
    placed = (
        P(None, "slab", "sub", None),
        P("slab", "sub", None, None),
        P("slab", "sub", None),
        P("slab", "sub"),
        P("slab", "sub", None),
        P("sub", None),
        P("slab", "sub", None, None),
        P("slab", "sub", None, None),
        P("slab", "sub", None, None),
        P(),
        P(),
    )
    return jax.shard_map(
        per_device,
        mesh=mesh,
        in_specs=placed,
        out_specs=(P(None, "slab", "sub", None), P("slab", "sub", None, None, None)),
        check_vma=False,
    )
```

```python
import functools
import math

import jax
import jax.numpy as jnp
from jax import lax
from jax.experimental import pallas as pl
from jax.experimental.pallas import tpu as pltpu
from jax.sharding import PartitionSpec as P

lattice_dirs = [
    (0, 0, 0),
    (1, 0, 0),
    (-1, 0, 0),
    (0, 1, 0),
    (0, -1, 0),
    (0, 0, 1),
    (0, 0, -1),
    (1, 1, 0),
    (-1, -1, 0),
    (1, -1, 0),
    (-1, 1, 0),
    (1, 0, 1),
    (-1, 0, -1),
    (1, 0, -1),
    (-1, 0, 1),
    (0, 1, 1),
    (0, -1, -1),
    (0, 1, -1),
    (0, -1, 1),
]
lattice_weights = [1.0 / 3.0] + [1.0 / 18.0] * 6 + [1.0 / 36.0] * 12
opposite_of = [0, 2, 1, 4, 3, 6, 5, 8, 7, 10, 9, 12, 11, 14, 13, 16, 15, 18, 17]
relax_rate = 1.25
forward_x = [1, 7, 9, 11, 13]
backward_x = [2, 8, 10, 12, 14]
upward_y = [3, 15, 17, 7, 10]
downward_y = [4, 16, 18, 9, 8]
sample_unroll = 256
spread_unroll = 256
kernel_memory = 16 << 20
BF = jnp.bfloat16
F32 = jnp.float32


def iota(shape, dim, dtype=F32):
    value = lax.broadcasted_iota(jnp.int32, shape, dim)
    return value if dtype == jnp.int32 else value.astype(F32).astype(dtype)


def dot_nt(a, b):
    return lax.dot_general(a, b, (((1,), (1,)), ((), ())), preferred_element_type=F32)


def dot_nn(a, b):
    return jnp.dot(a, b, preferred_element_type=F32)


def moments_of(pops):
    density = pops[0]
    moment = [None, None, None]
    for number in range(19):
        if number:
            density = density + pops[number]
        for axis in range(3):
            step = lattice_dirs[number][axis]
            if step == 0:
                continue
            if moment[axis] is None:
                moment[axis] = pops[number] if step == 1 else -pops[number]
            elif step == 1:
                moment[axis] = moment[axis] + pops[number]
            else:
                moment[axis] = moment[axis] - pops[number]
    return density, moment


def one_hot_rows(row, count, kind=BF):
    tall = jnp.broadcast_to(row, (16, row.shape[1])).astype(kind)
    one, zero = jnp.ones((), kind), jnp.zeros((), kind)
    parts = []
    for start in range(0, count, 16):
        number = iota((16, row.shape[1]), 0, F32) + float(start)
        parts.append(jnp.where(number.astype(kind) == tall, one, zero))
    return jnp.concatenate(parts, axis=0)


def fold_rows(blocks):
    row = iota(blocks[0].shape, 0, jnp.int32)
    half = 4
    while half:
        merged = []
        for s in range(half):
            a, b = blocks[s], blocks[s + half]
            merged.append(
                jnp.where(
                    (row & half) == 0,
                    a + pltpu.roll(a, 8 - half, 0),
                    b + pltpu.roll(b, half, 0),
                )
            )
        blocks = merged
        half //= 2
    return blocks[0]


def sample_kernel(
    slab_count,
    packed,
    *refs,
):
    sources, refs = refs[:7], refs[7:]
    slip_ref, refs = refs[0], refs[1:]
    if not packed:
        spot_ref, refs = refs[0], refs[1:]
    cols_ref, refs = refs[0], refs[1:]
    targets, (z_ref, y_ref, sampled_ref, sems) = refs[:7], refs[7:]
    copies = [
        pltpu.make_async_copy(source, target, sems.at[number])
        for number, (source, target) in enumerate(zip(sources, targets))
    ]
    for copy in copies:
        copy.start()
    count_ref, table_ref, marker_count_ref, id_ref, velocity_ref, pops_ref, cell_ref = targets
    slots, width = cell_ref.shape
    rows, depth = pops_ref.shape[1:]
    capacity = slots // slab_count
    for copy in copies[:5]:
        copy.wait()

    lane = iota((1, slots), 1, jnp.int32)
    alive = lane < count_ref[0]
    identity = id_ref[...]
    block = identity // slots
    spot = (identity % slots).astype(F32)

    def look_up(b, owner):
        return jnp.where(block == b, table_ref[b], owner)

    owner = lax.fori_loop(0, slab_count, look_up, jnp.zeros((1, slots), jnp.int32))
    owner = jnp.where(alive, owner, -1)
    owner_f = owner.astype(F32)
    chosen = jnp.where(iota((slab_count, slots), 0) == owner_f, 1.0, 0.0)
    before = jnp.where(
        iota((slots, slots), 0) < iota((slots, slots), 1), 1.0, 0.0
    ).astype(BF)
    earlier = dot_nn(chosen.astype(BF), before)
    position = jnp.sum(chosen * earlier, axis=0, keepdims=True)
    send_row = jnp.where(alive, owner_f * float(capacity) + position, -1.0)

    count = jnp.where(alive, marker_count_ref[...], 0).astype(F32)
    velocity = jnp.concatenate([velocity_ref[c] for c in range(3)], axis=0)
    stack = jnp.concatenate(
        [velocity, count, send_row, jnp.zeros((3, slots), F32)], axis=0
    )
    cols = jnp.transpose(stack)
    cols_ref[...] = cols
    for copy in copies[5:]:
        copy.wait()

    density, moment = moments_of([pops_ref[number] for number in range(19)])
    flow = jnp.concatenate([part / density for part in moment], axis=0)
    high = flow.astype(BF)
    low = (flow - high.astype(F32)).astype(BF)
    flow_pair = jnp.concatenate([high, low], axis=1)

    cells = cell_ref[...]
    z_ref[...] = (cells % depth).astype(F32)
    y_ref[...] = (cells // depth).astype(F32)

    group = math.gcd(slots, sample_unroll)

    def sample_group(step, carry):
        base = pl.multiple_of(step * group, group)
        for eight in range(0, group, 8):
            z_rows = z_ref[pl.ds(base + eight, 8), :]
            y_rows = y_ref[pl.ds(base + eight, 8), :]
            parts = [[], [], []]
            for first in range(0, 8, 2):
                picks = jnp.concatenate(
                    [one_hot_rows(z_rows[s : s + 1], depth) for s in (first, first + 1)], axis=1
                )
                picked = dot_nn(flow_pair, jnp.concatenate([picks, picks], axis=0))
                for s in (first, first + 1):
                    cut = slice((s - first) * width, (s - first + 1) * width)
                    tall = jnp.broadcast_to(y_rows[s : s + 1], (8, width))
                    found = [jnp.zeros((8, width), F32)] * 3
                    for start in range(0, rows, 8):
                        mask = iota((8, width), 0) + float(start) == tall
                        for c in range(3):
                            at = c * rows + start
                            found[c] = jnp.where(mask, picked[at : at + 8, cut], found[c])
                    for c in range(3):
                        parts[c].append(found[c])
            for c in range(3):
                sampled_ref[c, pl.ds(base + eight, 8), :] = fold_rows(parts[c])
        return carry

    lax.fori_loop(0, slots // group, sample_group, 0)

    live = iota((slots, width), 1) < cols[:, 3:4]
    slips = []
    for c in range(3):
        slips.append(jnp.where(live, cols[:, c : c + 1] - sampled_ref[c], 0.0).astype(BF))
    place = jnp.where(iota((slots, slots), 0) == send_row, 1.0, 0.0).astype(BF)
    sent = dot_nn(place, jnp.concatenate(slips, axis=1)).astype(BF)
    where_to = jnp.where(iota((width, slots), 0) == position, 1.0, 0.0).astype(BF)
    if packed:
        for c in range(3):
            slip_ref[:, c * capacity : (c + 1) * capacity, :] = sent[
                :, c * width : (c + 1) * width
            ].reshape(slab_count, capacity, width)
        taken = (iota((slab_count * 16, slots), 0, jnp.int32) // 16).astype(F32) == owner_f
        marks = dot_nt(jnp.where(taken, spot + 1.0, 0.0).astype(BF), where_to)
        slip_ref[:, 3 * capacity :, :] = marks.astype(BF).reshape(slab_count, 16, width)
    else:
        for c in range(3):
            slip_ref[c] = sent[:, c * width : (c + 1) * width]
        marks = dot_nt((chosen * (spot + 1.0)).astype(BF), where_to)
        spot_ref[...] = marks.astype(BF)


def owner_kernel(
    slab_count,
    packed,
    *refs,
):
    if packed:
        got_ref, list_ref, gap_ref, self_ref, pair_ref, out_ref = refs
        width = got_ref.shape[2]
        slots = list_ref.shape[1]
        capacity = slots // slab_count
        got = jnp.concatenate(
            [
                got_ref[:, c * capacity : (c + 1) * capacity, :].reshape(slots, width)
                for c in range(3)
            ],
            axis=1,
        )
        per_tile = width // capacity
        lane = iota((8, width), 1, jnp.int32)
        tiles = []
        for start in range(0, slab_count, per_tile):
            total = jnp.zeros((8, width), F32)
            for source in range(start, min(start + per_tile, slab_count)):
                mark = got_ref[source, 3 * capacity : 3 * capacity + 16, :].astype(F32)[:8]
                off = (source - start) * capacity
                if off:
                    mark = pltpu.roll(mark, off, 1)
                mine = (lane >= off) & (lane < off + capacity)
                total = jnp.where(mine, mark, total)
            tiles.append(total)
        spots = jnp.concatenate(tiles, axis=1) - 1.0
    else:
        got_ref, spot_ref, list_ref, gap_ref, self_ref, pair_ref, out_ref = refs
        width = got_ref.shape[2]
        slots = list_ref.shape[1]
        got = jnp.concatenate([got_ref[c] for c in range(3)], axis=1)
        spots = jnp.broadcast_to(spot_ref[...].astype(F32), (8, slots)) - 1.0

    spot_row = spots[:1]
    spot_col = jnp.transpose(spots)[:, :1]
    land = jnp.where(iota((slots, slots), 0) == spot_row, 1.0, 0.0).astype(BF)
    reply = jnp.where(iota((slots, slots), 1) == spot_col, 1.0, 0.0).astype(BF)
    pairs = list_ref.shape[0]
    filler = jnp.zeros((-2 * pairs % 8, slots), F32)
    turned = jnp.transpose(
        jnp.concatenate([list_ref[...].astype(F32), 1.0 / gap_ref[...], filler][: 2 + (2 * pairs % 8 > 0)], axis=0)
    )
    partner, inverse = turned[:, :pairs], turned[:, pairs : 2 * pairs]
    column = iota((slots, slots), 1)
    weight = jnp.zeros((slots, slots), F32)
    for k in range(pairs):
        weight = weight + jnp.where(column == partner[:, k : k + 1], inverse[:, k : k + 1], 0.0)
    high = weight.astype(BF)
    low = (weight - high.astype(F32)).astype(BF)

    owned = dot_nn(land, got).astype(BF)
    near = (dot_nn(high, owned) + dot_nn(low, owned)).astype(BF)
    coupling = jnp.concatenate([self_ref[...], pair_ref[...]], axis=0)
    fixed = []
    for c in range(3):
        cut = slice(c * width, (c + 1) * width)
        both = jnp.concatenate([owned[:, cut], near[:, cut]], axis=1)
        fixed.append(dot_nn(both, coupling).astype(BF))
    replies = dot_nn(reply, jnp.concatenate(fixed, axis=1)).astype(BF)
    for c in range(3):
        cut = replies[:, c * width : (c + 1) * width]
        if packed:
            out_ref[:, c * capacity : (c + 1) * capacity, :] = cut.reshape(
                slab_count, capacity, width
            )
        else:
            out_ref[c] = cut


def spread_kernel(
    slab_count,
    packed,
    back_ref,
    cols_ref,
    cell_ref,
    pops_ref,
    force_out_ref,
    collided_ref,
    up_ref,
    down_ref,
    first_ref,
    second_ref,
    z_ref,
    y_ref,
    force_ref,
):
    slots, width = cell_ref.shape
    rows, depth = pops_ref.shape[1:]
    capacity = slots // slab_count
    if packed:
        back = jnp.concatenate(
            [
                back_ref[:, c * capacity : (c + 1) * capacity, :].reshape(slots, width)
                for c in range(3)
            ],
            axis=1,
        )
    else:
        back = jnp.concatenate([back_ref[c] for c in range(3)], axis=1)
    cols = cols_ref[...]
    fetch = jnp.where(iota((slots, slots), 1) == cols[:, 4:5], 1.0, 0.0).astype(BF)
    own = dot_nn(fetch, back)
    live = iota((slots, width), 1) < cols[:, 3:4]
    for c in range(3):
        masked = jnp.where(live, own[:, c * width : (c + 1) * width], 0.0)
        force_ref[c] = masked
        force_out_ref[c] = masked.astype(BF)

    cells = cell_ref[...]
    z_ref[...] = (cells % depth).astype(F32)
    y_ref[...] = (cells // depth).astype(F32)

    group = math.gcd(slots, spread_unroll)

    def spread_group(step, total):
        base = pl.multiple_of(step * group, group)
        z_rows = z_ref[pl.ds(base, group), :]
        y_rows = y_ref[pl.ds(base, group), :]
        f_rows = [force_ref[c, pl.ds(base, group), :] for c in range(3)]
        picks, terms = [], []
        for s in range(group):
            picks.append(one_hot_rows(z_rows[s : s + 1], depth))
            tall = jnp.broadcast_to(y_rows[s : s + 1], (16, width)).astype(BF)
            parts = []
            for c in range(3):
                value = jnp.broadcast_to(f_rows[c][s : s + 1], (16, width)).astype(BF)
                for start in range(0, rows, 16):
                    number = (iota((16, width), 0) + float(start)).astype(BF)
                    parts.append(jnp.where(number == tall, value, jnp.zeros((), BF)))
            terms.append(jnp.concatenate(parts, axis=0))
        return total + dot_nt(jnp.concatenate(terms, axis=1), jnp.concatenate(picks, axis=1))

    total = lax.fori_loop(
        0, slots // group, spread_group, jnp.zeros((3 * rows, depth), F32)
    )

    force = [total[c * rows : (c + 1) * rows] for c in range(3)]
    pops = [pops_ref[number] for number in range(19)]
    density, moment = moments_of(pops)
    velocity = [(moment[c] + 0.5 * force[c]) / density for c in range(3)]
    speed_sq = velocity[0] * velocity[0] + velocity[1] * velocity[1] + velocity[2] * velocity[2]
    work_rate = velocity[0] * force[0] + velocity[1] * force[1] + velocity[2] * force[2]
    base_term = 1.0 - 1.5 * speed_sq
    even = (lax.axis_index("slab") & 1) == 0
    sent = {}
    for number in range(19):
        step = lattice_dirs[number]
        along, push = None, None
        for c in range(3):
            if step[c] == 0:
                continue
            v, f = (velocity[c], force[c]) if step[c] == 1 else (-velocity[c], -force[c])
            along = v if along is None else along + v
            push = f if push is None else push + f
        weight = lattice_weights[number]
        if along is None:
            equilibrium = weight * density * base_term
            source = ((1.0 - 0.5 * relax_rate) * weight * -3.0) * work_rate
        else:
            equilibrium = weight * density * (base_term + 3.0 * along + 4.5 * along * along)
            source = ((1.0 - 0.5 * relax_rate) * weight) * (
                3.0 * (push - work_rate) + 9.0 * along * push
            )
        value = pops[number] - relax_rate * (pops[number] - equilibrium) + source
        collided_ref[number] = value
        if step[0] != 0:
            sent.setdefault((forward_x if step[0] == 1 else backward_x).index(number), {})[
                step[0]
            ] = value
        if number in upward_y[:3]:
            at = upward_y.index(number)
            up_ref[at : at + 1, :] = value[rows - 1 :]
        if number in downward_y[:3]:
            at = downward_y.index(number)
            down_ref[at : at + 1, :] = value[:1]
    for at, pair in sent.items():
        first_ref[at] = jnp.where(even, pair[1], pair[-1]).astype(BF)
        second_ref[at] = jnp.where(even, pair[-1], pair[1]).astype(BF)
    up_ref[3:, :] = jnp.zeros((5, depth), F32)
    down_ref[3:, :] = jnp.zeros((5, depth), F32)


def stream_kernel(
    sub_total, collided_ref, one_ref, two_ref, first_ref, second_ref, read_ref
):
    rows, depth = collided_ref.shape[1:]
    row = iota((rows, depth), 0, jnp.int32)
    place = lax.axis_index("sub")
    slab_even = (lax.axis_index("slab") & 1) == 0
    sub_even = (place & 1) == 0
    low = jnp.where(sub_even, two_ref[...], one_ref[...])
    high = jnp.where(sub_even, one_ref[...], two_ref[...])
    low_wall = jnp.where(place == 0, 1, 0)
    high_wall = jnp.where(place == sub_total - 1, 1, 0)
    for number in range(19):
        step_x, step_y, step_z = lattice_dirs[number]
        if step_x == 1:
            at = forward_x.index(number)
            moved = jnp.where(slab_even, second_ref[at].astype(F32), first_ref[at].astype(F32))
        elif step_x == -1:
            at = backward_x.index(number)
            moved = jnp.where(slab_even, first_ref[at].astype(F32), second_ref[at].astype(F32))
        else:
            moved = collided_ref[number]
        if step_y != 0:
            rolled = pltpu.roll(moved, 1 if step_y == 1 else rows - 1, 0)
            edge_row = 0 if step_y == 1 else rows - 1
            at = (upward_y if step_y == 1 else downward_y).index(number)
            edge = (low if step_y == 1 else high)[at : at + 1]
            moved = jnp.where(row == edge_row, edge, rolled)
        if step_z != 0:
            moved = pltpu.roll(moved, 1 if step_z == 1 else depth - 1, 1)
        if step_y != 0:
            wall = low_wall if step_y == 1 else high_wall
            at_wall = (row == edge_row) & (wall == 1)
            moved = jnp.where(at_wall, collided_ref[opposite_of[number]], moved)
        read_ref[number] = moved


def whole(memory=pltpu.VMEM):
    return pl.BlockSpec(memory_space=memory)


def swap(value, axis, odd):
    count = lax.axis_size(axis)
    pairs = [(i, (i + 1 if i % 2 == odd else i - 1) % count) for i in range(count)]
    return lax.ppermute(value, axis, pairs)


def per_device(
    populations,
    marker_cell,
    marker_count,
    particle_count,
    particle_id,
    owner_table,
    particle_velocity,
    pair_list,
    pair_gap,
    self_coupling,
    pair_coupling,
):
    slab_count = lax.axis_size("slab")
    slots, width = marker_cell.shape[2:]
    planes, rows, depth = populations.shape[1:]
    assert planes == 1 and slots <= 256 and slots % slab_count == 0
    assert slab_count % 2 == 0 and lax.axis_size("sub") % 2 == 0
    capacity = slots // slab_count
    assert capacity <= width
    packed = capacity % 16 == 0 and width % capacity == 0
    pops = populations.reshape(19, rows, depth)
    cells = marker_cell.reshape(slots, width)
    shape = jax.ShapeDtypeStruct
    limits = pltpu.CompilerParams(vmem_limit_bytes=kernel_memory)

    if packed:
        sample_out = [shape((slab_count, 3 * capacity + 16, width), BF)]
    else:
        sample_out = [shape((3, slots, width), BF), shape((slab_count, width), BF)]
    sample_out.append(shape((slots, 8), F32))
    results = pl.pallas_call(
        functools.partial(sample_kernel, slab_count, packed),
        out_shape=sample_out,
        in_specs=[whole(pltpu.HBM)] * 7,
        out_specs=[whole()] * len(sample_out),
        scratch_shapes=[
            pltpu.SMEM((1,), jnp.int32),
            pltpu.SMEM((slab_count,), jnp.int32),
            pltpu.VMEM((1, slots), jnp.int32),
            pltpu.VMEM((1, slots), jnp.int32),
            pltpu.VMEM((3, 1, slots), F32),
            pltpu.VMEM((19, rows, depth), F32),
            pltpu.VMEM((slots, width), jnp.int32),
            pltpu.VMEM((slots, width), F32),
            pltpu.VMEM((slots, width), F32),
            pltpu.VMEM((3, slots, width), F32),
            pltpu.SemaphoreType.DMA((7,)),
        ],
        compiler_params=limits,
        name="sample",
    )(
        particle_count.reshape(1),
        *[
            pltpu.with_memory_space_constraint(value, pltpu.HBM)
            for value in (
                owner_table.reshape(slab_count),
                marker_count.reshape(1, slots),
                particle_id.reshape(1, slots),
                particle_velocity.reshape(3, 1, slots),
                pops,
                cells,
            )
        ],
    )
    cols = results[-1]

    def exchange(value):
        return lax.all_to_all(value, "slab", split_axis=0, concat_axis=0, tiled=True)

    def by_owner(value):
        value = value.reshape(3, slab_count, capacity, width)
        return jnp.transpose(value, (1, 0, 2, 3)).reshape(slab_count, 3 * capacity, width)

    def by_component(value):
        value = value.reshape(slab_count, 3, capacity, width)
        return jnp.transpose(value, (1, 0, 2, 3)).reshape(3, slots, width)

    if packed:
        arrived = [exchange(results[0])]
        reply_shape = shape((slab_count, 3 * capacity, width), BF)
    else:
        slip = jnp.concatenate([by_owner(results[0]), results[1][:, None, :]], axis=1)
        got = exchange(slip)
        arrived = [
            by_component(got[:, : 3 * capacity]),
            got[:, 3 * capacity, :capacity].reshape(1, slots),
        ]
        reply_shape = shape((3, slots, width), BF)
    reply = pl.pallas_call(
        functools.partial(owner_kernel, slab_count, packed),
        out_shape=reply_shape,
        in_specs=[whole()] * (len(arrived) + 4),
        out_specs=whole(),
        compiler_params=limits,
        name="owner",
    )(
        *arrived,
        jnp.transpose(pair_list.reshape(slots, -1)),
        jnp.transpose(pair_gap.reshape(slots, -1)),
        self_coupling,
        pair_coupling,
    )
    back = exchange(reply) if packed else by_component(exchange(by_owner(reply)))

    marker_force, collided, up, down, first, second = pl.pallas_call(
        functools.partial(spread_kernel, slab_count, packed),
        out_shape=[
            shape((3, slots, width), BF),
            shape((19, rows, depth), F32),
            shape((8, depth), F32),
            shape((8, depth), F32),
            shape((5, rows, depth), BF),
            shape((5, rows, depth), BF),
        ],
        in_specs=[whole()] * 4,
        out_specs=[whole()] * 6,
        scratch_shapes=[
            pltpu.VMEM((slots, width), F32),
            pltpu.VMEM((slots, width), F32),
            pltpu.VMEM((3, slots, width), F32),
        ],
        compiler_params=limits,
        name="spread",
    )(back, cols, cells, pops)

    slab_even = (lax.axis_index("slab") & 1) == 0
    sub_even = (lax.axis_index("sub") & 1) == 0
    first, second = swap(first, "slab", 0), swap(second, "slab", 1)
    top, bottom = slice(rows - 1, rows), slice(0, 1)
    one_up = jnp.where(slab_even, second[1, top], first[1, top])
    two_up = jnp.where(slab_even, first[2, top], second[2, top])
    one_down = jnp.where(slab_even, second[2, bottom], first[2, bottom])
    two_down = jnp.where(slab_even, first[1, bottom], second[1, bottom])
    up = jnp.concatenate([up[:3], one_up.astype(F32), two_up.astype(F32)])
    down = jnp.concatenate([down[:3], one_down.astype(F32), two_down.astype(F32)])
    low_high = (
        swap(jnp.where(sub_even, up, down), "sub", 0),
        swap(jnp.where(sub_even, down, up), "sub", 1),
    )
    read = pl.pallas_call(
        functools.partial(stream_kernel, lax.axis_size("sub")),
        out_shape=shape((19, rows, depth), F32),
        in_specs=[whole()] * 5,
        out_specs=whole(),
        compiler_params=limits,
        name="stream",
    )(collided, *low_high, first, second)
    marker_force = jnp.transpose(marker_force, (1, 0, 2))[None, None]
    return (read.reshape(19, 1, rows, depth), marker_force)


def solution(mesh):
    placed = (
        P(None, "slab", "sub", None),
        P("slab", "sub", None, None),
        P("slab", "sub", None),
        P("slab", "sub"),
        P("slab", "sub", None),
        P("sub", None),
        P("slab", "sub", None, None),
        P("slab", "sub", None, None),
        P("slab", "sub", None, None),
        P(),
        P(),
    )
    return jax.shard_map(
        per_device,
        mesh=mesh,
        in_specs=placed,
        out_specs=(P(None, "slab", "sub", None), P("slab", "sub", None, None, None)),
        check_vma=False,
    )
```

```python
import functools
import math

import jax
import jax.numpy as jnp
from jax import lax
from jax.experimental import pallas as pl
from jax.experimental.pallas import tpu as pltpu
from jax.sharding import PartitionSpec as P

lattice_dirs = [
    (0, 0, 0),
    (1, 0, 0),
    (-1, 0, 0),
    (0, 1, 0),
    (0, -1, 0),
    (0, 0, 1),
    (0, 0, -1),
    (1, 1, 0),
    (-1, -1, 0),
    (1, -1, 0),
    (-1, 1, 0),
    (1, 0, 1),
    (-1, 0, -1),
    (1, 0, -1),
    (-1, 0, 1),
    (0, 1, 1),
    (0, -1, -1),
    (0, 1, -1),
    (0, -1, 1),
]
lattice_weights = [1.0 / 3.0] + [1.0 / 18.0] * 6 + [1.0 / 36.0] * 12
opposite_of = [0, 2, 1, 4, 3, 6, 5, 8, 7, 10, 9, 12, 11, 14, 13, 16, 15, 18, 17]
relax_rate = 1.25
forward_x = [1, 7, 9, 11, 13]
backward_x = [2, 8, 10, 12, 14]
upward_y = [3, 15, 17, 7, 10]
downward_y = [4, 16, 18, 9, 8]
mark_rows = 8
kernel_memory = 16 << 20
BF = jnp.bfloat16
F32 = jnp.float32


def iota(shape, dim, dtype=F32):
    value = lax.broadcasted_iota(jnp.int32, shape, dim)
    return value if dtype == jnp.int32 else value.astype(F32).astype(dtype)


def dot_nt(a, b):
    return lax.dot_general(a, b, (((1,), (1,)), ((), ())), preferred_element_type=F32)


def dot_nn(a, b):
    return jnp.dot(a, b, preferred_element_type=F32)


def moments_of(pops):
    density = pops[0]
    moment = [None, None, None]
    for number in range(19):
        if number:
            density = density + pops[number]
        for axis in range(3):
            step = lattice_dirs[number][axis]
            if step == 0:
                continue
            if moment[axis] is None:
                moment[axis] = pops[number] if step == 1 else -pops[number]
            elif step == 1:
                moment[axis] = moment[axis] + pops[number]
            else:
                moment[axis] = moment[axis] - pops[number]
    return density, moment


def one_hot_rows(row, count, kind=BF):
    tall = jnp.broadcast_to(row, (16, row.shape[1])).astype(kind)
    one, zero = jnp.ones((), kind), jnp.zeros((), kind)
    parts = []
    for start in range(0, count, 16):
        number = iota((16, row.shape[1]), 0, F32) + float(start)
        parts.append(jnp.where(number.astype(kind) == tall, one, zero))
    return jnp.concatenate(parts, axis=0)


def fold_rows(blocks):
    row = iota(blocks[0].shape, 0, jnp.int32)
    half = 4
    while half:
        merged = []
        for s in range(half):
            a, b = blocks[s], blocks[s + half]
            merged.append(
                jnp.where(
                    (row & half) == 0,
                    a + pltpu.roll(a, 8 - half, 0),
                    b + pltpu.roll(b, half, 0),
                )
            )
        blocks = merged
        half //= 2
    return blocks[0]


def pieces_of(value):
    parts = []
    for step in range(3):
        part = value.astype(BF)
        parts.append(part)
        if step < 2:
            value = value - part.astype(F32)
    return parts


def sample_kernel(slab_count, packed, *refs):
    sources, refs = refs[:7], refs[7:]
    slip_ref, refs = refs[0], refs[1:]
    if not packed:
        spot_ref, refs = refs[0], refs[1:]
    send_ref, sorted_ref, z_ref, y_ref = refs[:4]
    targets, (sems,) = refs[4:11], refs[11:]
    copies = [
        pltpu.make_async_copy(source, target, sems.at[number])
        for number, (source, target) in enumerate(zip(sources, targets))
    ]
    for copy in copies:
        copy.start()
    count_ref, table_ref, marker_count_ref, id_ref, velocity_ref, pops_ref, cell_ref = targets
    slots, width = cell_ref.shape
    rows, depth = pops_ref.shape[1:]
    capacity = slots // slab_count
    for copy in copies[:5]:
        copy.wait()

    lane = iota((1, slots), 1, jnp.int32)
    alive = lane < count_ref[0]
    identity = id_ref[...]
    block = identity // slots
    spot = (identity % slots).astype(F32)

    def look_up(b, owner):
        return jnp.where(block == b, table_ref[b], owner)

    owner = lax.fori_loop(0, slab_count, look_up, jnp.zeros((1, slots), jnp.int32))
    owner = jnp.where(alive, owner, -1)
    owner_f = owner.astype(F32)
    chosen = jnp.where(iota((slab_count, slots), 0) == owner_f, 1.0, 0.0)
    before = jnp.where(
        iota((slots, slots), 0) < iota((slots, slots), 1), 1.0, 0.0
    ).astype(BF)
    earlier = dot_nn(chosen.astype(BF), before)
    position = jnp.sum(chosen * earlier, axis=0, keepdims=True)
    send_row = jnp.where(alive, owner_f * float(capacity) + position, -1.0)
    place = jnp.where(iota((slots, slots), 0) == send_row, 1.0, 0.0).astype(BF)

    where_to = jnp.where(iota((width, slots), 0) == position, 1.0, 0.0).astype(BF)
    if packed:
        taken = (iota((slab_count * mark_rows, slots), 0, jnp.int32) // mark_rows).astype(
            F32
        ) == owner_f
        marks = dot_nt(jnp.where(taken, spot + 1.0, 0.0).astype(BF), where_to)
        slip_ref[:, 3 * capacity :, :] = marks.reshape(slab_count, mark_rows, width).astype(BF)
    else:
        spot_ref[...] = dot_nt((chosen * (spot + 1.0)).astype(BF), where_to).astype(BF)

    count = marker_count_ref[...].astype(F32)
    pieces = pieces_of(jnp.concatenate([velocity_ref[c] for c in range(3)], axis=0))
    stack = jnp.concatenate(
        [piece.astype(F32) for piece in pieces] + [count, send_row, jnp.zeros((5, slots), F32)],
        axis=0,
    )
    turned = jnp.transpose(stack)
    send_ref[...] = turned[:, 8:16]
    arranged = dot_nn(place, turned.astype(BF))
    velocity = (arranged[:, 0:3] + arranged[:, 3:6]) + arranged[:, 6:9]
    sorted_ref[...] = arranged[:, 8:16]

    for copy in copies[5:]:
        copy.wait()
    cells = cell_ref[...]
    parted = jnp.concatenate([(cells % depth).astype(BF), (cells // depth).astype(BF)], axis=1)
    moved = dot_nn(place, parted)
    z_ref[...] = moved[:, :width]
    y_ref[...] = moved[:, width:]

    density, moment = moments_of([pops_ref[number] for number in range(19)])
    flow = jnp.concatenate([part / density for part in moment], axis=0)
    high = flow.astype(BF)
    low = (flow - high.astype(F32)).astype(BF)
    flow_pair = jnp.concatenate([high, low], axis=1)

    for base in range(0, slots, 16):
        found_rows = []
        for eight in range(base, base + 16, 8):
            z_rows = z_ref[eight : eight + 8, :]
            y_rows = y_ref[eight : eight + 8, :]
            parts = [[], [], []]
            for first in range(0, 8, 2):
                picks = jnp.concatenate(
                    [one_hot_rows(z_rows[s : s + 1], depth) for s in (first, first + 1)], axis=1
                )
                picked = dot_nn(flow_pair, jnp.concatenate([picks, picks], axis=0))
                for s in (first, first + 1):
                    cut = slice((s - first) * width, (s - first + 1) * width)
                    tall = jnp.broadcast_to(y_rows[s : s + 1], (8, width))
                    found = [jnp.zeros((8, width), F32)] * 3
                    for start in range(0, rows, 8):
                        mask = iota((8, width), 0) + float(start) == tall
                        for c in range(3):
                            at = c * rows + start
                            found[c] = jnp.where(mask, picked[at : at + 8, cut], found[c])
                    for c in range(3):
                        parts[c].append(found[c])
            found_rows.append([fold_rows(parts[c]) for c in range(3)])
        live = iota((16, width), 1) < arranged[base : base + 16, 9:10]
        for c in range(3):
            sampled = jnp.concatenate([found_rows[0][c], found_rows[1][c]], axis=0)
            slip = jnp.where(live, velocity[base : base + 16, c : c + 1] - sampled, 0.0)
            if packed:
                at = c * capacity + base % capacity
                slip_ref[base // capacity, at : at + 16, :] = slip.astype(BF)
            else:
                slip_ref[c, base : base + 16, :] = slip.astype(BF)


def weight_kernel(list_ref, gap_ref, weight_ref):
    pairs, slots = list_ref.shape
    filler = jnp.zeros((-2 * pairs % 8, slots), F32)
    turned = jnp.transpose(
        jnp.concatenate(
            [list_ref[...].astype(F32), 1.0 / gap_ref[...], filler][: 2 + (2 * pairs % 8 > 0)],
            axis=0,
        )
    )
    column = iota((slots, slots), 1)
    weight = jnp.zeros((slots, slots), F32)
    for k in range(pairs):
        inverse = turned[:, pairs + k : pairs + k + 1]
        weight = weight + jnp.where(column == turned[:, k : k + 1], inverse, 0.0)
    high = weight.astype(BF)
    weight_ref[0] = high
    weight_ref[1] = (weight - high.astype(F32)).astype(BF)


def owner_kernel(
    slab_count,
    packed,
    *refs,
):
    if packed:
        got_ref, weight_ref, self_ref, pair_ref, out_ref = refs
        width = got_ref.shape[2]
        slots = weight_ref.shape[1]
        capacity = slots // slab_count
        got = jnp.concatenate(
            [
                got_ref[:, c * capacity : (c + 1) * capacity, :].reshape(slots, width)
                for c in range(3)
            ],
            axis=1,
        )
        per_tile = width // capacity
        lane = iota((8, width), 1, jnp.int32)
        tiles = []
        for start in range(0, slab_count, per_tile):
            total = jnp.zeros((8, width), F32)
            for source in range(start, min(start + per_tile, slab_count)):
                mark = got_ref[source, 3 * capacity : 3 * capacity + mark_rows, :].astype(F32)
                off = (source - start) * capacity
                if off:
                    mark = pltpu.roll(mark, off, 1)
                mine = (lane >= off) & (lane < off + capacity)
                total = jnp.where(mine, mark, total)
            tiles.append(total)
        spots = jnp.concatenate(tiles, axis=1) - 1.0
    else:
        got_ref, spot_ref, weight_ref, self_ref, pair_ref, out_ref = refs
        width = got_ref.shape[2]
        slots = weight_ref.shape[1]
        got = jnp.concatenate([got_ref[c] for c in range(3)], axis=1)
        spots = jnp.broadcast_to(spot_ref[...].astype(F32), (8, slots)) - 1.0

    spot_row = spots[:1]
    spot_col = jnp.transpose(spots)[:, :1]
    land = jnp.where(iota((slots, slots), 0) == spot_row, 1.0, 0.0).astype(BF)
    reply = jnp.where(iota((slots, slots), 1) == spot_col, 1.0, 0.0).astype(BF)
    owned = dot_nn(land, got).astype(BF)
    near = (dot_nn(weight_ref[0], owned) + dot_nn(weight_ref[1], owned)).astype(BF)
    coupling = jnp.concatenate([self_ref[...], pair_ref[...]], axis=0)
    fixed = []
    for c in range(3):
        cut = slice(c * width, (c + 1) * width)
        both = jnp.concatenate([owned[:, cut], near[:, cut]], axis=1)
        fixed.append(dot_nn(both, coupling).astype(BF))
    replies = dot_nn(reply, jnp.concatenate(fixed, axis=1)).astype(BF)
    for c in range(3):
        cut = replies[:, c * width : (c + 1) * width]
        if packed:
            out_ref[:, c * capacity : (c + 1) * capacity, :] = cut.reshape(
                slab_count, capacity, width
            )
        else:
            out_ref[c] = cut


def returned_rows(slab_count, packed, back_ref, sorted_ref, base, count):
    if packed:
        capacity = sorted_ref.shape[0] // slab_count
        at, block = base % capacity, slice(base // capacity, (base + count - 1) // capacity + 1)
        take = min(count, capacity)
        parts = [
            back_ref[block, c * capacity + at : c * capacity + at + take, :].reshape(count, -1)
            for c in range(3)
        ]
    else:
        parts = [back_ref[c, base : base + count, :] for c in range(3)]
    live = iota(parts[0].shape, 1) < sorted_ref[base : base + count, 1:2]
    return [jnp.where(live, part.astype(F32), 0.0) for part in parts]


def finish_kernel(slab_count, packed, back_ref, sorted_ref, send_ref, out_ref):
    slots = sorted_ref.shape[0]
    masked = returned_rows(slab_count, packed, back_ref, sorted_ref, 0, slots)
    fetch = jnp.where(iota((slots, slots), 1) == send_ref[:, 2:3], 1.0, 0.0).astype(BF)
    for c in range(3):
        out_ref[c] = dot_nn(fetch, masked[c].astype(BF)).astype(BF)


def spread_kernel(
    slab_count,
    packed,
    back_ref,
    sorted_ref,
    z_ref,
    y_ref,
    pops_ref,
    collided_ref,
    up_ref,
    down_ref,
    first_ref,
    second_ref,
):
    slots, width = z_ref.shape
    rows, depth = pops_ref.shape[1:]
    picks, terms = [], []
    for base in range(0, slots, 16):
        f_rows = returned_rows(slab_count, packed, back_ref, sorted_ref, base, 16)
        z_rows = z_ref[base : base + 16, :]
        y_rows = y_ref[base : base + 16, :]
        for s in range(16):
            picks.append(one_hot_rows(z_rows[s : s + 1], depth))
            tall = jnp.broadcast_to(y_rows[s : s + 1], (16, width)).astype(BF)
            parts = []
            for c in range(3):
                value = jnp.broadcast_to(f_rows[c][s : s + 1], (16, width)).astype(BF)
                for start in range(0, rows, 16):
                    number = (iota((16, width), 0) + float(start)).astype(BF)
                    parts.append(jnp.where(number == tall, value, jnp.zeros((), BF)))
            terms.append(jnp.concatenate(parts, axis=0))
    total = dot_nt(jnp.concatenate(terms, axis=1), jnp.concatenate(picks, axis=1))

    force = [total[c * rows : (c + 1) * rows] for c in range(3)]
    pops = [pops_ref[number] for number in range(19)]
    density, moment = moments_of(pops)
    velocity = [(moment[c] + 0.5 * force[c]) / density for c in range(3)]
    speed_sq = velocity[0] * velocity[0] + velocity[1] * velocity[1] + velocity[2] * velocity[2]
    work_rate = velocity[0] * force[0] + velocity[1] * force[1] + velocity[2] * force[2]
    base_term = 1.0 - 1.5 * speed_sq
    even = (lax.axis_index("slab") & 1) == 0
    sent = {}
    for number in range(19):
        step = lattice_dirs[number]
        along, push = None, None
        for c in range(3):
            if step[c] == 0:
                continue
            v, f = (velocity[c], force[c]) if step[c] == 1 else (-velocity[c], -force[c])
            along = v if along is None else along + v
            push = f if push is None else push + f
        weight = lattice_weights[number]
        if along is None:
            equilibrium = weight * density * base_term
            source = ((1.0 - 0.5 * relax_rate) * weight * -3.0) * work_rate
        else:
            equilibrium = weight * density * (base_term + 3.0 * along + 4.5 * along * along)
            source = ((1.0 - 0.5 * relax_rate) * weight) * (
                3.0 * (push - work_rate) + 9.0 * along * push
            )
        value = pops[number] - relax_rate * (pops[number] - equilibrium) + source
        collided_ref[number] = value
        if step[0] != 0:
            sent.setdefault((forward_x if step[0] == 1 else backward_x).index(number), {})[
                step[0]
            ] = value
        if number in upward_y[:3]:
            at = upward_y.index(number)
            up_ref[at : at + 1, :] = value[rows - 1 :]
        if number in downward_y[:3]:
            at = downward_y.index(number)
            down_ref[at : at + 1, :] = value[:1]
    for at, pair in sent.items():
        first_ref[at] = jnp.where(even, pair[1], pair[-1]).astype(BF)
        second_ref[at] = jnp.where(even, pair[-1], pair[1]).astype(BF)
    up_ref[3:, :] = jnp.zeros((5, depth), F32)
    down_ref[3:, :] = jnp.zeros((5, depth), F32)


def stream_kernel(
    sub_total, collided_ref, one_ref, two_ref, first_ref, second_ref, read_ref
):
    rows, depth = collided_ref.shape[1:]
    row = iota((rows, depth), 0, jnp.int32)
    place = lax.axis_index("sub")
    slab_even = (lax.axis_index("slab") & 1) == 0
    sub_even = (place & 1) == 0
    low = jnp.where(sub_even, two_ref[...], one_ref[...])
    high = jnp.where(sub_even, one_ref[...], two_ref[...])
    low_wall = jnp.where(place == 0, 1, 0)
    high_wall = jnp.where(place == sub_total - 1, 1, 0)
    for number in range(19):
        step_x, step_y, step_z = lattice_dirs[number]
        if step_x == 1:
            at = forward_x.index(number)
            moved = jnp.where(slab_even, second_ref[at].astype(F32), first_ref[at].astype(F32))
        elif step_x == -1:
            at = backward_x.index(number)
            moved = jnp.where(slab_even, first_ref[at].astype(F32), second_ref[at].astype(F32))
        else:
            moved = collided_ref[number]
        if step_y != 0:
            rolled = pltpu.roll(moved, 1 if step_y == 1 else rows - 1, 0)
            edge_row = 0 if step_y == 1 else rows - 1
            at = (upward_y if step_y == 1 else downward_y).index(number)
            edge = (low if step_y == 1 else high)[at : at + 1]
            moved = jnp.where(row == edge_row, edge, rolled)
        if step_z != 0:
            moved = pltpu.roll(moved, 1 if step_z == 1 else depth - 1, 1)
        if step_y != 0:
            wall = low_wall if step_y == 1 else high_wall
            at_wall = (row == edge_row) & (wall == 1)
            moved = jnp.where(at_wall, collided_ref[opposite_of[number]], moved)
        read_ref[number] = moved


def whole(memory=pltpu.VMEM):
    return pl.BlockSpec(memory_space=memory)


def swap(value, axis, odd):
    count = lax.axis_size(axis)
    pairs = [(i, (i + 1 if i % 2 == odd else i - 1) % count) for i in range(count)]
    return lax.ppermute(value, axis, pairs)


def per_device(
    populations,
    marker_cell,
    marker_count,
    particle_count,
    particle_id,
    owner_table,
    particle_velocity,
    pair_list,
    pair_gap,
    self_coupling,
    pair_coupling,
):
    slab_count = lax.axis_size("slab")
    slots, width = marker_cell.shape[2:]
    planes, rows, depth = populations.shape[1:]
    assert planes == 1 and slots <= 256 and slots % slab_count == 0
    assert slab_count % 2 == 0 and lax.axis_size("sub") % 2 == 0
    capacity = slots // slab_count
    assert capacity <= width
    packed = capacity % 16 == 0 and width % capacity == 0
    pops = populations.reshape(19, rows, depth)
    cells = marker_cell.reshape(slots, width)
    shape = jax.ShapeDtypeStruct
    limits = pltpu.CompilerParams(vmem_limit_bytes=kernel_memory)

    if packed:
        sample_out = [shape((slab_count, 3 * capacity + mark_rows, width), BF)]
    else:
        sample_out = [shape((3, slots, width), BF), shape((slab_count, width), BF)]
    sample_out += [shape((slots, 8), F32)] * 2 + [shape((slots, width), F32)] * 2
    results = pl.pallas_call(
        functools.partial(sample_kernel, slab_count, packed),
        out_shape=sample_out,
        in_specs=[whole(pltpu.HBM)] * 7,
        out_specs=[whole()] * len(sample_out),
        scratch_shapes=[
            pltpu.SMEM((1,), jnp.int32),
            pltpu.SMEM((slab_count,), jnp.int32),
            pltpu.VMEM((1, slots), jnp.int32),
            pltpu.VMEM((1, slots), jnp.int32),
            pltpu.VMEM((3, 1, slots), F32),
            pltpu.VMEM((19, rows, depth), F32),
            pltpu.VMEM((slots, width), jnp.int32),
            pltpu.SemaphoreType.DMA((7,)),
        ],
        compiler_params=limits,
        name="sample",
    )(
        particle_count.reshape(1),
        *[
            pltpu.with_memory_space_constraint(value, pltpu.HBM)
            for value in (
                owner_table.reshape(slab_count),
                marker_count.reshape(1, slots),
                particle_id.reshape(1, slots),
                particle_velocity.reshape(3, 1, slots),
                pops,
                cells,
            )
        ],
    )
    send, ordered, z_cells, y_cells = results[-4:]
    weights = pl.pallas_call(
        weight_kernel,
        out_shape=shape((2, slots, slots), BF),
        in_specs=[whole()] * 2,
        out_specs=whole(),
        compiler_params=limits,
        cost_estimate=pl.CostEstimate(flops=10_000_000, bytes_accessed=300_000, transcendentals=0),
        name="weights",
    )(
        jnp.transpose(pair_list.reshape(slots, -1)),
        jnp.transpose(pair_gap.reshape(slots, -1)),
    )

    def exchange(value):
        return lax.all_to_all(value, "slab", split_axis=0, concat_axis=0, tiled=True)

    def by_owner(value):
        value = value.reshape(3, slab_count, capacity, width)
        return jnp.transpose(value, (1, 0, 2, 3)).reshape(slab_count, 3 * capacity, width)

    def by_component(value):
        value = value.reshape(slab_count, 3, capacity, width)
        return jnp.transpose(value, (1, 0, 2, 3)).reshape(3, slots, width)

    if packed:
        arrived = [exchange(results[0])]
        reply_shape = shape((slab_count, 3 * capacity, width), BF)
    else:
        slip = jnp.concatenate([by_owner(results[0]), results[1][:, None, :]], axis=1)
        got = exchange(slip)
        arrived = [
            by_component(got[:, : 3 * capacity]),
            got[:, 3 * capacity, :capacity].reshape(1, slots),
        ]
        reply_shape = shape((3, slots, width), BF)
    reply = pl.pallas_call(
        functools.partial(owner_kernel, slab_count, packed),
        out_shape=reply_shape,
        in_specs=[whole()] * (len(arrived) + 3),
        out_specs=whole(),
        compiler_params=limits,
        name="owner",
    )(
        *arrived,
        weights,
        self_coupling,
        pair_coupling,
    )
    back = exchange(reply) if packed else by_component(exchange(by_owner(reply)))

    collided, up, down, first, second = pl.pallas_call(
        functools.partial(spread_kernel, slab_count, packed),
        out_shape=[
            shape((19, rows, depth), F32),
            shape((8, depth), F32),
            shape((8, depth), F32),
            shape((5, rows, depth), BF),
            shape((5, rows, depth), BF),
        ],
        in_specs=[whole()] * 5,
        out_specs=[whole()] * 5,
        compiler_params=limits,
        name="spread",
    )(back, ordered, z_cells, y_cells, pops)
    marker_force = pl.pallas_call(
        functools.partial(finish_kernel, slab_count, packed),
        out_shape=shape((3, slots, width), BF),
        in_specs=[whole()] * 3,
        out_specs=whole(),
        compiler_params=limits,
        cost_estimate=pl.CostEstimate(flops=50_000_000, bytes_accessed=400_000, transcendentals=0),
        name="finish",
    )(back, ordered, send)

    slab_even = (lax.axis_index("slab") & 1) == 0
    sub_even = (lax.axis_index("sub") & 1) == 0
    first, second = swap(first, "slab", 0), swap(second, "slab", 1)
    top, bottom = slice(rows - 1, rows), slice(0, 1)
    one_up = jnp.where(slab_even, second[1, top], first[1, top])
    two_up = jnp.where(slab_even, first[2, top], second[2, top])
    one_down = jnp.where(slab_even, second[2, bottom], first[2, bottom])
    two_down = jnp.where(slab_even, first[1, bottom], second[1, bottom])
    up = jnp.concatenate([up[:3], one_up.astype(F32), two_up.astype(F32)])
    down = jnp.concatenate([down[:3], one_down.astype(F32), two_down.astype(F32)])
    low_high = (
        swap(jnp.where(sub_even, up, down), "sub", 0),
        swap(jnp.where(sub_even, down, up), "sub", 1),
    )
    read = pl.pallas_call(
        functools.partial(stream_kernel, lax.axis_size("sub")),
        out_shape=shape((19, rows, depth), F32),
        in_specs=[whole()] * 5,
        out_specs=whole(),
        compiler_params=limits,
        name="stream",
    )(collided, *low_high, first, second)
    marker_force = jnp.transpose(marker_force, (1, 0, 2))[None, None]
    return (read.reshape(19, 1, rows, depth), marker_force)


def solution(mesh):
    placed = (
        P(None, "slab", "sub", None),
        P("slab", "sub", None, None),
        P("slab", "sub", None),
        P("slab", "sub"),
        P("slab", "sub", None),
        P("sub", None),
        P("slab", "sub", None, None),
        P("slab", "sub", None, None),
        P("slab", "sub", None, None),
        P(),
        P(),
    )
    return jax.shard_map(
        per_device,
        mesh=mesh,
        in_specs=placed,
        out_specs=(P(None, "slab", "sub", None), P("slab", "sub", None, None, None)),
        check_vma=False,
    )
```

```python
import functools
import math

import jax
import jax.numpy as jnp
from jax import lax
from jax.experimental import pallas as pl
from jax.experimental.pallas import tpu as pltpu
from jax.sharding import PartitionSpec as P

lattice_dirs = [
    (0, 0, 0),
    (1, 0, 0),
    (-1, 0, 0),
    (0, 1, 0),
    (0, -1, 0),
    (0, 0, 1),
    (0, 0, -1),
    (1, 1, 0),
    (-1, -1, 0),
    (1, -1, 0),
    (-1, 1, 0),
    (1, 0, 1),
    (-1, 0, -1),
    (1, 0, -1),
    (-1, 0, 1),
    (0, 1, 1),
    (0, -1, -1),
    (0, 1, -1),
    (0, -1, 1),
]
lattice_weights = [1.0 / 3.0] + [1.0 / 18.0] * 6 + [1.0 / 36.0] * 12
opposite_of = [0, 2, 1, 4, 3, 6, 5, 8, 7, 10, 9, 12, 11, 14, 13, 16, 15, 18, 17]
relax_rate = 1.25
forward_x = [1, 7, 9, 11, 13]
backward_x = [2, 8, 10, 12, 14]
upward_y = [3, 15, 17, 7, 10]
downward_y = [4, 16, 18, 9, 8]
mark_rows = 8
kernel_memory = 16 << 20
BF = jnp.bfloat16
F32 = jnp.float32


def iota(shape, dim, dtype=F32):
    value = lax.broadcasted_iota(jnp.int32, shape, dim)
    return value if dtype == jnp.int32 else value.astype(F32).astype(dtype)


def dot_nt(a, b):
    return lax.dot_general(a, b, (((1,), (1,)), ((), ())), preferred_element_type=F32)


def dot_nn(a, b):
    return jnp.dot(a, b, preferred_element_type=F32)


def moments_of(pops):
    density = pops[0]
    moment = [None, None, None]
    for number in range(19):
        if number:
            density = density + pops[number]
        for axis in range(3):
            step = lattice_dirs[number][axis]
            if step == 0:
                continue
            if moment[axis] is None:
                moment[axis] = pops[number] if step == 1 else -pops[number]
            elif step == 1:
                moment[axis] = moment[axis] + pops[number]
            else:
                moment[axis] = moment[axis] - pops[number]
    return density, moment


def one_hot_rows(row, count, kind=BF):
    tall = jnp.broadcast_to(row, (16, row.shape[1])).astype(kind)
    one, zero = jnp.ones((), kind), jnp.zeros((), kind)
    parts = []
    for start in range(0, count, 16):
        number = iota((16, row.shape[1]), 0, F32) + float(start)
        parts.append(jnp.where(number.astype(kind) == tall, one, zero))
    return jnp.concatenate(parts, axis=0)


def fold_rows(blocks):
    row = iota(blocks[0].shape, 0, jnp.int32)
    half = 4
    while half:
        merged = []
        for s in range(half):
            a, b = blocks[s], blocks[s + half]
            merged.append(
                jnp.where(
                    (row & half) == 0,
                    a + pltpu.roll(a, 8 - half, 0),
                    b + pltpu.roll(b, half, 0),
                )
            )
        blocks = merged
        half //= 2
    return blocks[0]


def pieces_of(value):
    parts = []
    for step in range(3):
        part = value.astype(BF)
        parts.append(part)
        if step < 2:
            value = value - part.astype(F32)
    return parts


def pair_weights(list_ref, gap_ref, weight_ref):
    pairs, slots = list_ref.shape
    filler = jnp.zeros((-2 * pairs % 8, slots), F32)
    turned = jnp.transpose(
        jnp.concatenate(
            [list_ref[...].astype(F32), 1.0 / gap_ref[...], filler][: 2 + (2 * pairs % 8 > 0)],
            axis=0,
        )
    )
    column = iota((slots, slots), 1)
    weight = jnp.zeros((slots, slots), F32)
    for k in range(pairs):
        inverse = turned[:, pairs + k : pairs + k + 1]
        weight = weight + jnp.where(column == turned[:, k : k + 1], inverse, 0.0)
    high = weight.astype(BF)
    weight_ref[0] = high
    weight_ref[1] = (weight - high.astype(F32)).astype(BF)


def sample_kernel(slab_count, packed, *refs):
    sources, refs = refs[:9], refs[9:]
    slip_ref, refs = refs[0], refs[1:]
    if not packed:
        spot_ref, refs = refs[0], refs[1:]
    send_ref, sorted_ref, z_ref, y_ref, weight_ref = refs[:5]
    targets, (sems,) = refs[5:14], refs[14:]
    copies = [
        pltpu.make_async_copy(source, target, sems.at[number])
        for number, (source, target) in enumerate(zip(sources, targets))
    ]
    for copy in copies:
        copy.start()
    count_ref, table_ref, marker_count_ref, id_ref, velocity_ref, *targets = targets
    list_ref, gap_ref, cell_ref, pops_ref = targets
    slots, width = cell_ref.shape
    rows, depth = pops_ref.shape[1:]
    capacity = slots // slab_count
    for copy in copies[:5]:
        copy.wait()

    lane = iota((1, slots), 1, jnp.int32)
    alive = lane < count_ref[0]
    identity = id_ref[...]
    block = identity // slots
    spot = (identity % slots).astype(F32)

    def look_up(b, owner):
        return jnp.where(block == b, table_ref[b], owner)

    owner = lax.fori_loop(0, slab_count, look_up, jnp.zeros((1, slots), jnp.int32))
    owner = jnp.where(alive, owner, -1)
    owner_f = owner.astype(F32)
    chosen = jnp.where(iota((slab_count, slots), 0) == owner_f, 1.0, 0.0)
    before = jnp.where(
        iota((slots, slots), 0) < iota((slots, slots), 1), 1.0, 0.0
    ).astype(BF)
    earlier = dot_nn(chosen.astype(BF), before)
    position = jnp.sum(chosen * earlier, axis=0, keepdims=True)
    send_row = jnp.where(alive, owner_f * float(capacity) + position, -1.0)
    place = jnp.where(iota((slots, slots), 0) == send_row, 1.0, 0.0).astype(BF)

    where_to = jnp.where(iota((width, slots), 0) == position, 1.0, 0.0).astype(BF)
    if packed:
        taken = (iota((slab_count * mark_rows, slots), 0, jnp.int32) // mark_rows).astype(
            F32
        ) == owner_f
        marks = dot_nt(jnp.where(taken, spot + 1.0, 0.0).astype(BF), where_to)
        slip_ref[:, 3 * capacity :, :] = marks.reshape(slab_count, mark_rows, width).astype(BF)
    else:
        spot_ref[...] = dot_nt((chosen * (spot + 1.0)).astype(BF), where_to).astype(BF)

    count = marker_count_ref[...].astype(F32)
    pieces = pieces_of(jnp.concatenate([velocity_ref[c] for c in range(3)], axis=0))
    stack = jnp.concatenate(
        [piece.astype(F32) for piece in pieces] + [count, send_row, jnp.zeros((5, slots), F32)],
        axis=0,
    )
    turned = jnp.transpose(stack)
    send_ref[...] = turned[:, 8:16]
    arranged = dot_nn(place, turned.astype(BF))
    velocity = (arranged[:, 0:3] + arranged[:, 3:6]) + arranged[:, 6:9]
    sorted_ref[...] = arranged[:, 8:16]

    for copy in copies[5:7]:
        copy.wait()
    pair_weights(list_ref, gap_ref, weight_ref)
    for copy in copies[7:]:
        copy.wait()
    cells = cell_ref[...]
    parted = jnp.concatenate([(cells % depth).astype(BF), (cells // depth).astype(BF)], axis=1)
    moved = dot_nn(place, parted)
    z_ref[...] = moved[:, :width]
    y_ref[...] = moved[:, width:]

    density, moment = moments_of([pops_ref[number] for number in range(19)])
    flow = jnp.concatenate([part / density for part in moment], axis=0)
    high = flow.astype(BF)
    low = (flow - high.astype(F32)).astype(BF)
    flow_pair = jnp.concatenate([high, low], axis=1)

    for base in range(0, slots, 16):
        found_rows = []
        for eight in range(base, base + 16, 8):
            z_rows = z_ref[eight : eight + 8, :]
            y_rows = y_ref[eight : eight + 8, :]
            parts = [[], [], []]
            for first in range(0, 8, 2):
                picks = jnp.concatenate(
                    [one_hot_rows(z_rows[s : s + 1], depth) for s in (first, first + 1)], axis=1
                )
                picked = dot_nn(flow_pair, jnp.concatenate([picks, picks], axis=0))
                for s in (first, first + 1):
                    cut = slice((s - first) * width, (s - first + 1) * width)
                    tall = jnp.broadcast_to(y_rows[s : s + 1], (8, width))
                    found = [jnp.zeros((8, width), F32)] * 3
                    for start in range(0, rows, 8):
                        mask = iota((8, width), 0) + float(start) == tall
                        for c in range(3):
                            at = c * rows + start
                            found[c] = jnp.where(mask, picked[at : at + 8, cut], found[c])
                    for c in range(3):
                        parts[c].append(found[c])
            found_rows.append([fold_rows(parts[c]) for c in range(3)])
        live = iota((16, width), 1) < arranged[base : base + 16, 9:10]
        for c in range(3):
            sampled = jnp.concatenate([found_rows[0][c], found_rows[1][c]], axis=0)
            slip = jnp.where(live, velocity[base : base + 16, c : c + 1] - sampled, 0.0)
            if packed:
                at = c * capacity + base % capacity
                slip_ref[base // capacity, at : at + 16, :] = slip.astype(BF)
            else:
                slip_ref[c, base : base + 16, :] = slip.astype(BF)


def owner_kernel(
    slab_count,
    packed,
    *refs,
):
    if packed:
        got_ref, weight_ref, self_ref, pair_ref, out_ref = refs
        width = got_ref.shape[2]
        slots = weight_ref.shape[1]
        capacity = slots // slab_count
        got = jnp.concatenate(
            [
                got_ref[:, c * capacity : (c + 1) * capacity, :].reshape(slots, width)
                for c in range(3)
            ],
            axis=1,
        )
        per_tile = width // capacity
        lane = iota((8, width), 1, jnp.int32)
        tiles = []
        for start in range(0, slab_count, per_tile):
            total = jnp.zeros((8, width), F32)
            for source in range(start, min(start + per_tile, slab_count)):
                mark = got_ref[source, 3 * capacity : 3 * capacity + mark_rows, :].astype(F32)
                off = (source - start) * capacity
                if off:
                    mark = pltpu.roll(mark, off, 1)
                mine = (lane >= off) & (lane < off + capacity)
                total = jnp.where(mine, mark, total)
            tiles.append(total)
        spots = jnp.concatenate(tiles, axis=1) - 1.0
    else:
        got_ref, spot_ref, weight_ref, self_ref, pair_ref, out_ref = refs
        width = got_ref.shape[2]
        slots = weight_ref.shape[1]
        got = jnp.concatenate([got_ref[c] for c in range(3)], axis=1)
        spots = jnp.broadcast_to(spot_ref[...].astype(F32), (8, slots)) - 1.0

    spot_row = spots[:1]
    spot_col = jnp.transpose(spots)[:, :1]
    land = jnp.where(iota((slots, slots), 0) == spot_row, 1.0, 0.0).astype(BF)
    reply = jnp.where(iota((slots, slots), 1) == spot_col, 1.0, 0.0).astype(BF)
    owned = dot_nn(land, got).astype(BF)
    near = (dot_nn(weight_ref[0], owned) + dot_nn(weight_ref[1], owned)).astype(BF)
    coupling = jnp.concatenate([self_ref[...], pair_ref[...]], axis=0)
    fixed = []
    for c in range(3):
        cut = slice(c * width, (c + 1) * width)
        both = jnp.concatenate([owned[:, cut], near[:, cut]], axis=1)
        fixed.append(dot_nn(both, coupling).astype(BF))
    replies = dot_nn(reply, jnp.concatenate(fixed, axis=1)).astype(BF)
    for c in range(3):
        cut = replies[:, c * width : (c + 1) * width]
        if packed:
            out_ref[:, c * capacity : (c + 1) * capacity, :] = cut.reshape(
                slab_count, capacity, width
            )
        else:
            out_ref[c] = cut


def returned_rows(slab_count, packed, back_ref, sorted_ref, base, count):
    if packed:
        capacity = sorted_ref.shape[0] // slab_count
        at, block = base % capacity, slice(base // capacity, (base + count - 1) // capacity + 1)
        take = min(count, capacity)
        parts = [
            back_ref[block, c * capacity + at : c * capacity + at + take, :].reshape(count, -1)
            for c in range(3)
        ]
    else:
        parts = [back_ref[c, base : base + count, :] for c in range(3)]
    live = iota(parts[0].shape, 1) < sorted_ref[base : base + count, 1:2]
    return [jnp.where(live, part.astype(F32), 0.0) for part in parts]


def finish_kernel(slab_count, packed, back_ref, sorted_ref, send_ref, out_ref):
    slots = sorted_ref.shape[0]
    masked = returned_rows(slab_count, packed, back_ref, sorted_ref, 0, slots)
    fetch = jnp.where(iota((slots, slots), 1) == send_ref[:, 2:3], 1.0, 0.0).astype(BF)
    for c in range(3):
        out_ref[c] = dot_nn(fetch, masked[c].astype(BF)).astype(BF)


def spread_kernel(
    slab_count,
    packed,
    back_ref,
    sorted_ref,
    z_ref,
    y_ref,
    pops_ref,
    collided_ref,
    up_ref,
    down_ref,
    first_ref,
    second_ref,
):
    slots, width = z_ref.shape
    rows, depth = pops_ref.shape[1:]
    picks, terms = [], []
    for base in range(0, slots, 16):
        f_rows = returned_rows(slab_count, packed, back_ref, sorted_ref, base, 16)
        z_rows = z_ref[base : base + 16, :]
        y_rows = y_ref[base : base + 16, :]
        for s in range(16):
            picks.append(one_hot_rows(z_rows[s : s + 1], depth))
            tall = jnp.broadcast_to(y_rows[s : s + 1], (16, width)).astype(BF)
            parts = []
            for c in range(3):
                value = jnp.broadcast_to(f_rows[c][s : s + 1], (16, width)).astype(BF)
                for start in range(0, rows, 16):
                    number = (iota((16, width), 0) + float(start)).astype(BF)
                    parts.append(jnp.where(number == tall, value, jnp.zeros((), BF)))
            terms.append(jnp.concatenate(parts, axis=0))
    total = dot_nt(jnp.concatenate(terms, axis=1), jnp.concatenate(picks, axis=1))

    force = [total[c * rows : (c + 1) * rows] for c in range(3)]
    pops = [pops_ref[number] for number in range(19)]
    density, moment = moments_of(pops)
    velocity = [(moment[c] + 0.5 * force[c]) / density for c in range(3)]
    speed_sq = velocity[0] * velocity[0] + velocity[1] * velocity[1] + velocity[2] * velocity[2]
    work_rate = velocity[0] * force[0] + velocity[1] * force[1] + velocity[2] * force[2]
    base_term = 1.0 - 1.5 * speed_sq
    even = (lax.axis_index("slab") & 1) == 0
    sent = {}
    for number in range(19):
        step = lattice_dirs[number]
        along, push = None, None
        for c in range(3):
            if step[c] == 0:
                continue
            v, f = (velocity[c], force[c]) if step[c] == 1 else (-velocity[c], -force[c])
            along = v if along is None else along + v
            push = f if push is None else push + f
        weight = lattice_weights[number]
        if along is None:
            equilibrium = weight * density * base_term
            source = ((1.0 - 0.5 * relax_rate) * weight * -3.0) * work_rate
        else:
            equilibrium = weight * density * (base_term + 3.0 * along + 4.5 * along * along)
            source = ((1.0 - 0.5 * relax_rate) * weight) * (
                3.0 * (push - work_rate) + 9.0 * along * push
            )
        value = pops[number] - relax_rate * (pops[number] - equilibrium) + source
        collided_ref[number] = value
        if step[0] != 0:
            sent.setdefault((forward_x if step[0] == 1 else backward_x).index(number), {})[
                step[0]
            ] = value
        if number in upward_y[:3]:
            at = upward_y.index(number)
            up_ref[at : at + 1, :] = value[rows - 1 :]
        if number in downward_y[:3]:
            at = downward_y.index(number)
            down_ref[at : at + 1, :] = value[:1]
    for at, pair in sent.items():
        first_ref[at] = jnp.where(even, pair[1], pair[-1]).astype(BF)
        second_ref[at] = jnp.where(even, pair[-1], pair[1]).astype(BF)
    up_ref[3:, :] = jnp.zeros((5, depth), F32)
    down_ref[3:, :] = jnp.zeros((5, depth), F32)


def stream_kernel(
    sub_total, collided_ref, one_ref, two_ref, first_ref, second_ref, read_ref
):
    rows, depth = collided_ref.shape[1:]
    row = iota((rows, depth), 0, jnp.int32)
    place = lax.axis_index("sub")
    slab_even = (lax.axis_index("slab") & 1) == 0
    sub_even = (place & 1) == 0
    low = jnp.where(sub_even, two_ref[...], one_ref[...])
    high = jnp.where(sub_even, one_ref[...], two_ref[...])
    low_wall = jnp.where(place == 0, 1, 0)
    high_wall = jnp.where(place == sub_total - 1, 1, 0)
    for number in range(19):
        step_x, step_y, step_z = lattice_dirs[number]
        if step_x == 1:
            at = forward_x.index(number)
            moved = jnp.where(slab_even, second_ref[at].astype(F32), first_ref[at].astype(F32))
        elif step_x == -1:
            at = backward_x.index(number)
            moved = jnp.where(slab_even, first_ref[at].astype(F32), second_ref[at].astype(F32))
        else:
            moved = collided_ref[number]
        if step_y != 0:
            rolled = pltpu.roll(moved, 1 if step_y == 1 else rows - 1, 0)
            edge_row = 0 if step_y == 1 else rows - 1
            at = (upward_y if step_y == 1 else downward_y).index(number)
            edge = (low if step_y == 1 else high)[at : at + 1]
            moved = jnp.where(row == edge_row, edge, rolled)
        if step_z != 0:
            moved = pltpu.roll(moved, 1 if step_z == 1 else depth - 1, 1)
        if step_y != 0:
            wall = low_wall if step_y == 1 else high_wall
            at_wall = (row == edge_row) & (wall == 1)
            moved = jnp.where(at_wall, collided_ref[opposite_of[number]], moved)
        read_ref[number] = moved


def whole(memory=pltpu.VMEM):
    return pl.BlockSpec(memory_space=memory)


def swap(value, axis, odd):
    count = lax.axis_size(axis)
    pairs = [(i, (i + 1 if i % 2 == odd else i - 1) % count) for i in range(count)]
    return lax.ppermute(value, axis, pairs)


def per_device(
    populations,
    marker_cell,
    marker_count,
    particle_count,
    particle_id,
    owner_table,
    particle_velocity,
    pair_list,
    pair_gap,
    self_coupling,
    pair_coupling,
):
    slab_count = lax.axis_size("slab")
    slots, width = marker_cell.shape[2:]
    planes, rows, depth = populations.shape[1:]
    assert planes == 1 and slots <= 256 and slots % slab_count == 0
    assert slab_count % 2 == 0 and lax.axis_size("sub") % 2 == 0
    capacity = slots // slab_count
    assert capacity <= width
    packed = capacity % 16 == 0 and width % capacity == 0
    pops = populations.reshape(19, rows, depth)
    cells = marker_cell.reshape(slots, width)
    shape = jax.ShapeDtypeStruct
    limits = pltpu.CompilerParams(vmem_limit_bytes=kernel_memory)

    if packed:
        sample_out = [shape((slab_count, 3 * capacity + mark_rows, width), BF)]
    else:
        sample_out = [shape((3, slots, width), BF), shape((slab_count, width), BF)]
    sample_out += [shape((slots, 8), F32)] * 2 + [shape((slots, width), F32)] * 2
    sample_out.append(shape((2, slots, slots), BF))
    results = pl.pallas_call(
        functools.partial(sample_kernel, slab_count, packed),
        out_shape=sample_out,
        in_specs=[whole(pltpu.HBM)] * 9,
        out_specs=[whole()] * len(sample_out),
        scratch_shapes=[
            pltpu.SMEM((1,), jnp.int32),
            pltpu.SMEM((slab_count,), jnp.int32),
            pltpu.VMEM((1, slots), jnp.int32),
            pltpu.VMEM((1, slots), jnp.int32),
            pltpu.VMEM((3, 1, slots), F32),
            pltpu.VMEM((pair_list.shape[3], slots), jnp.int32),
            pltpu.VMEM((pair_list.shape[3], slots), F32),
            pltpu.VMEM((slots, width), jnp.int32),
            pltpu.VMEM((19, rows, depth), F32),
            pltpu.SemaphoreType.DMA((9,)),
        ],
        compiler_params=limits,
        name="sample",
    )(
        particle_count.reshape(1),
        *[
            pltpu.with_memory_space_constraint(value, pltpu.HBM)
            for value in (
                owner_table.reshape(slab_count),
                marker_count.reshape(1, slots),
                particle_id.reshape(1, slots),
                particle_velocity.reshape(3, 1, slots),
                jnp.transpose(pair_list.reshape(slots, -1)),
                jnp.transpose(pair_gap.reshape(slots, -1)),
                cells,
                pops,
            )
        ],
    )
    send, ordered, z_cells, y_cells, weights = results[-5:]

    def exchange(value):
        return lax.all_to_all(value, "slab", split_axis=0, concat_axis=0, tiled=True)

    def by_owner(value):
        value = value.reshape(3, slab_count, capacity, width)
        return jnp.transpose(value, (1, 0, 2, 3)).reshape(slab_count, 3 * capacity, width)

    def by_component(value):
        value = value.reshape(slab_count, 3, capacity, width)
        return jnp.transpose(value, (1, 0, 2, 3)).reshape(3, slots, width)

    if packed:
        arrived = [exchange(results[0])]
        reply_shape = shape((slab_count, 3 * capacity, width), BF)
    else:
        slip = jnp.concatenate([by_owner(results[0]), results[1][:, None, :]], axis=1)
        got = exchange(slip)
        arrived = [
            by_component(got[:, : 3 * capacity]),
            got[:, 3 * capacity, :capacity].reshape(1, slots),
        ]
        reply_shape = shape((3, slots, width), BF)
    reply = pl.pallas_call(
        functools.partial(owner_kernel, slab_count, packed),
        out_shape=reply_shape,
        in_specs=[whole()] * (len(arrived) + 3),
        out_specs=whole(),
        compiler_params=limits,
        name="owner",
    )(
        *arrived,
        weights,
        self_coupling,
        pair_coupling,
    )
    back = exchange(reply) if packed else by_component(exchange(by_owner(reply)))

    collided, up, down, first, second = pl.pallas_call(
        functools.partial(spread_kernel, slab_count, packed),
        out_shape=[
            shape((19, rows, depth), F32),
            shape((8, depth), F32),
            shape((8, depth), F32),
            shape((5, rows, depth), BF),
            shape((5, rows, depth), BF),
        ],
        in_specs=[whole()] * 5,
        out_specs=[whole()] * 5,
        compiler_params=limits,
        name="spread",
    )(back, ordered, z_cells, y_cells, pops)
    marker_force = pl.pallas_call(
        functools.partial(finish_kernel, slab_count, packed),
        out_shape=shape((3, slots, width), BF),
        in_specs=[whole()] * 3,
        out_specs=whole(),
        compiler_params=limits,
        cost_estimate=pl.CostEstimate(flops=50_000_000, bytes_accessed=400_000, transcendentals=0),
        name="finish",
    )(back, ordered, send)

    slab_even = (lax.axis_index("slab") & 1) == 0
    sub_even = (lax.axis_index("sub") & 1) == 0
    first, second = swap(first, "slab", 0), swap(second, "slab", 1)
    top, bottom = slice(rows - 1, rows), slice(0, 1)
    one_up = jnp.where(slab_even, second[1, top], first[1, top])
    two_up = jnp.where(slab_even, first[2, top], second[2, top])
    one_down = jnp.where(slab_even, second[2, bottom], first[2, bottom])
    two_down = jnp.where(slab_even, first[1, bottom], second[1, bottom])
    up = jnp.concatenate([up[:3], one_up.astype(F32), two_up.astype(F32)])
    down = jnp.concatenate([down[:3], one_down.astype(F32), two_down.astype(F32)])
    low_high = (
        swap(jnp.where(sub_even, up, down), "sub", 0),
        swap(jnp.where(sub_even, down, up), "sub", 1),
    )
    read = pl.pallas_call(
        functools.partial(stream_kernel, lax.axis_size("sub")),
        out_shape=shape((19, rows, depth), F32),
        in_specs=[whole()] * 5,
        out_specs=whole(),
        compiler_params=limits,
        name="stream",
    )(collided, *low_high, first, second)
    marker_force = jnp.transpose(marker_force, (1, 0, 2))[None, None]
    return (read.reshape(19, 1, rows, depth), marker_force)


def solution(mesh):
    placed = (
        P(None, "slab", "sub", None),
        P("slab", "sub", None, None),
        P("slab", "sub", None),
        P("slab", "sub"),
        P("slab", "sub", None),
        P("sub", None),
        P("slab", "sub", None, None),
        P("slab", "sub", None, None),
        P("slab", "sub", None, None),
        P(),
        P(),
    )
    return jax.shard_map(
        per_device,
        mesh=mesh,
        in_specs=placed,
        out_specs=(P(None, "slab", "sub", None), P("slab", "sub", None, None, None)),
        check_vma=False,
    )
```

```python
import functools
import math

import jax
import jax.numpy as jnp
from jax import lax
from jax.experimental import pallas as pl
from jax.experimental.pallas import tpu as pltpu
from jax.sharding import PartitionSpec as P

lattice_dirs = [
    (0, 0, 0),
    (1, 0, 0),
    (-1, 0, 0),
    (0, 1, 0),
    (0, -1, 0),
    (0, 0, 1),
    (0, 0, -1),
    (1, 1, 0),
    (-1, -1, 0),
    (1, -1, 0),
    (-1, 1, 0),
    (1, 0, 1),
    (-1, 0, -1),
    (1, 0, -1),
    (-1, 0, 1),
    (0, 1, 1),
    (0, -1, -1),
    (0, 1, -1),
    (0, -1, 1),
]
lattice_weights = [1.0 / 3.0] + [1.0 / 18.0] * 6 + [1.0 / 36.0] * 12
opposite_of = [0, 2, 1, 4, 3, 6, 5, 8, 7, 10, 9, 12, 11, 14, 13, 16, 15, 18, 17]
relax_rate = 1.25
forward_x = [1, 7, 9, 11, 13]
backward_x = [2, 8, 10, 12, 14]
upward_y = [3, 15, 17, 7, 10]
downward_y = [4, 16, 18, 9, 8]
mark_rows = 8
kernel_memory = 16 << 20
BF = jnp.bfloat16
F32 = jnp.float32
PICK = jnp.float8_e4m3fn


def iota(shape, dim, dtype=F32):
    value = lax.broadcasted_iota(jnp.int32, shape, dim)
    return value if dtype == jnp.int32 else value.astype(F32).astype(dtype)


def dot_nt(a, b):
    return lax.dot_general(a, b, (((1,), (1,)), ((), ())), preferred_element_type=F32)


def dot_nn(a, b):
    return jnp.dot(a, b, preferred_element_type=F32)


def moments_of(pops):
    density = pops[0]
    moment = [None, None, None]
    for number in range(19):
        if number:
            density = density + pops[number]
        for axis in range(3):
            step = lattice_dirs[number][axis]
            if step == 0:
                continue
            if moment[axis] is None:
                moment[axis] = pops[number] if step == 1 else -pops[number]
            elif step == 1:
                moment[axis] = moment[axis] + pops[number]
            else:
                moment[axis] = moment[axis] - pops[number]
    return density, moment


def one_hot_rows(row, count):
    tile = (32, row.shape[1])
    tall = jnp.broadcast_to(row, tile).astype(BF)
    one, zero = jnp.ones(tile, F32).astype(PICK), jnp.zeros(tile, F32).astype(PICK)
    parts = []
    for start in range(0, count, 32):
        number = (iota(tile, 0) + float(start)).astype(BF)
        parts.append(jnp.where(number == tall, one, zero))
    return jnp.concatenate(parts, axis=0)


def fold_rows(blocks):
    row = iota(blocks[0].shape, 0, jnp.int32)
    half = 4
    while half:
        merged = []
        for s in range(half):
            a, b = blocks[s], blocks[s + half]
            merged.append(
                jnp.where(
                    (row & half) == 0,
                    a + pltpu.roll(a, 8 - half, 0),
                    b + pltpu.roll(b, half, 0),
                )
            )
        blocks = merged
        half //= 2
    return blocks[0]


def pieces_of(value):
    parts = []
    for step in range(3):
        part = value.astype(BF)
        parts.append(part)
        if step < 2:
            value = value - part.astype(F32)
    return parts


def pair_weights(list_ref, gap_ref):
    pairs, slots = list_ref.shape
    filler = jnp.zeros((-2 * pairs % 8, slots), F32)
    turned = jnp.transpose(
        jnp.concatenate(
            [list_ref[...].astype(F32), 1.0 / gap_ref[...], filler][: 2 + (2 * pairs % 8 > 0)],
            axis=0,
        )
    )
    column = iota((slots, slots), 1)
    weight = jnp.zeros((slots, slots), F32)
    for k in range(pairs):
        inverse = turned[:, pairs + k : pairs + k + 1]
        weight = weight + jnp.where(column == turned[:, k : k + 1], inverse, 0.0)
    high = weight.astype(BF)
    return jnp.concatenate([high, (weight - high.astype(F32)).astype(BF)], axis=1)


def sample_kernel(slab_count, packed, *refs):
    sources, refs = refs[:7], refs[7:]
    slip_ref, refs = refs[0], refs[1:]
    if not packed:
        spot_ref, refs = refs[0], refs[1:]
    send_ref, sorted_ref, z_ref, y_ref = refs[:4]
    targets, (sems,) = refs[4:11], refs[11:]
    copies = [
        pltpu.make_async_copy(source, target, sems.at[number])
        for number, (source, target) in enumerate(zip(sources, targets))
    ]
    for copy in copies:
        copy.start()
    count_ref, table_ref, marker_count_ref, id_ref, velocity_ref, cell_ref, pops_ref = targets
    slots, width = cell_ref.shape
    rows, depth = pops_ref.shape[1:]
    capacity = slots // slab_count
    for copy in copies[:5]:
        copy.wait()

    lane = iota((1, slots), 1, jnp.int32)
    alive = lane < count_ref[0]
    identity = id_ref[...]
    block = identity // slots
    spot = (identity % slots).astype(F32)

    def look_up(b, owner):
        return jnp.where(block == b, table_ref[b], owner)

    owner = lax.fori_loop(0, slab_count, look_up, jnp.zeros((1, slots), jnp.int32))
    owner = jnp.where(alive, owner, -1)
    owner_f = owner.astype(F32)
    chosen = jnp.where(iota((slab_count, slots), 0) == owner_f, 1.0, 0.0)
    before = jnp.where(
        iota((slots, slots), 0) < iota((slots, slots), 1), 1.0, 0.0
    ).astype(BF)
    earlier = dot_nn(chosen.astype(BF), before)
    position = jnp.sum(chosen * earlier, axis=0, keepdims=True)
    send_row = jnp.where(alive, owner_f * float(capacity) + position, -1.0)
    place = jnp.where(iota((slots, slots), 0) == send_row, 1.0, 0.0).astype(BF)

    where_to = jnp.where(iota((width, slots), 0) == position, 1.0, 0.0).astype(BF)
    if packed:
        taken = (iota((slab_count * mark_rows, slots), 0, jnp.int32) // mark_rows).astype(
            F32
        ) == owner_f
        marks = dot_nt(jnp.where(taken, spot + 1.0, 0.0).astype(BF), where_to)
        slip_ref[:, 3 * capacity :, :] = marks.reshape(slab_count, mark_rows, width).astype(BF)
    else:
        spot_ref[...] = dot_nt((chosen * (spot + 1.0)).astype(BF), where_to).astype(BF)

    count = marker_count_ref[...].astype(F32)
    pieces = pieces_of(jnp.concatenate([velocity_ref[c] for c in range(3)], axis=0))
    stack = jnp.concatenate(
        [piece.astype(F32) for piece in pieces] + [count, send_row, jnp.zeros((5, slots), F32)],
        axis=0,
    )
    turned = jnp.transpose(stack)
    send_ref[...] = turned[:, 8:16]
    arranged = dot_nn(place, turned.astype(BF))
    velocity = (arranged[:, 0:3] + arranged[:, 3:6]) + arranged[:, 6:9]
    sorted_ref[...] = arranged[:, 8:16]

    for copy in copies[5:]:
        copy.wait()
    cells = cell_ref[...]
    parted = jnp.concatenate([(cells % depth).astype(BF), (cells // depth).astype(BF)], axis=1)
    moved = dot_nn(place, parted)
    z_ref[...] = moved[:, :width]
    y_ref[...] = moved[:, width:]

    density, moment = moments_of([pops_ref[number] for number in range(19)])
    flow = jnp.concatenate([part / density for part in moment], axis=0)
    high = flow.astype(BF)
    low = (flow - high.astype(F32)).astype(BF)
    flow_pair = jnp.concatenate([high, low], axis=1)

    for base in range(0, slots, 16):
        found_rows = []
        for eight in range(base, base + 16, 8):
            z_rows = z_ref[eight : eight + 8, :]
            y_rows = y_ref[eight : eight + 8, :]
            parts = [[], [], []]
            for first in range(0, 8, 2):
                picks = jnp.concatenate(
                    [one_hot_rows(z_rows[s : s + 1], depth) for s in (first, first + 1)], axis=1
                )
                picked = dot_nn(flow_pair, jnp.concatenate([picks, picks], axis=0))
                for s in (first, first + 1):
                    cut = slice((s - first) * width, (s - first + 1) * width)
                    tall = jnp.broadcast_to(y_rows[s : s + 1], (8, width))
                    found = [jnp.zeros((8, width), F32)] * 3
                    for start in range(0, rows, 8):
                        mask = iota((8, width), 0) + float(start) == tall
                        for c in range(3):
                            at = c * rows + start
                            found[c] = jnp.where(mask, picked[at : at + 8, cut], found[c])
                    for c in range(3):
                        parts[c].append(found[c])
            found_rows.append([fold_rows(parts[c]) for c in range(3)])
        live = iota((16, width), 1) < arranged[base : base + 16, 9:10]
        for c in range(3):
            sampled = jnp.concatenate([found_rows[0][c], found_rows[1][c]], axis=0)
            slip = jnp.where(live, velocity[base : base + 16, c : c + 1] - sampled, 0.0)
            if packed:
                at = c * capacity + base % capacity
                slip_ref[base // capacity, at : at + 16, :] = slip.astype(BF)
            else:
                slip_ref[c, base : base + 16, :] = slip.astype(BF)


def owner_kernel(
    slab_count,
    packed,
    *refs,
):
    if packed:
        got_ref, list_ref, gap_ref, self_ref, pair_ref, out_ref = refs
        width = got_ref.shape[2]
        slots = list_ref.shape[1]
        capacity = slots // slab_count
        got = jnp.concatenate(
            [
                got_ref[:, c * capacity : (c + 1) * capacity, :].reshape(slots, width)
                for c in range(3)
            ],
            axis=1,
        )
        per_tile = width // capacity
        lane = iota((8, width), 1, jnp.int32)
        tiles = []
        for start in range(0, slab_count, per_tile):
            total = jnp.zeros((8, width), F32)
            for source in range(start, min(start + per_tile, slab_count)):
                mark = got_ref[source, 3 * capacity : 3 * capacity + mark_rows, :].astype(F32)
                off = (source - start) * capacity
                if off:
                    mark = pltpu.roll(mark, off, 1)
                mine = (lane >= off) & (lane < off + capacity)
                total = jnp.where(mine, mark, total)
            tiles.append(total)
        spots = jnp.concatenate(tiles, axis=1) - 1.0
    else:
        got_ref, spot_ref, list_ref, gap_ref, self_ref, pair_ref, out_ref = refs
        width = got_ref.shape[2]
        slots = list_ref.shape[1]
        got = jnp.concatenate([got_ref[c] for c in range(3)], axis=1)
        spots = jnp.broadcast_to(spot_ref[...].astype(F32), (8, slots)) - 1.0

    spot_row = spots[:1]
    spot_col = jnp.transpose(spots)[:, :1]
    land = jnp.where(iota((slots, slots), 0) == spot_row, 1.0, 0.0).astype(BF)
    reply = jnp.where(iota((slots, slots), 1) == spot_col, 1.0, 0.0).astype(BF)
    chosen = dot_nn(reply, pair_weights(list_ref, gap_ref)).astype(BF)
    owned = dot_nn(land, got).astype(BF)
    near = (dot_nn(chosen[:, :slots], owned) + dot_nn(chosen[:, slots:], owned)).astype(BF)
    coupling = jnp.concatenate([self_ref[...], pair_ref[...]], axis=0)
    for c in range(3):
        span = slice(c * width, (c + 1) * width)
        both = jnp.concatenate([got[:, span], near[:, span]], axis=1)
        cut = dot_nn(both, coupling).astype(BF)
        if packed:
            out_ref[:, c * capacity : (c + 1) * capacity, :] = cut.reshape(
                slab_count, capacity, width
            )
        else:
            out_ref[c] = cut


def returned_rows(slab_count, packed, back_ref, sorted_ref, base, count):
    if packed:
        capacity = sorted_ref.shape[0] // slab_count
        at, block = base % capacity, slice(base // capacity, (base + count - 1) // capacity + 1)
        take = min(count, capacity)
        parts = [
            back_ref[block, c * capacity + at : c * capacity + at + take, :].reshape(count, -1)
            for c in range(3)
        ]
    else:
        parts = [back_ref[c, base : base + count, :] for c in range(3)]
    live = iota(parts[0].shape, 1) < sorted_ref[base : base + count, 1:2]
    return [jnp.where(live, part.astype(F32), 0.0) for part in parts]


def finish_kernel(slab_count, packed, back_ref, sorted_ref, send_ref, out_ref):
    slots = sorted_ref.shape[0]
    masked = returned_rows(slab_count, packed, back_ref, sorted_ref, 0, slots)
    fetch = jnp.where(iota((slots, slots), 1) == send_ref[:, 2:3], 1.0, 0.0).astype(BF)
    for c in range(3):
        out_ref[c] = dot_nn(fetch, masked[c].astype(BF)).astype(BF)


def spread_kernel(
    slab_count,
    packed,
    back_ref,
    sorted_ref,
    z_ref,
    y_ref,
    pops_ref,
    collided_ref,
    up_ref,
    down_ref,
    first_ref,
    second_ref,
):
    slots, width = z_ref.shape
    rows, depth = pops_ref.shape[1:]
    picks, terms = [], []
    for base in range(0, slots, 16):
        f_rows = returned_rows(slab_count, packed, back_ref, sorted_ref, base, 16)
        z_rows = z_ref[base : base + 16, :]
        y_rows = y_ref[base : base + 16, :]
        for s in range(16):
            picks.append(one_hot_rows(z_rows[s : s + 1], depth))
            tall = jnp.broadcast_to(y_rows[s : s + 1], (16, width)).astype(BF)
            parts = []
            for c in range(3):
                value = jnp.broadcast_to(f_rows[c][s : s + 1], (16, width)).astype(BF)
                for start in range(0, rows, 16):
                    number = (iota((16, width), 0) + float(start)).astype(BF)
                    parts.append(jnp.where(number == tall, value, jnp.zeros((), BF)))
            terms.append(jnp.concatenate(parts, axis=0))
    total = dot_nt(jnp.concatenate(terms, axis=1), jnp.concatenate(picks, axis=1))

    force = [total[c * rows : (c + 1) * rows] for c in range(3)]
    pops = [pops_ref[number] for number in range(19)]
    density, moment = moments_of(pops)
    velocity = [(moment[c] + 0.5 * force[c]) / density for c in range(3)]
    speed_sq = velocity[0] * velocity[0] + velocity[1] * velocity[1] + velocity[2] * velocity[2]
    work_rate = velocity[0] * force[0] + velocity[1] * force[1] + velocity[2] * force[2]
    base_term = 1.0 - 1.5 * speed_sq
    even = (lax.axis_index("slab") & 1) == 0
    sent = {}
    for number in range(19):
        step = lattice_dirs[number]
        along, push = None, None
        for c in range(3):
            if step[c] == 0:
                continue
            v, f = (velocity[c], force[c]) if step[c] == 1 else (-velocity[c], -force[c])
            along = v if along is None else along + v
            push = f if push is None else push + f
        weight = lattice_weights[number]
        if along is None:
            equilibrium = weight * density * base_term
            source = ((1.0 - 0.5 * relax_rate) * weight * -3.0) * work_rate
        else:
            equilibrium = weight * density * (base_term + 3.0 * along + 4.5 * along * along)
            source = ((1.0 - 0.5 * relax_rate) * weight) * (
                3.0 * (push - work_rate) + 9.0 * along * push
            )
        value = pops[number] - relax_rate * (pops[number] - equilibrium) + source
        collided_ref[number] = value
        if step[0] != 0:
            sent.setdefault((forward_x if step[0] == 1 else backward_x).index(number), {})[
                step[0]
            ] = value
        if number in upward_y[:3]:
            at = upward_y.index(number)
            up_ref[at : at + 1, :] = value[rows - 1 :]
        if number in downward_y[:3]:
            at = downward_y.index(number)
            down_ref[at : at + 1, :] = value[:1]
    for at, pair in sent.items():
        first_ref[at] = jnp.where(even, pair[1], pair[-1]).astype(BF)
        second_ref[at] = jnp.where(even, pair[-1], pair[1]).astype(BF)
    up_ref[3:, :] = jnp.zeros((5, depth), F32)
    down_ref[3:, :] = jnp.zeros((5, depth), F32)


def stream_kernel(
    sub_total, collided_ref, one_ref, two_ref, first_ref, second_ref, read_ref
):
    rows, depth = collided_ref.shape[1:]
    row = iota((rows, depth), 0, jnp.int32)
    place = lax.axis_index("sub")
    slab_even = (lax.axis_index("slab") & 1) == 0
    sub_even = (place & 1) == 0
    low = jnp.where(sub_even, two_ref[...], one_ref[...])
    high = jnp.where(sub_even, one_ref[...], two_ref[...])
    low_wall = jnp.where(place == 0, 1, 0)
    high_wall = jnp.where(place == sub_total - 1, 1, 0)
    for number in range(19):
        step_x, step_y, step_z = lattice_dirs[number]
        if step_x == 1:
            at = forward_x.index(number)
            moved = jnp.where(slab_even, second_ref[at].astype(F32), first_ref[at].astype(F32))
        elif step_x == -1:
            at = backward_x.index(number)
            moved = jnp.where(slab_even, first_ref[at].astype(F32), second_ref[at].astype(F32))
        else:
            moved = collided_ref[number]
        if step_y != 0:
            rolled = pltpu.roll(moved, 1 if step_y == 1 else rows - 1, 0)
            edge_row = 0 if step_y == 1 else rows - 1
            at = (upward_y if step_y == 1 else downward_y).index(number)
            edge = (low if step_y == 1 else high)[at : at + 1]
            moved = jnp.where(row == edge_row, edge, rolled)
        if step_z != 0:
            moved = pltpu.roll(moved, 1 if step_z == 1 else depth - 1, 1)
        if step_y != 0:
            wall = low_wall if step_y == 1 else high_wall
            at_wall = (row == edge_row) & (wall == 1)
            moved = jnp.where(at_wall, collided_ref[opposite_of[number]], moved)
        read_ref[number] = moved


def whole(memory=pltpu.VMEM):
    return pl.BlockSpec(memory_space=memory)


def swap(value, axis, odd):
    count = lax.axis_size(axis)
    pairs = [(i, (i + 1 if i % 2 == odd else i - 1) % count) for i in range(count)]
    return lax.ppermute(value, axis, pairs)


def per_device(
    populations,
    marker_cell,
    marker_count,
    particle_count,
    particle_id,
    owner_table,
    particle_velocity,
    pair_list,
    pair_gap,
    self_coupling,
    pair_coupling,
):
    slab_count = lax.axis_size("slab")
    slots, width = marker_cell.shape[2:]
    planes, rows, depth = populations.shape[1:]
    assert planes == 1 and slots <= 256 and slots % slab_count == 0
    assert slab_count % 2 == 0 and lax.axis_size("sub") % 2 == 0
    capacity = slots // slab_count
    assert capacity <= width
    packed = capacity % 16 == 0 and width % capacity == 0
    pops = populations.reshape(19, rows, depth)
    cells = marker_cell.reshape(slots, width)
    shape = jax.ShapeDtypeStruct
    limits = pltpu.CompilerParams(vmem_limit_bytes=kernel_memory)

    if packed:
        sample_out = [shape((slab_count, 3 * capacity + mark_rows, width), BF)]
    else:
        sample_out = [shape((3, slots, width), BF), shape((slab_count, width), BF)]
    sample_out += [shape((slots, 8), F32)] * 2 + [shape((slots, width), F32)] * 2
    results = pl.pallas_call(
        functools.partial(sample_kernel, slab_count, packed),
        out_shape=sample_out,
        in_specs=[whole(pltpu.HBM)] * 7,
        out_specs=[whole()] * len(sample_out),
        scratch_shapes=[
            pltpu.SMEM((1,), jnp.int32),
            pltpu.SMEM((slab_count,), jnp.int32),
            pltpu.VMEM((1, slots), jnp.int32),
            pltpu.VMEM((1, slots), jnp.int32),
            pltpu.VMEM((3, 1, slots), F32),
            pltpu.VMEM((slots, width), jnp.int32),
            pltpu.VMEM((19, rows, depth), F32),
            pltpu.SemaphoreType.DMA((7,)),
        ],
        compiler_params=limits,
        name="sample",
    )(
        particle_count.reshape(1),
        *[
            pltpu.with_memory_space_constraint(value, pltpu.HBM)
            for value in (
                owner_table.reshape(slab_count),
                marker_count.reshape(1, slots),
                particle_id.reshape(1, slots),
                particle_velocity.reshape(3, 1, slots),
                cells,
                pops,
            )
        ],
    )
    send, ordered, z_cells, y_cells = results[-4:]

    def exchange(value):
        return lax.all_to_all(value, "slab", split_axis=0, concat_axis=0, tiled=True)

    def by_owner(value):
        value = value.reshape(3, slab_count, capacity, width)
        return jnp.transpose(value, (1, 0, 2, 3)).reshape(slab_count, 3 * capacity, width)

    def by_component(value):
        value = value.reshape(slab_count, 3, capacity, width)
        return jnp.transpose(value, (1, 0, 2, 3)).reshape(3, slots, width)

    if packed:
        arrived = [exchange(results[0])]
        reply_shape = shape((slab_count, 3 * capacity, width), BF)
    else:
        slip = jnp.concatenate([by_owner(results[0]), results[1][:, None, :]], axis=1)
        got = exchange(slip)
        arrived = [
            by_component(got[:, : 3 * capacity]),
            got[:, 3 * capacity, :capacity].reshape(1, slots),
        ]
        reply_shape = shape((3, slots, width), BF)
    reply = pl.pallas_call(
        functools.partial(owner_kernel, slab_count, packed),
        out_shape=reply_shape,
        in_specs=[whole()] * (len(arrived) + 4),
        out_specs=whole(),
        compiler_params=limits,
        name="owner",
    )(
        *arrived,
        jnp.transpose(pair_list.reshape(slots, -1)),
        jnp.transpose(pair_gap.reshape(slots, -1)),
        self_coupling,
        pair_coupling,
    )
    back = exchange(reply) if packed else by_component(exchange(by_owner(reply)))

    collided, up, down, first, second = pl.pallas_call(
        functools.partial(spread_kernel, slab_count, packed),
        out_shape=[
            shape((19, rows, depth), F32),
            shape((8, depth), F32),
            shape((8, depth), F32),
            shape((5, rows, depth), BF),
            shape((5, rows, depth), BF),
        ],
        in_specs=[whole()] * 5,
        out_specs=[whole()] * 5,
        compiler_params=limits,
        name="spread",
    )(back, ordered, z_cells, y_cells, pops)
    marker_force = pl.pallas_call(
        functools.partial(finish_kernel, slab_count, packed),
        out_shape=shape((3, slots, width), BF),
        in_specs=[whole()] * 3,
        out_specs=whole(),
        compiler_params=limits,
        cost_estimate=pl.CostEstimate(flops=50_000_000, bytes_accessed=400_000, transcendentals=0),
        name="finish",
    )(back, ordered, send)

    slab_even = (lax.axis_index("slab") & 1) == 0
    sub_even = (lax.axis_index("sub") & 1) == 0
    first, second = swap(first, "slab", 0), swap(second, "slab", 1)
    top, bottom = slice(rows - 1, rows), slice(0, 1)
    one_up = jnp.where(slab_even, second[1, top], first[1, top])
    two_up = jnp.where(slab_even, first[2, top], second[2, top])
    one_down = jnp.where(slab_even, second[2, bottom], first[2, bottom])
    two_down = jnp.where(slab_even, first[1, bottom], second[1, bottom])
    up = jnp.concatenate([up[:3], one_up.astype(F32), two_up.astype(F32)])
    down = jnp.concatenate([down[:3], one_down.astype(F32), two_down.astype(F32)])
    low_high = (
        swap(jnp.where(sub_even, up, down), "sub", 0),
        swap(jnp.where(sub_even, down, up), "sub", 1),
    )
    read = pl.pallas_call(
        functools.partial(stream_kernel, lax.axis_size("sub")),
        out_shape=shape((19, rows, depth), F32),
        in_specs=[whole()] * 5,
        out_specs=whole(),
        compiler_params=limits,
        name="stream",
    )(collided, *low_high, first, second)
    marker_force = jnp.transpose(marker_force, (1, 0, 2))[None, None]
    return (read.reshape(19, 1, rows, depth), marker_force)


def solution(mesh):
    placed = (
        P(None, "slab", "sub", None),
        P("slab", "sub", None, None),
        P("slab", "sub", None),
        P("slab", "sub"),
        P("slab", "sub", None),
        P("sub", None),
        P("slab", "sub", None, None),
        P("slab", "sub", None, None),
        P("slab", "sub", None, None),
        P(),
        P(),
    )
    return jax.shard_map(
        per_device,
        mesh=mesh,
        in_specs=placed,
        out_specs=(P(None, "slab", "sub", None), P("slab", "sub", None, None, None)),
        check_vma=False,
    )
```

```python
import functools
import math

import jax
import jax.numpy as jnp
from jax import lax
from jax.experimental import pallas as pl
from jax.experimental.pallas import tpu as pltpu
from jax.sharding import PartitionSpec as P

lattice_dirs = [
    (0, 0, 0),
    (1, 0, 0),
    (-1, 0, 0),
    (0, 1, 0),
    (0, -1, 0),
    (0, 0, 1),
    (0, 0, -1),
    (1, 1, 0),
    (-1, -1, 0),
    (1, -1, 0),
    (-1, 1, 0),
    (1, 0, 1),
    (-1, 0, -1),
    (1, 0, -1),
    (-1, 0, 1),
    (0, 1, 1),
    (0, -1, -1),
    (0, 1, -1),
    (0, -1, 1),
]
lattice_weights = [1.0 / 3.0] + [1.0 / 18.0] * 6 + [1.0 / 36.0] * 12
opposite_of = [0, 2, 1, 4, 3, 6, 5, 8, 7, 10, 9, 12, 11, 14, 13, 16, 15, 18, 17]
relax_rate = 1.25
forward_x = [1, 7, 9, 11, 13]
backward_x = [2, 8, 10, 12, 14]
upward_y = [3, 15, 17, 7, 10]
downward_y = [4, 16, 18, 9, 8]
mark_rows = 8
kernel_memory = 16 << 20
BF = jnp.bfloat16
F32 = jnp.float32
PICK = jnp.float8_e4m3fn


def iota(shape, dim, dtype=F32):
    value = lax.broadcasted_iota(jnp.int32, shape, dim)
    return value if dtype == jnp.int32 else value.astype(F32).astype(dtype)


def dot_nt(a, b):
    return lax.dot_general(a, b, (((1,), (1,)), ((), ())), preferred_element_type=F32)


def dot_nn(a, b):
    return jnp.dot(a, b, preferred_element_type=F32)


def moments_of(pops):
    density = pops[0]
    moment = [None, None, None]
    for number in range(19):
        if number:
            density = density + pops[number]
        for axis in range(3):
            step = lattice_dirs[number][axis]
            if step == 0:
                continue
            if moment[axis] is None:
                moment[axis] = pops[number] if step == 1 else -pops[number]
            elif step == 1:
                moment[axis] = moment[axis] + pops[number]
            else:
                moment[axis] = moment[axis] - pops[number]
    return density, moment


def one_hot_rows(row, count):
    tile = (32, row.shape[1])
    tall = jnp.broadcast_to(row, tile).astype(BF)
    one, zero = jnp.ones(tile, F32).astype(PICK), jnp.zeros(tile, F32).astype(PICK)
    parts = []
    for start in range(0, count, 32):
        number = (iota(tile, 0) + float(start)).astype(BF)
        parts.append(jnp.where(number == tall, one, zero))
    return jnp.concatenate(parts, axis=0)


def fold_rows(blocks):
    row = iota(blocks[0].shape, 0, jnp.int32)
    half = 4
    while half:
        merged = []
        for s in range(half):
            a, b = blocks[s], blocks[s + half]
            merged.append(
                jnp.where(
                    (row & half) == 0,
                    a + pltpu.roll(a, 8 - half, 0),
                    b + pltpu.roll(b, half, 0),
                )
            )
        blocks = merged
        half //= 2
    return blocks[0]


def pieces_of(value):
    parts = []
    for step in range(3):
        part = value.astype(BF)
        parts.append(part)
        if step < 2:
            value = value - part.astype(F32)
    return parts


def pair_weights(list_ref, gap_ref):
    pairs, slots = list_ref.shape
    row = iota((slots, slots), 0, jnp.int32)
    inverse = 1.0 / gap_ref[...]
    weight = jnp.zeros((slots, slots), F32)
    for k in range(pairs):
        weight = weight + jnp.where(row == list_ref[k : k + 1, :], inverse[k : k + 1], 0.0)
    high = weight.astype(BF)
    return high, (weight - high.astype(F32)).astype(BF)


def sample_kernel(slab_count, packed, *refs):
    sources, refs = refs[:7], refs[7:]
    slip_ref, refs = refs[0], refs[1:]
    if not packed:
        spot_ref, refs = refs[0], refs[1:]
    send_ref, sorted_ref, z_ref, y_ref = refs[:4]
    targets, (sems,) = refs[4:11], refs[11:]
    copies = [
        pltpu.make_async_copy(source, target, sems.at[number])
        for number, (source, target) in enumerate(zip(sources, targets))
    ]
    for copy in copies:
        copy.start()
    count_ref, table_ref, marker_count_ref, id_ref, velocity_ref, cell_ref, pops_ref = targets
    slots, width = cell_ref.shape
    rows, depth = pops_ref.shape[1:]
    capacity = slots // slab_count
    for copy in copies[:5]:
        copy.wait()

    lane = iota((1, slots), 1, jnp.int32)
    alive = lane < count_ref[0]
    identity = id_ref[...]
    block = identity // slots
    spot = (identity % slots).astype(F32)

    def look_up(b, owner):
        return jnp.where(block == b, table_ref[b], owner)

    owner = lax.fori_loop(
        0, slab_count, look_up, jnp.zeros((1, slots), jnp.int32), unroll=slab_count <= 16
    )
    owner = jnp.where(alive, owner, -1)
    owner_f = owner.astype(F32)
    chosen = jnp.where(iota((slab_count, slots), 0) == owner_f, 1.0, 0.0)
    before = jnp.where(
        iota((slots, slots), 0) < iota((slots, slots), 1), 1.0, 0.0
    ).astype(BF)
    earlier = dot_nn(chosen.astype(BF), before)
    position = jnp.sum(chosen * earlier, axis=0, keepdims=True)
    send_row = jnp.where(alive, owner_f * float(capacity) + position, -1.0)
    place = jnp.where(iota((slots, slots), 0) == send_row, 1.0, 0.0).astype(BF)

    where_to = jnp.where(iota((width, slots), 0) == position, 1.0, 0.0).astype(BF)
    if packed:
        taken = (iota((slab_count * mark_rows, slots), 0, jnp.int32) // mark_rows).astype(
            F32
        ) == owner_f
        marks = dot_nt(jnp.where(taken, spot + 1.0, 0.0).astype(BF), where_to)
        slip_ref[:, 3 * capacity :, :] = marks.reshape(slab_count, mark_rows, width).astype(BF)
    else:
        spot_ref[...] = dot_nt((chosen * (spot + 1.0)).astype(BF), where_to).astype(BF)

    count = marker_count_ref[...].astype(F32)
    pieces = pieces_of(jnp.concatenate([velocity_ref[c] for c in range(3)], axis=0))
    stack = jnp.concatenate(
        [piece.astype(F32) for piece in pieces] + [count, send_row, jnp.zeros((5, slots), F32)],
        axis=0,
    )
    turned = jnp.transpose(stack)
    send_ref[...] = turned[:, 8:16]
    arranged = dot_nn(place, turned.astype(BF))
    velocity = (arranged[:, 0:3] + arranged[:, 3:6]) + arranged[:, 6:9]
    sorted_ref[...] = arranged[:, 8:16]

    for copy in copies[5:]:
        copy.wait()
    cells = cell_ref[...]
    parted = jnp.concatenate([(cells % depth).astype(BF), (cells // depth).astype(BF)], axis=1)
    moved = dot_nn(place, parted)
    z_ref[...] = moved[:, :width]
    y_ref[...] = moved[:, width:]

    density, moment = moments_of([pops_ref[number] for number in range(19)])
    flow = jnp.concatenate([part / density for part in moment], axis=0)
    high = flow.astype(BF)
    low = (flow - high.astype(F32)).astype(BF)
    flow_pair = jnp.concatenate([high, low], axis=1)

    for base in range(0, slots, 16):
        found_rows = []
        for eight in range(base, base + 16, 8):
            z_rows = z_ref[eight : eight + 8, :]
            y_rows = y_ref[eight : eight + 8, :]
            parts = [[], [], []]
            for first in range(0, 8, 2):
                picks = jnp.concatenate(
                    [one_hot_rows(z_rows[s : s + 1], depth) for s in (first, first + 1)], axis=1
                )
                picked = dot_nn(flow_pair, jnp.concatenate([picks, picks], axis=0))
                for s in (first, first + 1):
                    cut = slice((s - first) * width, (s - first + 1) * width)
                    tall = jnp.broadcast_to(y_rows[s : s + 1], (8, width))
                    found = [jnp.zeros((8, width), F32)] * 3
                    for start in range(0, rows, 8):
                        mask = iota((8, width), 0) + float(start) == tall
                        for c in range(3):
                            at = c * rows + start
                            found[c] = jnp.where(mask, picked[at : at + 8, cut], found[c])
                    for c in range(3):
                        parts[c].append(found[c])
            found_rows.append([fold_rows(parts[c]) for c in range(3)])
        live = iota((16, width), 1) < arranged[base : base + 16, 9:10]
        for c in range(3):
            sampled = jnp.concatenate([found_rows[0][c], found_rows[1][c]], axis=0)
            slip = jnp.where(live, velocity[base : base + 16, c : c + 1] - sampled, 0.0)
            if packed:
                at = c * capacity + base % capacity
                slip_ref[base // capacity, at : at + 16, :] = slip.astype(BF)
            else:
                slip_ref[c, base : base + 16, :] = slip.astype(BF)


def owner_kernel(
    slab_count,
    packed,
    *refs,
):
    if packed:
        got_ref, list_ref, gap_ref, self_ref, pair_ref, out_ref = refs
        width = got_ref.shape[2]
        slots = list_ref.shape[1]
        capacity = slots // slab_count
        got = jnp.concatenate(
            [
                got_ref[:, c * capacity : (c + 1) * capacity, :].reshape(slots, width)
                for c in range(3)
            ],
            axis=1,
        )
        per_tile = width // capacity
        lane = iota((8, width), 1, jnp.int32)
        tiles = []
        for start in range(0, slab_count, per_tile):
            total = jnp.zeros((8, width), F32)
            for source in range(start, min(start + per_tile, slab_count)):
                mark = got_ref[source, 3 * capacity : 3 * capacity + mark_rows, :].astype(F32)
                off = (source - start) * capacity
                if off:
                    mark = pltpu.roll(mark, off, 1)
                mine = (lane >= off) & (lane < off + capacity)
                total = jnp.where(mine, mark, total)
            tiles.append(total)
        spots = jnp.concatenate(tiles, axis=1) - 1.0
    else:
        got_ref, spot_ref, list_ref, gap_ref, self_ref, pair_ref, out_ref = refs
        width = got_ref.shape[2]
        slots = list_ref.shape[1]
        got = jnp.concatenate([got_ref[c] for c in range(3)], axis=1)
        spots = jnp.broadcast_to(spot_ref[...].astype(F32), (8, slots)) - 1.0

    spot_row = spots[:1]
    spot_col = jnp.transpose(spots)[:, :1]
    land = jnp.where(iota((slots, slots), 0) == spot_row, 1.0, 0.0).astype(BF)
    reply = jnp.where(iota((slots, slots), 1) == spot_col, 1.0, 0.0).astype(BF)
    chosen = [dot_nt(reply, part).astype(BF) for part in pair_weights(list_ref, gap_ref)]
    owned = dot_nn(land, got).astype(BF)
    near = (dot_nn(chosen[0], owned) + dot_nn(chosen[1], owned)).astype(BF)
    coupling = jnp.concatenate([self_ref[...], pair_ref[...]], axis=0)
    for c in range(3):
        span = slice(c * width, (c + 1) * width)
        both = jnp.concatenate([got[:, span], near[:, span]], axis=1)
        cut = dot_nn(both, coupling).astype(BF)
        if packed:
            out_ref[:, c * capacity : (c + 1) * capacity, :] = cut.reshape(
                slab_count, capacity, width
            )
        else:
            out_ref[c] = cut


def returned_rows(slab_count, packed, back_ref, sorted_ref, base, count):
    if packed:
        capacity = sorted_ref.shape[0] // slab_count
        at, block = base % capacity, slice(base // capacity, (base + count - 1) // capacity + 1)
        take = min(count, capacity)
        parts = [
            back_ref[block, c * capacity + at : c * capacity + at + take, :].reshape(count, -1)
            for c in range(3)
        ]
    else:
        parts = [back_ref[c, base : base + count, :] for c in range(3)]
    live = iota(parts[0].shape, 1) < sorted_ref[base : base + count, 1:2]
    return [jnp.where(live, part.astype(F32), 0.0) for part in parts]


def finish_kernel(slab_count, packed, back_ref, sorted_ref, send_ref, out_ref):
    slots = sorted_ref.shape[0]
    masked = returned_rows(slab_count, packed, back_ref, sorted_ref, 0, slots)
    fetch = jnp.where(iota((slots, slots), 1) == send_ref[:, 2:3], 1.0, 0.0).astype(BF)
    for c in range(3):
        out_ref[c] = dot_nn(fetch, masked[c].astype(BF)).astype(BF)


def spread_kernel(
    slab_count,
    packed,
    back_ref,
    sorted_ref,
    z_ref,
    y_ref,
    pops_ref,
    collided_ref,
    up_ref,
    down_ref,
    first_ref,
    second_ref,
):
    slots, width = z_ref.shape
    rows, depth = pops_ref.shape[1:]
    picks, terms = [], []
    for base in range(0, slots, 16):
        f_rows = returned_rows(slab_count, packed, back_ref, sorted_ref, base, 16)
        z_rows = z_ref[base : base + 16, :]
        y_rows = y_ref[base : base + 16, :]
        for s in range(16):
            picks.append(one_hot_rows(z_rows[s : s + 1], depth))
            tall = jnp.broadcast_to(y_rows[s : s + 1], (16, width)).astype(BF)
            parts = []
            for c in range(3):
                value = jnp.broadcast_to(f_rows[c][s : s + 1], (16, width)).astype(BF)
                for start in range(0, rows, 16):
                    number = (iota((16, width), 0) + float(start)).astype(BF)
                    parts.append(jnp.where(number == tall, value, jnp.zeros((), BF)))
            terms.append(jnp.concatenate(parts, axis=0))
    total = dot_nt(jnp.concatenate(terms, axis=1), jnp.concatenate(picks, axis=1))

    force = [total[c * rows : (c + 1) * rows] for c in range(3)]
    pops = [pops_ref[number] for number in range(19)]
    density, moment = moments_of(pops)
    velocity = [(moment[c] + 0.5 * force[c]) / density for c in range(3)]
    speed_sq = velocity[0] * velocity[0] + velocity[1] * velocity[1] + velocity[2] * velocity[2]
    work_rate = velocity[0] * force[0] + velocity[1] * force[1] + velocity[2] * force[2]
    base_term = 1.0 - 1.5 * speed_sq
    even = (lax.axis_index("slab") & 1) == 0
    sent = {}
    for number in range(19):
        step = lattice_dirs[number]
        along, push = None, None
        for c in range(3):
            if step[c] == 0:
                continue
            v, f = (velocity[c], force[c]) if step[c] == 1 else (-velocity[c], -force[c])
            along = v if along is None else along + v
            push = f if push is None else push + f
        weight = lattice_weights[number]
        if along is None:
            equilibrium = weight * density * base_term
            source = ((1.0 - 0.5 * relax_rate) * weight * -3.0) * work_rate
        else:
            equilibrium = weight * density * (base_term + 3.0 * along + 4.5 * along * along)
            source = ((1.0 - 0.5 * relax_rate) * weight) * (
                3.0 * (push - work_rate) + 9.0 * along * push
            )
        value = pops[number] - relax_rate * (pops[number] - equilibrium) + source
        collided_ref[number] = value
        if step[0] != 0:
            sent.setdefault((forward_x if step[0] == 1 else backward_x).index(number), {})[
                step[0]
            ] = value
        if number in upward_y[:3]:
            at = upward_y.index(number)
            up_ref[at : at + 1, :] = value[rows - 1 :]
        if number in downward_y[:3]:
            at = downward_y.index(number)
            down_ref[at : at + 1, :] = value[:1]
    for at, pair in sent.items():
        first_ref[at] = jnp.where(even, pair[1], pair[-1]).astype(BF)
        second_ref[at] = jnp.where(even, pair[-1], pair[1]).astype(BF)
    up_ref[3:, :] = jnp.zeros((5, depth), F32)
    down_ref[3:, :] = jnp.zeros((5, depth), F32)


def stream_kernel(
    sub_total, collided_ref, one_ref, two_ref, first_ref, second_ref, read_ref, out_ref, sems
):
    rows, depth = collided_ref.shape[1:]
    row = iota((rows, depth), 0, jnp.int32)
    place = lax.axis_index("sub")
    slab_even = (lax.axis_index("slab") & 1) == 0
    sub_even = (place & 1) == 0
    low = jnp.where(sub_even, two_ref[...], one_ref[...])
    high = jnp.where(sub_even, one_ref[...], two_ref[...])
    low_wall = jnp.where(place == 0, 1, 0)
    high_wall = jnp.where(place == sub_total - 1, 1, 0)
    copies = []
    for number in range(19):
        step_x, step_y, step_z = lattice_dirs[number]
        if step_x == 1:
            at = forward_x.index(number)
            moved = jnp.where(slab_even, second_ref[at].astype(F32), first_ref[at].astype(F32))
        elif step_x == -1:
            at = backward_x.index(number)
            moved = jnp.where(slab_even, first_ref[at].astype(F32), second_ref[at].astype(F32))
        else:
            moved = collided_ref[number]
        if step_y != 0:
            rolled = pltpu.roll(moved, 1 if step_y == 1 else rows - 1, 0)
            edge_row = 0 if step_y == 1 else rows - 1
            at = (upward_y if step_y == 1 else downward_y).index(number)
            edge = (low if step_y == 1 else high)[at : at + 1]
            moved = jnp.where(row == edge_row, edge, rolled)
        if step_z != 0:
            moved = pltpu.roll(moved, 1 if step_z == 1 else depth - 1, 1)
        if step_y != 0:
            wall = low_wall if step_y == 1 else high_wall
            at_wall = (row == edge_row) & (wall == 1)
            moved = jnp.where(at_wall, collided_ref[opposite_of[number]], moved)
        out_ref[number] = moved
        copies.append(
            pltpu.make_async_copy(out_ref.at[number], read_ref.at[number], sems.at[number])
        )
        copies[-1].start()
    for copy in copies:
        copy.wait()


def whole(memory=pltpu.VMEM):
    return pl.BlockSpec(memory_space=memory)


def swap(value, axis, odd):
    count = lax.axis_size(axis)
    pairs = [(i, (i + 1 if i % 2 == odd else i - 1) % count) for i in range(count)]
    return lax.ppermute(value, axis, pairs)


def per_device(
    populations,
    marker_cell,
    marker_count,
    particle_count,
    particle_id,
    owner_table,
    particle_velocity,
    pair_list,
    pair_gap,
    self_coupling,
    pair_coupling,
):
    slab_count = lax.axis_size("slab")
    slots, width = marker_cell.shape[2:]
    planes, rows, depth = populations.shape[1:]
    assert planes == 1 and slots <= 256 and slots % slab_count == 0
    assert slab_count % 2 == 0 and lax.axis_size("sub") % 2 == 0
    capacity = slots // slab_count
    assert capacity <= width
    packed = capacity % 16 == 0 and width % capacity == 0
    pops = populations.reshape(19, rows, depth)
    cells = marker_cell.reshape(slots, width)
    shape = jax.ShapeDtypeStruct
    limits = pltpu.CompilerParams(vmem_limit_bytes=kernel_memory)

    if packed:
        sample_out = [shape((slab_count, 3 * capacity + mark_rows, width), BF)]
    else:
        sample_out = [shape((3, slots, width), BF), shape((slab_count, width), BF)]
    sample_out += [shape((slots, 8), F32)] * 2 + [shape((slots, width), F32)] * 2
    results = pl.pallas_call(
        functools.partial(sample_kernel, slab_count, packed),
        out_shape=sample_out,
        in_specs=[whole(pltpu.HBM)] * 7,
        out_specs=[whole()] * len(sample_out),
        scratch_shapes=[
            pltpu.SMEM((1,), jnp.int32),
            pltpu.SMEM((slab_count,), jnp.int32),
            pltpu.VMEM((1, slots), jnp.int32),
            pltpu.VMEM((1, slots), jnp.int32),
            pltpu.VMEM((3, 1, slots), F32),
            pltpu.VMEM((slots, width), jnp.int32),
            pltpu.VMEM((19, rows, depth), F32),
            pltpu.SemaphoreType.DMA((7,)),
        ],
        compiler_params=limits,
        name="sample",
    )(
        particle_count.reshape(1),
        *[
            pltpu.with_memory_space_constraint(value, pltpu.HBM)
            for value in (
                owner_table.reshape(slab_count),
                marker_count.reshape(1, slots),
                particle_id.reshape(1, slots),
                particle_velocity.reshape(3, 1, slots),
                cells,
                pops,
            )
        ],
    )
    send, ordered, z_cells, y_cells = results[-4:]

    def exchange(value):
        return lax.all_to_all(value, "slab", split_axis=0, concat_axis=0, tiled=True)

    def by_owner(value):
        value = value.reshape(3, slab_count, capacity, width)
        return jnp.transpose(value, (1, 0, 2, 3)).reshape(slab_count, 3 * capacity, width)

    def by_component(value):
        value = value.reshape(slab_count, 3, capacity, width)
        return jnp.transpose(value, (1, 0, 2, 3)).reshape(3, slots, width)

    if packed:
        arrived = [exchange(results[0])]
        reply_shape = shape((slab_count, 3 * capacity, width), BF)
    else:
        slip = jnp.concatenate([by_owner(results[0]), results[1][:, None, :]], axis=1)
        got = exchange(slip)
        arrived = [
            by_component(got[:, : 3 * capacity]),
            got[:, 3 * capacity, :capacity].reshape(1, slots),
        ]
        reply_shape = shape((3, slots, width), BF)
    reply = pl.pallas_call(
        functools.partial(owner_kernel, slab_count, packed),
        out_shape=reply_shape,
        in_specs=[whole()] * (len(arrived) + 4),
        out_specs=whole(),
        compiler_params=limits,
        name="owner",
    )(
        *arrived,
        jnp.transpose(pair_list.reshape(slots, -1)),
        jnp.transpose(pair_gap.reshape(slots, -1)),
        self_coupling,
        pair_coupling,
    )
    back = exchange(reply) if packed else by_component(exchange(by_owner(reply)))

    collided, up, down, first, second = pl.pallas_call(
        functools.partial(spread_kernel, slab_count, packed),
        out_shape=[
            shape((19, rows, depth), F32),
            shape((8, depth), F32),
            shape((8, depth), F32),
            shape((5, rows, depth), BF),
            shape((5, rows, depth), BF),
        ],
        in_specs=[whole()] * 5,
        out_specs=[whole()] * 5,
        compiler_params=limits,
        name="spread",
    )(back, ordered, z_cells, y_cells, pops)
    marker_force = pl.pallas_call(
        functools.partial(finish_kernel, slab_count, packed),
        out_shape=shape((3, slots, width), BF),
        in_specs=[whole()] * 3,
        out_specs=whole(),
        compiler_params=limits,
        cost_estimate=pl.CostEstimate(flops=50_000_000, bytes_accessed=400_000, transcendentals=0),
        name="finish",
    )(back, ordered, send)

    slab_even = (lax.axis_index("slab") & 1) == 0
    sub_even = (lax.axis_index("sub") & 1) == 0
    first, second = swap(first, "slab", 0), swap(second, "slab", 1)
    top, bottom = slice(rows - 1, rows), slice(0, 1)
    one_up = jnp.where(slab_even, second[1, top], first[1, top])
    two_up = jnp.where(slab_even, first[2, top], second[2, top])
    one_down = jnp.where(slab_even, second[2, bottom], first[2, bottom])
    two_down = jnp.where(slab_even, first[1, bottom], second[1, bottom])
    up = jnp.concatenate([up[:3], one_up.astype(F32), two_up.astype(F32)])
    down = jnp.concatenate([down[:3], one_down.astype(F32), two_down.astype(F32)])
    low_high = (
        swap(jnp.where(sub_even, up, down), "sub", 0),
        swap(jnp.where(sub_even, down, up), "sub", 1),
    )
    read = pl.pallas_call(
        functools.partial(stream_kernel, lax.axis_size("sub")),
        out_shape=shape((19, rows, depth), F32),
        in_specs=[whole()] * 5,
        out_specs=whole(pltpu.HBM),
        scratch_shapes=[pltpu.VMEM((19, rows, depth), F32), pltpu.SemaphoreType.DMA((19,))],
        compiler_params=limits,
        name="stream",
    )(collided, *low_high, first, second)
    marker_force = jnp.transpose(marker_force, (1, 0, 2))[None, None]
    return (read.reshape(19, 1, rows, depth), marker_force)


def solution(mesh):
    placed = (
        P(None, "slab", "sub", None),
        P("slab", "sub", None, None),
        P("slab", "sub", None),
        P("slab", "sub"),
        P("slab", "sub", None),
        P("sub", None),
        P("slab", "sub", None, None),
        P("slab", "sub", None, None),
        P("slab", "sub", None, None),
        P(),
        P(),
    )
    return jax.shard_map(
        per_device,
        mesh=mesh,
        in_specs=placed,
        out_specs=(P(None, "slab", "sub", None), P("slab", "sub", None, None, None)),
        check_vma=False,
    )
```

```python
import functools
import math

import jax
import jax.numpy as jnp
from jax import lax
from jax.experimental import pallas as pl
from jax.experimental.pallas import tpu as pltpu
from jax.sharding import PartitionSpec as P

lattice_dirs = [
    (0, 0, 0),
    (1, 0, 0),
    (-1, 0, 0),
    (0, 1, 0),
    (0, -1, 0),
    (0, 0, 1),
    (0, 0, -1),
    (1, 1, 0),
    (-1, -1, 0),
    (1, -1, 0),
    (-1, 1, 0),
    (1, 0, 1),
    (-1, 0, -1),
    (1, 0, -1),
    (-1, 0, 1),
    (0, 1, 1),
    (0, -1, -1),
    (0, 1, -1),
    (0, -1, 1),
]
lattice_weights = [1.0 / 3.0] + [1.0 / 18.0] * 6 + [1.0 / 36.0] * 12
opposite_of = [0, 2, 1, 4, 3, 6, 5, 8, 7, 10, 9, 12, 11, 14, 13, 16, 15, 18, 17]
relax_rate = 1.25
forward_x = [1, 7, 9, 11, 13]
backward_x = [2, 8, 10, 12, 14]
upward_y = [3, 15, 17, 7, 10]
downward_y = [4, 16, 18, 9, 8]
mark_rows = 8
kernel_memory = 16 << 20
BF = jnp.bfloat16
F32 = jnp.float32
PICK = jnp.float8_e4m3fn


def iota(shape, dim, dtype=F32):
    value = lax.broadcasted_iota(jnp.int32, shape, dim)
    return value if dtype == jnp.int32 else value.astype(F32).astype(dtype)


def dot_nt(a, b):
    return lax.dot_general(a, b, (((1,), (1,)), ((), ())), preferred_element_type=F32)


def dot_nn(a, b):
    return jnp.dot(a, b, preferred_element_type=F32)


def moments_of(pops):
    density = pops[0]
    moment = [None, None, None]
    for number in range(19):
        if number:
            density = density + pops[number]
        for axis in range(3):
            step = lattice_dirs[number][axis]
            if step == 0:
                continue
            if moment[axis] is None:
                moment[axis] = pops[number] if step == 1 else -pops[number]
            elif step == 1:
                moment[axis] = moment[axis] + pops[number]
            else:
                moment[axis] = moment[axis] - pops[number]
    return density, moment


def one_hot_rows(row, count):
    tile = (32, row.shape[1])
    tall = jnp.broadcast_to(row, tile).astype(BF)
    one, zero = jnp.ones(tile, F32).astype(PICK), jnp.zeros(tile, F32).astype(PICK)
    parts = []
    for start in range(0, count, 32):
        number = (iota(tile, 0) + float(start)).astype(BF)
        parts.append(jnp.where(number == tall, one, zero))
    return jnp.concatenate(parts, axis=0)


def fold_rows(blocks):
    row = iota(blocks[0].shape, 0, jnp.int32)
    half = 4
    while half:
        merged = []
        for s in range(half):
            a, b = blocks[s], blocks[s + half]
            merged.append(
                jnp.where(
                    (row & half) == 0,
                    a + pltpu.roll(a, 8 - half, 0),
                    b + pltpu.roll(b, half, 0),
                )
            )
        blocks = merged
        half //= 2
    return blocks[0]


def pair_weights(list_ref, gap_ref):
    pairs, slots = list_ref.shape
    row = iota((slots, slots), 0, jnp.int32)
    inverse = 1.0 / gap_ref[...]
    weight = jnp.zeros((slots, slots), F32)
    for k in range(pairs):
        weight = weight + jnp.where(row == list_ref[k : k + 1, :], inverse[k : k + 1], 0.0)
    high = weight.astype(BF)
    return high, (weight - high.astype(F32)).astype(BF)


def sample_kernel(slab_count, packed, *refs):
    sources, refs = refs[:7], refs[7:]
    slip_ref, refs = refs[0], refs[1:]
    if not packed:
        spot_ref, refs = refs[0], refs[1:]
    send_ref, sorted_ref, z_ref, y_ref = refs[:4]
    targets, (sems,) = refs[4:11], refs[11:]
    copies = [
        pltpu.make_async_copy(source, target, sems.at[number])
        for number, (source, target) in enumerate(zip(sources, targets))
    ]
    for copy in copies:
        copy.start()
    count_ref, table_ref, marker_count_ref, id_ref, velocity_ref, cell_ref, pops_ref = targets
    slots, width = cell_ref.shape
    rows, depth = pops_ref.shape[1:]
    capacity = slots // slab_count
    for copy in copies[:5]:
        copy.wait()

    lane = iota((1, slots), 1, jnp.int32)
    alive = lane < count_ref[0]
    identity = id_ref[...]
    block = identity // slots
    spot = (identity % slots).astype(F32)

    def look_up(b, owner):
        return jnp.where(block == b, table_ref[b], owner)

    owner = lax.fori_loop(
        0, slab_count, look_up, jnp.zeros((1, slots), jnp.int32), unroll=slab_count <= 16
    )
    owner = jnp.where(alive, owner, -1)
    owner_f = owner.astype(F32)
    chosen = jnp.where(iota((slab_count, slots), 0) == owner_f, 1.0, 0.0)
    before = jnp.where(
        iota((slots, slots), 0) < iota((slots, slots), 1), 1.0, 0.0
    ).astype(BF)
    earlier = dot_nn(chosen.astype(BF), before)
    position = jnp.sum(chosen * earlier, axis=0, keepdims=True)
    send_row = jnp.where(alive, owner_f * float(capacity) + position, -1.0)
    place = jnp.where(iota((slots, slots), 0) == send_row, 1.0, 0.0).astype(BF)

    where_to = jnp.where(iota((width, slots), 0) == position, 1.0, 0.0).astype(BF)
    if packed:
        taken = (iota((slab_count * mark_rows, slots), 0, jnp.int32) // mark_rows).astype(
            F32
        ) == owner_f
        marks = dot_nt(jnp.where(taken, spot + 1.0, 0.0).astype(BF), where_to)
        slip_ref[:, 3 * capacity :, :] = marks.reshape(slab_count, mark_rows, width).astype(BF)
    else:
        spot_ref[...] = dot_nt((chosen * (spot + 1.0)).astype(BF), where_to).astype(BF)

    count = jnp.where(alive, marker_count_ref[...], 0).astype(F32)
    stack = jnp.concatenate(
        [velocity_ref[c] for c in range(3)] + [count, send_row, jnp.zeros((3, slots), F32)], axis=0
    )
    own = jnp.transpose(stack)
    send_ref[...] = own
    sorted_ref[...] = dot_nn(place, own.astype(BF))

    for copy in copies[5:]:
        copy.wait()
    cells = cell_ref[...]
    z_all, y_all = (cells % depth).astype(F32), (cells // depth).astype(F32)
    moved = dot_nn(place, jnp.concatenate([z_all, y_all], axis=1).astype(BF))
    z_ref[...] = moved[:, :width]
    y_ref[...] = moved[:, width:]

    density, moment = moments_of([pops_ref[number] for number in range(19)])
    flow = jnp.concatenate([part / density for part in moment], axis=0)
    high = flow.astype(BF)
    low = (flow - high.astype(F32)).astype(BF)
    flow_pair = jnp.concatenate([high, low], axis=1)

    slips = []
    for base in range(0, slots, 16):
        found_rows = []
        for eight in range(base, base + 16, 8):
            z_rows = z_all[eight : eight + 8]
            y_rows = y_all[eight : eight + 8]
            parts = [[], [], []]
            for first in range(0, 8, 2):
                picks = jnp.concatenate(
                    [one_hot_rows(z_rows[s : s + 1], depth) for s in (first, first + 1)], axis=1
                )
                picked = dot_nn(flow_pair, jnp.concatenate([picks, picks], axis=0))
                for s in (first, first + 1):
                    cut = slice((s - first) * width, (s - first + 1) * width)
                    tall = jnp.broadcast_to(y_rows[s : s + 1], (8, width))
                    found = [jnp.zeros((8, width), F32)] * 3
                    for start in range(0, rows, 8):
                        mask = iota((8, width), 0) + float(start) == tall
                        for c in range(3):
                            at = c * rows + start
                            found[c] = jnp.where(mask, picked[at : at + 8, cut], found[c])
                    for c in range(3):
                        parts[c].append(found[c])
            found_rows.append([fold_rows(parts[c]) for c in range(3)])
        live = iota((16, width), 1) < own[base : base + 16, 3:4]
        row = []
        for c in range(3):
            sampled = jnp.concatenate([found_rows[0][c], found_rows[1][c]], axis=0)
            slip = jnp.where(live, own[base : base + 16, c : c + 1] - sampled, 0.0)
            row.append(slip.astype(BF))
        slips.append(jnp.concatenate(row, axis=1))
    sent = dot_nn(place, jnp.concatenate(slips, axis=0)).astype(BF)
    for c in range(3):
        cut = sent[:, c * width : (c + 1) * width]
        if packed:
            slip_ref[:, c * capacity : (c + 1) * capacity, :] = cut.reshape(
                slab_count, capacity, width
            )
        else:
            slip_ref[c] = cut


def owner_kernel(
    slab_count,
    packed,
    *refs,
):
    if packed:
        got_ref, list_ref, gap_ref, self_ref, pair_ref, out_ref = refs
        width = got_ref.shape[2]
        slots = list_ref.shape[1]
        capacity = slots // slab_count
        got = jnp.concatenate(
            [
                got_ref[:, c * capacity : (c + 1) * capacity, :].reshape(slots, width)
                for c in range(3)
            ],
            axis=1,
        )
        per_tile = width // capacity
        lane = iota((8, width), 1, jnp.int32)
        tiles = []
        for start in range(0, slab_count, per_tile):
            total = jnp.zeros((8, width), F32)
            for source in range(start, min(start + per_tile, slab_count)):
                mark = got_ref[source, 3 * capacity : 3 * capacity + mark_rows, :].astype(F32)
                off = (source - start) * capacity
                if off:
                    mark = pltpu.roll(mark, off, 1)
                mine = (lane >= off) & (lane < off + capacity)
                total = jnp.where(mine, mark, total)
            tiles.append(total)
        spots = jnp.concatenate(tiles, axis=1) - 1.0
    else:
        got_ref, spot_ref, list_ref, gap_ref, self_ref, pair_ref, out_ref = refs
        width = got_ref.shape[2]
        slots = list_ref.shape[1]
        got = jnp.concatenate([got_ref[c] for c in range(3)], axis=1)
        spots = jnp.broadcast_to(spot_ref[...].astype(F32), (8, slots)) - 1.0

    spot_row = spots[:1]
    spot_col = jnp.transpose(spots)[:, :1]
    land = jnp.where(iota((slots, slots), 0) == spot_row, 1.0, 0.0).astype(BF)
    reply = jnp.where(iota((slots, slots), 1) == spot_col, 1.0, 0.0).astype(BF)
    chosen = [dot_nt(reply, part).astype(BF) for part in pair_weights(list_ref, gap_ref)]
    owned = dot_nn(land, got).astype(BF)
    near = (dot_nn(chosen[0], owned) + dot_nn(chosen[1], owned)).astype(BF)
    coupling = jnp.concatenate([self_ref[...], pair_ref[...]], axis=0)
    for c in range(3):
        span = slice(c * width, (c + 1) * width)
        both = jnp.concatenate([got[:, span], near[:, span]], axis=1)
        cut = dot_nn(both, coupling).astype(BF)
        if packed:
            out_ref[:, c * capacity : (c + 1) * capacity, :] = cut.reshape(
                slab_count, capacity, width
            )
        else:
            out_ref[c] = cut


def returned_rows(slab_count, packed, back_ref, sorted_ref, base, count):
    if packed:
        capacity = sorted_ref.shape[0] // slab_count
        at, block = base % capacity, slice(base // capacity, (base + count - 1) // capacity + 1)
        take = min(count, capacity)
        parts = [
            back_ref[block, c * capacity + at : c * capacity + at + take, :].reshape(count, -1)
            for c in range(3)
        ]
    else:
        parts = [back_ref[c, base : base + count, :] for c in range(3)]
    live = iota(parts[0].shape, 1) < sorted_ref[base : base + count, 3:4]
    return [jnp.where(live, part.astype(F32), 0.0) for part in parts]


def finish_kernel(slab_count, packed, back_ref, sorted_ref, send_ref, out_ref):
    slots = sorted_ref.shape[0]
    masked = returned_rows(slab_count, packed, back_ref, sorted_ref, 0, slots)
    fetch = jnp.where(iota((slots, slots), 1) == send_ref[:, 4:5], 1.0, 0.0).astype(BF)
    for c in range(3):
        out_ref[c] = dot_nn(fetch, masked[c].astype(BF)).astype(BF)


def spread_kernel(
    slab_count,
    packed,
    back_ref,
    sorted_ref,
    z_ref,
    y_ref,
    pops_ref,
    collided_ref,
    up_ref,
    down_ref,
    first_ref,
    second_ref,
):
    slots, width = z_ref.shape
    rows, depth = pops_ref.shape[1:]
    picks, terms = [], []
    for base in range(0, slots, 16):
        f_rows = returned_rows(slab_count, packed, back_ref, sorted_ref, base, 16)
        z_rows = z_ref[base : base + 16, :]
        y_rows = y_ref[base : base + 16, :]
        for s in range(16):
            picks.append(one_hot_rows(z_rows[s : s + 1], depth))
            tall = jnp.broadcast_to(y_rows[s : s + 1], (16, width)).astype(BF)
            parts = []
            for c in range(3):
                value = jnp.broadcast_to(f_rows[c][s : s + 1], (16, width)).astype(BF)
                for start in range(0, rows, 16):
                    number = (iota((16, width), 0) + float(start)).astype(BF)
                    parts.append(jnp.where(number == tall, value, jnp.zeros((), BF)))
            terms.append(jnp.concatenate(parts, axis=0))
    total = dot_nt(jnp.concatenate(terms, axis=1), jnp.concatenate(picks, axis=1))

    force = [total[c * rows : (c + 1) * rows] for c in range(3)]
    pops = [pops_ref[number] for number in range(19)]
    density, moment = moments_of(pops)
    velocity = [(moment[c] + 0.5 * force[c]) / density for c in range(3)]
    speed_sq = velocity[0] * velocity[0] + velocity[1] * velocity[1] + velocity[2] * velocity[2]
    work_rate = velocity[0] * force[0] + velocity[1] * force[1] + velocity[2] * force[2]
    base_term = 1.0 - 1.5 * speed_sq
    even = (lax.axis_index("slab") & 1) == 0
    sent = {}
    for number in range(19):
        step = lattice_dirs[number]
        along, push = None, None
        for c in range(3):
            if step[c] == 0:
                continue
            v, f = (velocity[c], force[c]) if step[c] == 1 else (-velocity[c], -force[c])
            along = v if along is None else along + v
            push = f if push is None else push + f
        weight = lattice_weights[number]
        if along is None:
            equilibrium = weight * density * base_term
            source = ((1.0 - 0.5 * relax_rate) * weight * -3.0) * work_rate
        else:
            equilibrium = weight * density * (base_term + 3.0 * along + 4.5 * along * along)
            source = ((1.0 - 0.5 * relax_rate) * weight) * (
                3.0 * (push - work_rate) + 9.0 * along * push
            )
        value = pops[number] - relax_rate * (pops[number] - equilibrium) + source
        collided_ref[number] = value
        if step[0] != 0:
            sent.setdefault((forward_x if step[0] == 1 else backward_x).index(number), {})[
                step[0]
            ] = value
        if number in upward_y[:3]:
            at = upward_y.index(number)
            up_ref[at : at + 1, :] = value[rows - 1 :]
        if number in downward_y[:3]:
            at = downward_y.index(number)
            down_ref[at : at + 1, :] = value[:1]
    for at, pair in sent.items():
        first_ref[at] = jnp.where(even, pair[1], pair[-1]).astype(BF)
        second_ref[at] = jnp.where(even, pair[-1], pair[1]).astype(BF)
    up_ref[3:, :] = jnp.zeros((5, depth), F32)
    down_ref[3:, :] = jnp.zeros((5, depth), F32)


def stream_kernel(
    sub_total, collided_ref, one_ref, two_ref, first_ref, second_ref, read_ref
):
    rows, depth = collided_ref.shape[1:]
    row = iota((rows, depth), 0, jnp.int32)
    place = lax.axis_index("sub")
    slab_even = (lax.axis_index("slab") & 1) == 0
    sub_even = (place & 1) == 0
    low = jnp.where(sub_even, two_ref[...], one_ref[...])
    high = jnp.where(sub_even, one_ref[...], two_ref[...])
    low_wall = jnp.where(place == 0, 1, 0)
    high_wall = jnp.where(place == sub_total - 1, 1, 0)
    for number in range(19):
        step_x, step_y, step_z = lattice_dirs[number]
        if step_x == 1:
            at = forward_x.index(number)
            moved = jnp.where(slab_even, second_ref[at].astype(F32), first_ref[at].astype(F32))
        elif step_x == -1:
            at = backward_x.index(number)
            moved = jnp.where(slab_even, first_ref[at].astype(F32), second_ref[at].astype(F32))
        else:
            moved = collided_ref[number]
        if step_y != 0:
            rolled = pltpu.roll(moved, 1 if step_y == 1 else rows - 1, 0)
            edge_row = 0 if step_y == 1 else rows - 1
            at = (upward_y if step_y == 1 else downward_y).index(number)
            edge = (low if step_y == 1 else high)[at : at + 1]
            moved = jnp.where(row == edge_row, edge, rolled)
        if step_z != 0:
            moved = pltpu.roll(moved, 1 if step_z == 1 else depth - 1, 1)
        if step_y != 0:
            wall = low_wall if step_y == 1 else high_wall
            at_wall = (row == edge_row) & (wall == 1)
            moved = jnp.where(at_wall, collided_ref[opposite_of[number]], moved)
        read_ref[number] = moved


def whole(memory=pltpu.VMEM):
    return pl.BlockSpec(memory_space=memory)


def swap(value, axis, odd):
    count = lax.axis_size(axis)
    pairs = [(i, (i + 1 if i % 2 == odd else i - 1) % count) for i in range(count)]
    return lax.ppermute(value, axis, pairs)


def per_device(
    populations,
    marker_cell,
    marker_count,
    particle_count,
    particle_id,
    owner_table,
    particle_velocity,
    pair_list,
    pair_gap,
    self_coupling,
    pair_coupling,
):
    slab_count = lax.axis_size("slab")
    slots, width = marker_cell.shape[2:]
    planes, rows, depth = populations.shape[1:]
    assert planes == 1 and slots <= 256 and slots % slab_count == 0
    assert slab_count % 2 == 0 and lax.axis_size("sub") % 2 == 0
    capacity = slots // slab_count
    assert capacity <= width
    packed = capacity % 16 == 0 and width % capacity == 0
    pops = populations.reshape(19, rows, depth)
    cells = marker_cell.reshape(slots, width)
    shape = jax.ShapeDtypeStruct
    limits = pltpu.CompilerParams(vmem_limit_bytes=kernel_memory)

    if packed:
        sample_out = [shape((slab_count, 3 * capacity + mark_rows, width), BF)]
    else:
        sample_out = [shape((3, slots, width), BF), shape((slab_count, width), BF)]
    sample_out += [shape((slots, 8), F32)] * 2 + [shape((slots, width), F32)] * 2
    results = pl.pallas_call(
        functools.partial(sample_kernel, slab_count, packed),
        out_shape=sample_out,
        in_specs=[whole(pltpu.HBM)] * 7,
        out_specs=[whole()] * len(sample_out),
        scratch_shapes=[
            pltpu.SMEM((1,), jnp.int32),
            pltpu.SMEM((slab_count,), jnp.int32),
            pltpu.VMEM((1, slots), jnp.int32),
            pltpu.VMEM((1, slots), jnp.int32),
            pltpu.VMEM((3, 1, slots), F32),
            pltpu.VMEM((slots, width), jnp.int32),
            pltpu.VMEM((19, rows, depth), F32),
            pltpu.SemaphoreType.DMA((7,)),
        ],
        compiler_params=limits,
        name="sample",
    )(
        particle_count.reshape(1),
        *[
            pltpu.with_memory_space_constraint(value, pltpu.HBM)
            for value in (
                owner_table.reshape(slab_count),
                marker_count.reshape(1, slots),
                particle_id.reshape(1, slots),
                particle_velocity.reshape(3, 1, slots),
                cells,
                pops,
            )
        ],
    )
    send, ordered, z_cells, y_cells = results[-4:]

    def exchange(value):
        return lax.all_to_all(value, "slab", split_axis=0, concat_axis=0, tiled=True)

    def by_owner(value):
        value = value.reshape(3, slab_count, capacity, width)
        return jnp.transpose(value, (1, 0, 2, 3)).reshape(slab_count, 3 * capacity, width)

    def by_component(value):
        value = value.reshape(slab_count, 3, capacity, width)
        return jnp.transpose(value, (1, 0, 2, 3)).reshape(3, slots, width)

    if packed:
        arrived = [exchange(results[0])]
        reply_shape = shape((slab_count, 3 * capacity, width), BF)
    else:
        slip = jnp.concatenate([by_owner(results[0]), results[1][:, None, :]], axis=1)
        got = exchange(slip)
        arrived = [
            by_component(got[:, : 3 * capacity]),
            got[:, 3 * capacity, :capacity].reshape(1, slots),
        ]
        reply_shape = shape((3, slots, width), BF)
    reply = pl.pallas_call(
        functools.partial(owner_kernel, slab_count, packed),
        out_shape=reply_shape,
        in_specs=[whole()] * (len(arrived) + 4),
        out_specs=whole(),
        compiler_params=limits,
        name="owner",
    )(
        *arrived,
        jnp.transpose(pair_list.reshape(slots, -1)),
        jnp.transpose(pair_gap.reshape(slots, -1)),
        self_coupling,
        pair_coupling,
    )
    back = exchange(reply) if packed else by_component(exchange(by_owner(reply)))

    collided, up, down, first, second = pl.pallas_call(
        functools.partial(spread_kernel, slab_count, packed),
        out_shape=[
            shape((19, rows, depth), F32),
            shape((8, depth), F32),
            shape((8, depth), F32),
            shape((5, rows, depth), BF),
            shape((5, rows, depth), BF),
        ],
        in_specs=[whole()] * 5,
        out_specs=[whole()] * 5,
        compiler_params=limits,
        name="spread",
    )(back, ordered, z_cells, y_cells, pops)
    marker_force = pl.pallas_call(
        functools.partial(finish_kernel, slab_count, packed),
        out_shape=shape((3, slots, width), BF),
        in_specs=[whole()] * 3,
        out_specs=whole(),
        compiler_params=limits,
        cost_estimate=pl.CostEstimate(flops=50_000_000, bytes_accessed=400_000, transcendentals=0),
        name="finish",
    )(back, ordered, send)

    slab_even = (lax.axis_index("slab") & 1) == 0
    sub_even = (lax.axis_index("sub") & 1) == 0
    first, second = swap(first, "slab", 0), swap(second, "slab", 1)
    top, bottom = slice(rows - 1, rows), slice(0, 1)
    one_up = jnp.where(slab_even, second[1, top], first[1, top])
    two_up = jnp.where(slab_even, first[2, top], second[2, top])
    one_down = jnp.where(slab_even, second[2, bottom], first[2, bottom])
    two_down = jnp.where(slab_even, first[1, bottom], second[1, bottom])
    up = jnp.concatenate([up[:3], one_up.astype(F32), two_up.astype(F32)])
    down = jnp.concatenate([down[:3], one_down.astype(F32), two_down.astype(F32)])
    low_high = (
        swap(jnp.where(sub_even, up, down), "sub", 0),
        swap(jnp.where(sub_even, down, up), "sub", 1),
    )
    read = pl.pallas_call(
        functools.partial(stream_kernel, lax.axis_size("sub")),
        out_shape=shape((19, rows, depth), F32),
        in_specs=[whole()] * 5,
        out_specs=whole(),
        compiler_params=limits,
        name="stream",
    )(collided, *low_high, first, second)
    marker_force = jnp.transpose(marker_force, (1, 0, 2))[None, None]
    return (read.reshape(19, 1, rows, depth), marker_force)


def solution(mesh):
    placed = (
        P(None, "slab", "sub", None),
        P("slab", "sub", None, None),
        P("slab", "sub", None),
        P("slab", "sub"),
        P("slab", "sub", None),
        P("sub", None),
        P("slab", "sub", None, None),
        P("slab", "sub", None, None),
        P("slab", "sub", None, None),
        P(),
        P(),
    )
    return jax.shard_map(
        per_device,
        mesh=mesh,
        in_specs=placed,
        out_specs=(P(None, "slab", "sub", None), P("slab", "sub", None, None, None)),
        check_vma=False,
    )
```

```python
import functools
import math

import jax
import jax.numpy as jnp
from jax import lax
from jax.experimental import pallas as pl
from jax.experimental.pallas import tpu as pltpu
from jax.sharding import PartitionSpec as P

lattice_dirs = [
    (0, 0, 0),
    (1, 0, 0),
    (-1, 0, 0),
    (0, 1, 0),
    (0, -1, 0),
    (0, 0, 1),
    (0, 0, -1),
    (1, 1, 0),
    (-1, -1, 0),
    (1, -1, 0),
    (-1, 1, 0),
    (1, 0, 1),
    (-1, 0, -1),
    (1, 0, -1),
    (-1, 0, 1),
    (0, 1, 1),
    (0, -1, -1),
    (0, 1, -1),
    (0, -1, 1),
]
lattice_weights = [1.0 / 3.0] + [1.0 / 18.0] * 6 + [1.0 / 36.0] * 12
opposite_of = [0, 2, 1, 4, 3, 6, 5, 8, 7, 10, 9, 12, 11, 14, 13, 16, 15, 18, 17]
relax_rate = 1.25
forward_x = [1, 7, 9, 11, 13]
backward_x = [2, 8, 10, 12, 14]
upward_y = [3, 15, 17, 7, 10]
downward_y = [4, 16, 18, 9, 8]
mark_rows = 8
kernel_memory = 16 << 20
BF = jnp.bfloat16
F32 = jnp.float32
PICK = jnp.float8_e4m3fn


def iota(shape, dim, dtype=F32):
    value = lax.broadcasted_iota(jnp.int32, shape, dim)
    return value if dtype == jnp.int32 else value.astype(F32).astype(dtype)


def dot_nt(a, b):
    return lax.dot_general(a, b, (((1,), (1,)), ((), ())), preferred_element_type=F32)


def dot_nn(a, b):
    return jnp.dot(a, b, preferred_element_type=F32)


def moments_of(pops):
    density = pops[0]
    moment = [None, None, None]
    for number in range(19):
        if number:
            density = density + pops[number]
        for axis in range(3):
            step = lattice_dirs[number][axis]
            if step == 0:
                continue
            if moment[axis] is None:
                moment[axis] = pops[number] if step == 1 else -pops[number]
            elif step == 1:
                moment[axis] = moment[axis] + pops[number]
            else:
                moment[axis] = moment[axis] - pops[number]
    return density, moment


def one_hot_rows(row, count):
    tile = (32, row.shape[1])
    tall = jnp.broadcast_to(row, tile).astype(BF)
    one, zero = jnp.ones(tile, F32).astype(PICK), jnp.zeros(tile, F32).astype(PICK)
    parts = []
    for start in range(0, count, 32):
        number = (iota(tile, 0) + float(start)).astype(BF)
        parts.append(jnp.where(number == tall, one, zero))
    return jnp.concatenate(parts, axis=0)


def fold_rows(blocks):
    row = iota(blocks[0].shape, 0, jnp.int32)
    half = 4
    while half:
        merged = []
        for s in range(half):
            a, b = blocks[s], blocks[s + half]
            merged.append(
                jnp.where(
                    (row & half) == 0,
                    a + pltpu.roll(a, 8 - half, 0),
                    b + pltpu.roll(b, half, 0),
                )
            )
        blocks = merged
        half //= 2
    return blocks[0]


def pair_weights(list_ref, gap_ref):
    pairs, slots = list_ref.shape
    row = iota((slots, slots), 0, jnp.int32)
    inverse = 1.0 / gap_ref[...]
    weight = jnp.zeros((slots, slots), F32)
    for k in range(pairs):
        weight = weight + jnp.where(row == list_ref[k : k + 1, :], inverse[k : k + 1], 0.0)
    high = weight.astype(BF)
    return high, (weight - high.astype(F32)).astype(BF)


def sample_kernel(slab_count, packed, *refs):
    left_ref, sources, refs = refs[0], refs[1:7], refs[7:]
    slip_ref, refs = refs[0], refs[1:]
    if not packed:
        spot_ref, refs = refs[0], refs[1:]
    send_ref, sorted_ref, z_ref, y_ref = refs[:4]
    targets, (sems,) = refs[4:10], refs[10:]
    copies = [
        pltpu.make_async_copy(source, target, sems.at[number])
        for number, (source, target) in enumerate(zip(sources, targets))
    ]
    for copy in copies:
        copy.start()
    table_ref, marker_count_ref, id_ref, velocity_ref, cell_ref, pops_ref = targets
    slots, width = cell_ref.shape
    rows, depth = pops_ref.shape[1:]
    capacity = slots // slab_count
    for copy in copies[:4]:
        copy.wait()

    alive = left_ref[...] > 0
    identity = id_ref[...]
    block = identity // slots
    spot = (identity % slots).astype(F32)

    def look_up(b, owner):
        return jnp.where(block == b, table_ref[b], owner)

    owner = lax.fori_loop(
        0, slab_count, look_up, jnp.zeros((1, slots), jnp.int32), unroll=slab_count <= 16
    )
    owner = jnp.where(alive, owner, -1)
    owner_f = owner.astype(F32)
    chosen = jnp.where(iota((slab_count, slots), 0) == owner_f, 1.0, 0.0)
    before = jnp.where(
        iota((slots, slots), 0) < iota((slots, slots), 1), 1.0, 0.0
    ).astype(BF)
    earlier = dot_nn(chosen.astype(BF), before)
    position = jnp.sum(chosen * earlier, axis=0, keepdims=True)
    send_row = jnp.where(alive, owner_f * float(capacity) + position, -1.0)
    place = jnp.where(iota((slots, slots), 0) == send_row, 1.0, 0.0).astype(BF)

    where_to = jnp.where(iota((width, slots), 0) == position, 1.0, 0.0).astype(BF)
    if packed:
        taken = (iota((slab_count * mark_rows, slots), 0, jnp.int32) // mark_rows).astype(
            F32
        ) == owner_f
        marks = dot_nt(jnp.where(taken, spot + 1.0, 0.0).astype(BF), where_to)
        slip_ref[:, 3 * capacity :, :] = marks.reshape(slab_count, mark_rows, width).astype(BF)
    else:
        spot_ref[...] = dot_nt((chosen * (spot + 1.0)).astype(BF), where_to).astype(BF)

    count = jnp.where(alive, marker_count_ref[...], 0).astype(F32)
    stack = jnp.concatenate(
        [velocity_ref[c] for c in range(3)] + [count, send_row, jnp.zeros((3, slots), F32)], axis=0
    )
    own = jnp.transpose(stack)
    send_ref[...] = own
    sorted_ref[...] = dot_nn(place, own.astype(BF))

    for copy in copies[4:]:
        copy.wait()
    cells = cell_ref[...]
    z_all, y_all = (cells % depth).astype(F32), (cells // depth).astype(F32)
    moved = dot_nn(place, jnp.concatenate([z_all, y_all], axis=1).astype(BF))
    z_ref[...] = moved[:, :width]
    y_ref[...] = moved[:, width:]

    density, moment = moments_of([pops_ref[number] for number in range(19)])
    flow = jnp.concatenate([part / density for part in moment], axis=0)
    high = flow.astype(BF)
    low = (flow - high.astype(F32)).astype(BF)
    flow_pair = jnp.concatenate([high, low], axis=1)

    slips = []
    for base in range(0, slots, 16):
        found_rows = []
        for eight in range(base, base + 16, 8):
            z_rows = z_all[eight : eight + 8]
            y_rows = y_all[eight : eight + 8]
            parts = [[], [], []]
            for first in range(0, 8, 2):
                picks = jnp.concatenate(
                    [one_hot_rows(z_rows[s : s + 1], depth) for s in (first, first + 1)], axis=1
                )
                picked = dot_nn(flow_pair, jnp.concatenate([picks, picks], axis=0))
                for s in (first, first + 1):
                    cut = slice((s - first) * width, (s - first + 1) * width)
                    tall = jnp.broadcast_to(y_rows[s : s + 1], (8, width))
                    found = [jnp.zeros((8, width), F32)] * 3
                    for start in range(0, rows, 8):
                        mask = iota((8, width), 0) + float(start) == tall
                        for c in range(3):
                            at = c * rows + start
                            found[c] = jnp.where(mask, picked[at : at + 8, cut], found[c])
                    for c in range(3):
                        parts[c].append(found[c])
            found_rows.append([fold_rows(parts[c]) for c in range(3)])
        live = iota((16, width), 1) < own[base : base + 16, 3:4]
        row = []
        for c in range(3):
            sampled = jnp.concatenate([found_rows[0][c], found_rows[1][c]], axis=0)
            slip = jnp.where(live, own[base : base + 16, c : c + 1] - sampled, 0.0)
            row.append(slip.astype(BF))
        slips.append(jnp.concatenate(row, axis=1))
    sent = dot_nn(place, jnp.concatenate(slips, axis=0)).astype(BF)
    for c in range(3):
        cut = sent[:, c * width : (c + 1) * width]
        if packed:
            slip_ref[:, c * capacity : (c + 1) * capacity, :] = cut.reshape(
                slab_count, capacity, width
            )
        else:
            slip_ref[c] = cut


def owner_kernel(
    slab_count,
    packed,
    *refs,
):
    if packed:
        got_ref, list_ref, gap_ref, self_ref, pair_ref, out_ref = refs
        width = got_ref.shape[2]
        slots = list_ref.shape[1]
        capacity = slots // slab_count
        got = jnp.concatenate(
            [
                got_ref[:, c * capacity : (c + 1) * capacity, :].reshape(slots, width)
                for c in range(3)
            ],
            axis=1,
        )
        per_tile = width // capacity
        lane = iota((8, width), 1, jnp.int32)
        tiles = []
        for start in range(0, slab_count, per_tile):
            total = jnp.zeros((8, width), F32)
            for source in range(start, min(start + per_tile, slab_count)):
                mark = got_ref[source, 3 * capacity : 3 * capacity + mark_rows, :].astype(F32)
                off = (source - start) * capacity
                if off:
                    mark = pltpu.roll(mark, off, 1)
                mine = (lane >= off) & (lane < off + capacity)
                total = jnp.where(mine, mark, total)
            tiles.append(total)
        spots = jnp.concatenate(tiles, axis=1) - 1.0
    else:
        got_ref, spot_ref, list_ref, gap_ref, self_ref, pair_ref, out_ref = refs
        width = got_ref.shape[2]
        slots = list_ref.shape[1]
        got = jnp.concatenate([got_ref[c] for c in range(3)], axis=1)
        spots = jnp.broadcast_to(spot_ref[...].astype(F32), (8, slots)) - 1.0

    spot_row = spots[:1]
    spot_col = jnp.transpose(spots)[:, :1]
    land = jnp.where(iota((slots, slots), 0) == spot_row, 1.0, 0.0).astype(BF)
    reply = jnp.where(iota((slots, slots), 1) == spot_col, 1.0, 0.0).astype(BF)
    chosen = [dot_nt(reply, part).astype(BF) for part in pair_weights(list_ref, gap_ref)]
    owned = dot_nn(land, got).astype(BF)
    near = (dot_nn(chosen[0], owned) + dot_nn(chosen[1], owned)).astype(BF)
    coupling = jnp.concatenate([self_ref[...], pair_ref[...]], axis=0)
    for c in range(3):
        span = slice(c * width, (c + 1) * width)
        both = jnp.concatenate([got[:, span], near[:, span]], axis=1)
        cut = dot_nn(both, coupling).astype(BF)
        if packed:
            out_ref[:, c * capacity : (c + 1) * capacity, :] = cut.reshape(
                slab_count, capacity, width
            )
        else:
            out_ref[c] = cut


def returned_rows(slab_count, packed, back_ref, sorted_ref, base, count):
    if packed:
        capacity = sorted_ref.shape[0] // slab_count
        at, block = base % capacity, slice(base // capacity, (base + count - 1) // capacity + 1)
        take = min(count, capacity)
        parts = [
            back_ref[block, c * capacity + at : c * capacity + at + take, :].reshape(count, -1)
            for c in range(3)
        ]
    else:
        parts = [back_ref[c, base : base + count, :] for c in range(3)]
    live = iota(parts[0].shape, 1) < sorted_ref[base : base + count, 3:4]
    return [jnp.where(live, part.astype(F32), 0.0) for part in parts]


def finish_kernel(slab_count, packed, back_ref, sorted_ref, send_ref, out_ref):
    slots = sorted_ref.shape[0]
    masked = returned_rows(slab_count, packed, back_ref, sorted_ref, 0, slots)
    fetch = jnp.where(iota((slots, slots), 1) == send_ref[:, 4:5], 1.0, 0.0).astype(BF)
    for c in range(3):
        out_ref[c] = dot_nn(fetch, masked[c].astype(BF)).astype(BF)


def spread_kernel(
    slab_count,
    packed,
    back_ref,
    sorted_ref,
    z_ref,
    y_ref,
    pops_ref,
    collided_ref,
    up_ref,
    down_ref,
    first_ref,
    second_ref,
):
    slots, width = z_ref.shape
    rows, depth = pops_ref.shape[1:]
    picks, terms = [], []
    for base in range(0, slots, 16):
        f_rows = returned_rows(slab_count, packed, back_ref, sorted_ref, base, 16)
        z_rows = z_ref[base : base + 16, :]
        y_rows = y_ref[base : base + 16, :]
        for s in range(16):
            picks.append(one_hot_rows(z_rows[s : s + 1], depth))
            tall = jnp.broadcast_to(y_rows[s : s + 1], (16, width)).astype(BF)
            parts = []
            for c in range(3):
                value = jnp.broadcast_to(f_rows[c][s : s + 1], (16, width)).astype(BF)
                for start in range(0, rows, 16):
                    number = (iota((16, width), 0) + float(start)).astype(BF)
                    parts.append(jnp.where(number == tall, value, jnp.zeros((), BF)))
            terms.append(jnp.concatenate(parts, axis=0))
    total = dot_nt(jnp.concatenate(terms, axis=1), jnp.concatenate(picks, axis=1))

    force = [total[c * rows : (c + 1) * rows] for c in range(3)]
    pops = [pops_ref[number] for number in range(19)]
    density, moment = moments_of(pops)
    velocity = [(moment[c] + 0.5 * force[c]) / density for c in range(3)]
    speed_sq = velocity[0] * velocity[0] + velocity[1] * velocity[1] + velocity[2] * velocity[2]
    work_rate = velocity[0] * force[0] + velocity[1] * force[1] + velocity[2] * force[2]
    base_term = 1.0 - 1.5 * speed_sq
    even = (lax.axis_index("slab") & 1) == 0
    sent = {}
    for number in range(19):
        step = lattice_dirs[number]
        along, push = None, None
        for c in range(3):
            if step[c] == 0:
                continue
            v, f = (velocity[c], force[c]) if step[c] == 1 else (-velocity[c], -force[c])
            along = v if along is None else along + v
            push = f if push is None else push + f
        weight = lattice_weights[number]
        if along is None:
            equilibrium = weight * density * base_term
            source = ((1.0 - 0.5 * relax_rate) * weight * -3.0) * work_rate
        else:
            equilibrium = weight * density * (base_term + 3.0 * along + 4.5 * along * along)
            source = ((1.0 - 0.5 * relax_rate) * weight) * (
                3.0 * (push - work_rate) + 9.0 * along * push
            )
        value = pops[number] - relax_rate * (pops[number] - equilibrium) + source
        collided_ref[number] = value
        if step[0] != 0:
            sent.setdefault((forward_x if step[0] == 1 else backward_x).index(number), {})[
                step[0]
            ] = value
        if number in upward_y[:3]:
            at = upward_y.index(number)
            up_ref[at : at + 1, :] = value[rows - 1 :]
        if number in downward_y[:3]:
            at = downward_y.index(number)
            down_ref[at : at + 1, :] = value[:1]
    for at, pair in sent.items():
        first_ref[at] = jnp.where(even, pair[1], pair[-1]).astype(BF)
        second_ref[at] = jnp.where(even, pair[-1], pair[1]).astype(BF)
    up_ref[3:, :] = jnp.zeros((5, depth), F32)
    down_ref[3:, :] = jnp.zeros((5, depth), F32)


def stream_kernel(
    sub_total, collided_ref, one_ref, two_ref, first_ref, second_ref, read_ref
):
    rows, depth = collided_ref.shape[1:]
    row = iota((rows, depth), 0, jnp.int32)
    place = lax.axis_index("sub")
    slab_even = (lax.axis_index("slab") & 1) == 0
    sub_even = (place & 1) == 0
    low = jnp.where(sub_even, two_ref[...], one_ref[...])
    high = jnp.where(sub_even, one_ref[...], two_ref[...])
    low_wall = jnp.where(place == 0, 1, 0)
    high_wall = jnp.where(place == sub_total - 1, 1, 0)
    for number in range(19):
        step_x, step_y, step_z = lattice_dirs[number]
        if step_x == 1:
            at = forward_x.index(number)
            moved = jnp.where(slab_even, second_ref[at].astype(F32), first_ref[at].astype(F32))
        elif step_x == -1:
            at = backward_x.index(number)
            moved = jnp.where(slab_even, first_ref[at].astype(F32), second_ref[at].astype(F32))
        else:
            moved = collided_ref[number]
        if step_y != 0:
            rolled = pltpu.roll(moved, 1 if step_y == 1 else rows - 1, 0)
            edge_row = 0 if step_y == 1 else rows - 1
            at = (upward_y if step_y == 1 else downward_y).index(number)
            edge = (low if step_y == 1 else high)[at : at + 1]
            moved = jnp.where(row == edge_row, edge, rolled)
        if step_z != 0:
            moved = pltpu.roll(moved, 1 if step_z == 1 else depth - 1, 1)
        if step_y != 0:
            wall = low_wall if step_y == 1 else high_wall
            at_wall = (row == edge_row) & (wall == 1)
            moved = jnp.where(at_wall, collided_ref[opposite_of[number]], moved)
        read_ref[number] = moved


def whole(memory=pltpu.VMEM):
    return pl.BlockSpec(memory_space=memory)


def swap(value, axis, odd):
    count = lax.axis_size(axis)
    pairs = [(i, (i + 1 if i % 2 == odd else i - 1) % count) for i in range(count)]
    return lax.ppermute(value, axis, pairs)


def per_device(
    populations,
    marker_cell,
    marker_count,
    particle_count,
    particle_id,
    owner_table,
    particle_velocity,
    pair_list,
    pair_gap,
    self_coupling,
    pair_coupling,
):
    slab_count = lax.axis_size("slab")
    slots, width = marker_cell.shape[2:]
    planes, rows, depth = populations.shape[1:]
    assert planes == 1 and slots <= 256 and slots % slab_count == 0
    assert slab_count % 2 == 0 and lax.axis_size("sub") % 2 == 0
    capacity = slots // slab_count
    assert capacity <= width
    packed = capacity % 16 == 0 and width % capacity == 0
    pops = populations.reshape(19, rows, depth)
    cells = marker_cell.reshape(slots, width)
    shape = jax.ShapeDtypeStruct
    limits = pltpu.CompilerParams(vmem_limit_bytes=kernel_memory)

    if packed:
        sample_out = [shape((slab_count, 3 * capacity + mark_rows, width), BF)]
    else:
        sample_out = [shape((3, slots, width), BF), shape((slab_count, width), BF)]
    sample_out += [shape((slots, 8), F32)] * 2 + [shape((slots, width), F32)] * 2
    results = pl.pallas_call(
        functools.partial(sample_kernel, slab_count, packed),
        out_shape=sample_out,
        in_specs=[whole()] + [whole(pltpu.HBM)] * 6,
        out_specs=[whole()] * len(sample_out),
        scratch_shapes=[
            pltpu.SMEM((slab_count,), jnp.int32),
            pltpu.VMEM((1, slots), jnp.int32),
            pltpu.VMEM((1, slots), jnp.int32),
            pltpu.VMEM((3, 1, slots), F32),
            pltpu.VMEM((slots, width), jnp.int32),
            pltpu.VMEM((19, rows, depth), F32),
            pltpu.SemaphoreType.DMA((6,)),
        ],
        compiler_params=limits,
        name="sample",
    )(
        particle_count - lax.broadcasted_iota(jnp.int32, (1, slots), 1),
        *[
            pltpu.with_memory_space_constraint(value, pltpu.HBM)
            for value in (
                owner_table.reshape(slab_count),
                marker_count.reshape(1, slots),
                particle_id.reshape(1, slots),
                particle_velocity.reshape(3, 1, slots),
                cells,
                pops,
            )
        ],
    )
    send, ordered, z_cells, y_cells = results[-4:]

    def exchange(value):
        return lax.all_to_all(value, "slab", split_axis=0, concat_axis=0, tiled=True)

    def by_owner(value):
        value = value.reshape(3, slab_count, capacity, width)
        return jnp.transpose(value, (1, 0, 2, 3)).reshape(slab_count, 3 * capacity, width)

    def by_component(value):
        value = value.reshape(slab_count, 3, capacity, width)
        return jnp.transpose(value, (1, 0, 2, 3)).reshape(3, slots, width)

    if packed:
        arrived = [exchange(results[0])]
        reply_shape = shape((slab_count, 3 * capacity, width), BF)
    else:
        slip = jnp.concatenate([by_owner(results[0]), results[1][:, None, :]], axis=1)
        got = exchange(slip)
        arrived = [
            by_component(got[:, : 3 * capacity]),
            got[:, 3 * capacity, :capacity].reshape(1, slots),
        ]
        reply_shape = shape((3, slots, width), BF)
    reply = pl.pallas_call(
        functools.partial(owner_kernel, slab_count, packed),
        out_shape=reply_shape,
        in_specs=[whole()] * (len(arrived) + 4),
        out_specs=whole(),
        compiler_params=limits,
        name="owner",
    )(
        *arrived,
        jnp.transpose(pair_list.reshape(slots, -1)),
        jnp.transpose(pair_gap.reshape(slots, -1)),
        self_coupling,
        pair_coupling,
    )
    back = exchange(reply) if packed else by_component(exchange(by_owner(reply)))

    collided, up, down, first, second = pl.pallas_call(
        functools.partial(spread_kernel, slab_count, packed),
        out_shape=[
            shape((19, rows, depth), F32),
            shape((8, depth), F32),
            shape((8, depth), F32),
            shape((5, rows, depth), BF),
            shape((5, rows, depth), BF),
        ],
        in_specs=[whole()] * 5,
        out_specs=[whole()] * 5,
        compiler_params=limits,
        name="spread",
    )(back, ordered, z_cells, y_cells, pops)
    marker_force = pl.pallas_call(
        functools.partial(finish_kernel, slab_count, packed),
        out_shape=shape((3, slots, width), BF),
        in_specs=[whole()] * 3,
        out_specs=whole(),
        compiler_params=limits,
        cost_estimate=pl.CostEstimate(flops=50_000_000, bytes_accessed=400_000, transcendentals=0),
        name="finish",
    )(back, ordered, send)

    slab_even = (lax.axis_index("slab") & 1) == 0
    sub_even = (lax.axis_index("sub") & 1) == 0
    first, second = swap(first, "slab", 0), swap(second, "slab", 1)
    top, bottom = slice(rows - 1, rows), slice(0, 1)
    one_up = jnp.where(slab_even, second[1, top], first[1, top])
    two_up = jnp.where(slab_even, first[2, top], second[2, top])
    one_down = jnp.where(slab_even, second[2, bottom], first[2, bottom])
    two_down = jnp.where(slab_even, first[1, bottom], second[1, bottom])
    up = jnp.concatenate([up[:3], one_up.astype(F32), two_up.astype(F32)])
    down = jnp.concatenate([down[:3], one_down.astype(F32), two_down.astype(F32)])
    low_high = (
        swap(jnp.where(sub_even, up, down), "sub", 0),
        swap(jnp.where(sub_even, down, up), "sub", 1),
    )
    read = pl.pallas_call(
        functools.partial(stream_kernel, lax.axis_size("sub")),
        out_shape=shape((19, rows, depth), F32),
        in_specs=[whole()] * 5,
        out_specs=whole(),
        compiler_params=limits,
        name="stream",
    )(collided, *low_high, first, second)
    marker_force = jnp.transpose(marker_force, (1, 0, 2))[None, None]
    return (read.reshape(19, 1, rows, depth), marker_force)


def solution(mesh):
    placed = (
        P(None, "slab", "sub", None),
        P("slab", "sub", None, None),
        P("slab", "sub", None),
        P("slab", "sub"),
        P("slab", "sub", None),
        P("sub", None),
        P("slab", "sub", None, None),
        P("slab", "sub", None, None),
        P("slab", "sub", None, None),
        P(),
        P(),
    )
    return jax.shard_map(
        per_device,
        mesh=mesh,
        in_specs=placed,
        out_specs=(P(None, "slab", "sub", None), P("slab", "sub", None, None, None)),
        check_vma=False,
    )
```

```python
import functools
import math

import jax
import jax.numpy as jnp
from jax import lax
from jax.experimental import pallas as pl
from jax.experimental.pallas import tpu as pltpu
from jax.sharding import PartitionSpec as P

lattice_dirs = [
    (0, 0, 0),
    (1, 0, 0),
    (-1, 0, 0),
    (0, 1, 0),
    (0, -1, 0),
    (0, 0, 1),
    (0, 0, -1),
    (1, 1, 0),
    (-1, -1, 0),
    (1, -1, 0),
    (-1, 1, 0),
    (1, 0, 1),
    (-1, 0, -1),
    (1, 0, -1),
    (-1, 0, 1),
    (0, 1, 1),
    (0, -1, -1),
    (0, 1, -1),
    (0, -1, 1),
]
lattice_weights = [1.0 / 3.0] + [1.0 / 18.0] * 6 + [1.0 / 36.0] * 12
opposite_of = [0, 2, 1, 4, 3, 6, 5, 8, 7, 10, 9, 12, 11, 14, 13, 16, 15, 18, 17]
relax_rate = 1.25
forward_x = [1, 7, 9, 11, 13]
backward_x = [2, 8, 10, 12, 14]
upward_y = [3, 15, 17, 7, 10]
downward_y = [4, 16, 18, 9, 8]
mark_rows = 8
kernel_memory = 12 << 20
BF = jnp.bfloat16
F32 = jnp.float32
PICK = jnp.float8_e4m3fn


def iota(shape, dim, dtype=F32):
    value = lax.broadcasted_iota(jnp.int32, shape, dim)
    return value if dtype == jnp.int32 else value.astype(F32).astype(dtype)


def dot_nt(a, b):
    return lax.dot_general(a, b, (((1,), (1,)), ((), ())), preferred_element_type=F32)


def dot_nn(a, b):
    return jnp.dot(a, b, preferred_element_type=F32)


def moments_of(pops):
    density = pops[0]
    moment = [None, None, None]
    for number in range(19):
        if number:
            density = density + pops[number]
        for axis in range(3):
            step = lattice_dirs[number][axis]
            if step == 0:
                continue
            if moment[axis] is None:
                moment[axis] = pops[number] if step == 1 else -pops[number]
            elif step == 1:
                moment[axis] = moment[axis] + pops[number]
            else:
                moment[axis] = moment[axis] - pops[number]
    return density, moment


def one_hot_rows(row, count):
    tile = (32, row.shape[1])
    tall = jnp.broadcast_to(row, tile).astype(BF)
    one, zero = jnp.ones(tile, F32).astype(PICK), jnp.zeros(tile, F32).astype(PICK)
    parts = []
    for start in range(0, count, 32):
        number = (iota(tile, 0) + float(start)).astype(BF)
        parts.append(jnp.where(number == tall, one, zero))
    return jnp.concatenate(parts, axis=0)


def fold_rows(blocks):
    row = iota(blocks[0].shape, 0, jnp.int32)
    half = 4
    while half:
        merged = []
        for s in range(half):
            a, b = blocks[s], blocks[s + half]
            merged.append(
                jnp.where(
                    (row & half) == 0,
                    a + pltpu.roll(a, 8 - half, 0),
                    b + pltpu.roll(b, half, 0),
                )
            )
        blocks = merged
        half //= 2
    return blocks[0]


def pair_weights(list_ref, gap_ref):
    pairs, slots = list_ref.shape
    row = iota((slots, slots), 0, jnp.int32)
    inverse = 1.0 / gap_ref[...]
    weight = jnp.zeros((slots, slots), F32)
    for k in range(pairs):
        weight = weight + jnp.where(row == list_ref[k : k + 1, :], inverse[k : k + 1], 0.0)
    high = weight.astype(BF)
    return high, (weight - high.astype(F32)).astype(BF)


def sample_kernel(slab_count, packed, *refs):
    left_ref, sources, refs = refs[0], refs[1:7], refs[7:]
    slip_ref, refs = refs[0], refs[1:]
    if not packed:
        spot_ref, refs = refs[0], refs[1:]
    send_ref, sorted_ref, z_ref, y_ref = refs[:4]
    targets, (sems,) = refs[4:10], refs[10:]
    copies = [
        pltpu.make_async_copy(source, target, sems.at[number])
        for number, (source, target) in enumerate(zip(sources, targets))
    ]
    for copy in copies:
        copy.start()
    table_ref, marker_count_ref, id_ref, velocity_ref, cell_ref, pops_ref = targets
    slots, width = cell_ref.shape
    rows, depth = pops_ref.shape[1:]
    capacity = slots // slab_count
    for copy in copies[:4]:
        copy.wait()

    alive = left_ref[...] > 0
    identity = id_ref[...]
    block = identity // slots
    spot = (identity % slots).astype(F32)

    def look_up(b, owner):
        return jnp.where(block == b, table_ref[b], owner)

    owner = lax.fori_loop(
        0, slab_count, look_up, jnp.zeros((1, slots), jnp.int32), unroll=slab_count <= 16
    )
    owner = jnp.where(alive, owner, -1)
    owner_f = owner.astype(F32)
    chosen = jnp.where(iota((slab_count, slots), 0) == owner_f, 1.0, 0.0)
    before = jnp.where(
        iota((slots, slots), 0) < iota((slots, slots), 1), 1.0, 0.0
    ).astype(BF)
    earlier = dot_nn(chosen.astype(BF), before)
    position = jnp.sum(chosen * earlier, axis=0, keepdims=True)
    send_row = jnp.where(alive, owner_f * float(capacity) + position, -1.0)
    place = jnp.where(iota((slots, slots), 0) == send_row, 1.0, 0.0).astype(BF)

    where_to = jnp.where(iota((width, slots), 0) == position, 1.0, 0.0).astype(BF)
    if packed:
        taken = (iota((slab_count * mark_rows, slots), 0, jnp.int32) // mark_rows).astype(
            F32
        ) == owner_f
        marks = dot_nt(jnp.where(taken, spot + 1.0, 0.0).astype(BF), where_to)
        slip_ref[:, 3 * capacity :, :] = marks.reshape(slab_count, mark_rows, width).astype(BF)
    else:
        spot_ref[...] = dot_nt((chosen * (spot + 1.0)).astype(BF), where_to).astype(BF)

    count = jnp.where(alive, marker_count_ref[...], 0).astype(F32)
    stack = jnp.concatenate(
        [velocity_ref[c] for c in range(3)] + [count, send_row, jnp.zeros((3, slots), F32)], axis=0
    )
    own = jnp.transpose(stack)
    send_ref[...] = own
    sorted_ref[...] = dot_nn(place, own.astype(BF))

    for copy in copies[4:]:
        copy.wait()
    cells = cell_ref[...]
    z_all, y_all = (cells % depth).astype(F32), (cells // depth).astype(F32)
    moved = dot_nn(place, jnp.concatenate([z_all, y_all], axis=1).astype(BF))
    z_ref[...] = moved[:, :width]
    y_ref[...] = moved[:, width:]

    density, moment = moments_of([pops_ref[number] for number in range(19)])
    flow = jnp.concatenate([part / density for part in moment], axis=0)
    high = flow.astype(BF)
    low = (flow - high.astype(F32)).astype(BF)
    flow_pair = jnp.concatenate([high, low], axis=1)

    slips = []
    for base in range(0, slots, 16):
        found_rows = []
        for eight in range(base, base + 16, 8):
            z_rows = z_all[eight : eight + 8]
            y_rows = y_all[eight : eight + 8]
            parts = [[], [], []]
            for first in range(0, 8, 2):
                if (eight + first) // 2 % 4 == 3:
                    picked = []
                    for s in (first, first + 1):
                        index = jnp.broadcast_to(z_rows[s : s + 1].astype(jnp.int32), (8, depth))
                        picked.append(
                            jnp.concatenate(
                                [
                                    jnp.take_along_axis(flow[k : k + 8], index, axis=1)
                                    for k in range(0, 3 * rows, 8)
                                ],
                                axis=0,
                            )
                        )
                    picked = jnp.concatenate(picked, axis=1)
                else:
                    picks = jnp.concatenate(
                        [one_hot_rows(z_rows[s : s + 1], depth) for s in (first, first + 1)],
                        axis=1,
                    )
                    picked = dot_nn(flow_pair, jnp.concatenate([picks, picks], axis=0))
                for s in (first, first + 1):
                    cut = slice((s - first) * width, (s - first + 1) * width)
                    tall = jnp.broadcast_to(y_rows[s : s + 1], (8, width))
                    found = [jnp.zeros((8, width), F32)] * 3
                    for start in range(0, rows, 8):
                        mask = iota((8, width), 0) + float(start) == tall
                        for c in range(3):
                            at = c * rows + start
                            found[c] = jnp.where(mask, picked[at : at + 8, cut], found[c])
                    for c in range(3):
                        parts[c].append(found[c])
            found_rows.append([fold_rows(parts[c]) for c in range(3)])
        live = iota((16, width), 1) < own[base : base + 16, 3:4]
        row = []
        for c in range(3):
            sampled = jnp.concatenate([found_rows[0][c], found_rows[1][c]], axis=0)
            slip = jnp.where(live, own[base : base + 16, c : c + 1] - sampled, 0.0)
            row.append(slip.astype(BF))
        slips.append(jnp.concatenate(row, axis=1))
    sent = dot_nn(place, jnp.concatenate(slips, axis=0)).astype(BF)
    for c in range(3):
        cut = sent[:, c * width : (c + 1) * width]
        if packed:
            slip_ref[:, c * capacity : (c + 1) * capacity, :] = cut.reshape(
                slab_count, capacity, width
            )
        else:
            slip_ref[c] = cut


def owner_kernel(
    slab_count,
    packed,
    *refs,
):
    if packed:
        got_ref, list_ref, gap_ref, self_ref, pair_ref, out_ref = refs
        width = got_ref.shape[2]
        slots = list_ref.shape[1]
        capacity = slots // slab_count
        got = jnp.concatenate(
            [
                got_ref[:, c * capacity : (c + 1) * capacity, :].reshape(slots, width)
                for c in range(3)
            ],
            axis=1,
        )
        per_tile = width // capacity
        lane = iota((8, width), 1, jnp.int32)
        tiles = []
        for start in range(0, slab_count, per_tile):
            total = jnp.zeros((8, width), F32)
            for source in range(start, min(start + per_tile, slab_count)):
                mark = got_ref[source, 3 * capacity : 3 * capacity + mark_rows, :].astype(F32)
                off = (source - start) * capacity
                if off:
                    mark = pltpu.roll(mark, off, 1)
                mine = (lane >= off) & (lane < off + capacity)
                total = jnp.where(mine, mark, total)
            tiles.append(total)
        spots = jnp.concatenate(tiles, axis=1) - 1.0
    else:
        got_ref, spot_ref, list_ref, gap_ref, self_ref, pair_ref, out_ref = refs
        width = got_ref.shape[2]
        slots = list_ref.shape[1]
        got = jnp.concatenate([got_ref[c] for c in range(3)], axis=1)
        spots = jnp.broadcast_to(spot_ref[...].astype(F32), (8, slots)) - 1.0

    spot_row = spots[:1]
    spot_col = jnp.transpose(spots)[:, :1]
    land = jnp.where(iota((slots, slots), 0) == spot_row, 1.0, 0.0).astype(BF)
    reply = jnp.where(iota((slots, slots), 1) == spot_col, 1.0, 0.0).astype(BF)
    chosen = [dot_nt(reply, part).astype(BF) for part in pair_weights(list_ref, gap_ref)]
    owned = dot_nn(land, got).astype(BF)
    near = (dot_nn(chosen[0], owned) + dot_nn(chosen[1], owned)).astype(BF)
    coupling = jnp.concatenate([self_ref[...], pair_ref[...]], axis=0)
    for c in range(3):
        span = slice(c * width, (c + 1) * width)
        both = jnp.concatenate([got[:, span], near[:, span]], axis=1)
        cut = dot_nn(both, coupling).astype(BF)
        if packed:
            out_ref[:, c * capacity : (c + 1) * capacity, :] = cut.reshape(
                slab_count, capacity, width
            )
        else:
            out_ref[c] = cut


def returned_rows(slab_count, packed, back_ref, sorted_ref, base, count):
    if packed:
        capacity = sorted_ref.shape[0] // slab_count
        at, block = base % capacity, slice(base // capacity, (base + count - 1) // capacity + 1)
        take = min(count, capacity)
        parts = [
            back_ref[block, c * capacity + at : c * capacity + at + take, :].reshape(count, -1)
            for c in range(3)
        ]
    else:
        parts = [back_ref[c, base : base + count, :] for c in range(3)]
    live = iota(parts[0].shape, 1) < sorted_ref[base : base + count, 3:4]
    return [jnp.where(live, part.astype(F32), 0.0) for part in parts]


def finish_kernel(slab_count, packed, back_ref, sorted_ref, send_ref, out_ref):
    slots = sorted_ref.shape[0]
    masked = returned_rows(slab_count, packed, back_ref, sorted_ref, 0, slots)
    fetch = jnp.where(iota((slots, slots), 1) == send_ref[:, 4:5], 1.0, 0.0).astype(BF)
    for c in range(3):
        out_ref[c] = dot_nn(fetch, masked[c].astype(BF)).astype(BF)


def spread_kernel(
    slab_count,
    packed,
    back_ref,
    sorted_ref,
    z_ref,
    y_ref,
    pops_ref,
    collided_ref,
    up_ref,
    down_ref,
    first_ref,
    second_ref,
):
    slots, width = z_ref.shape
    rows, depth = pops_ref.shape[1:]
    picks, terms = [], []
    for base in range(0, slots, 16):
        f_rows = returned_rows(slab_count, packed, back_ref, sorted_ref, base, 16)
        z_rows = z_ref[base : base + 16, :]
        y_rows = y_ref[base : base + 16, :]
        for s in range(16):
            picks.append(one_hot_rows(z_rows[s : s + 1], depth))
            tall = jnp.broadcast_to(y_rows[s : s + 1], (16, width)).astype(BF)
            parts = []
            for c in range(3):
                value = jnp.broadcast_to(f_rows[c][s : s + 1], (16, width)).astype(BF)
                for start in range(0, rows, 16):
                    number = (iota((16, width), 0) + float(start)).astype(BF)
                    parts.append(jnp.where(number == tall, value, jnp.zeros((), BF)))
            terms.append(jnp.concatenate(parts, axis=0))
    total = dot_nt(jnp.concatenate(terms, axis=1), jnp.concatenate(picks, axis=1))

    force = [total[c * rows : (c + 1) * rows] for c in range(3)]
    pops = [pops_ref[number] for number in range(19)]
    density, moment = moments_of(pops)
    velocity = [(moment[c] + 0.5 * force[c]) / density for c in range(3)]
    speed_sq = velocity[0] * velocity[0] + velocity[1] * velocity[1] + velocity[2] * velocity[2]
    work_rate = velocity[0] * force[0] + velocity[1] * force[1] + velocity[2] * force[2]
    base_term = 1.0 - 1.5 * speed_sq
    even = (lax.axis_index("slab") & 1) == 0
    sent = {}
    for number in range(19):
        step = lattice_dirs[number]
        along, push = None, None
        for c in range(3):
            if step[c] == 0:
                continue
            v, f = (velocity[c], force[c]) if step[c] == 1 else (-velocity[c], -force[c])
            along = v if along is None else along + v
            push = f if push is None else push + f
        weight = lattice_weights[number]
        if along is None:
            equilibrium = weight * density * base_term
            source = ((1.0 - 0.5 * relax_rate) * weight * -3.0) * work_rate
        else:
            equilibrium = weight * density * (base_term + 3.0 * along + 4.5 * along * along)
            source = ((1.0 - 0.5 * relax_rate) * weight) * (
                3.0 * (push - work_rate) + 9.0 * along * push
            )
        value = pops[number] - relax_rate * (pops[number] - equilibrium) + source
        collided_ref[number] = value
        if step[0] != 0:
            sent.setdefault((forward_x if step[0] == 1 else backward_x).index(number), {})[
                step[0]
            ] = value
        if number in upward_y[:3]:
            at = upward_y.index(number)
            up_ref[at : at + 1, :] = value[rows - 1 :]
        if number in downward_y[:3]:
            at = downward_y.index(number)
            down_ref[at : at + 1, :] = value[:1]
    for at, pair in sent.items():
        first_ref[at] = jnp.where(even, pair[1], pair[-1]).astype(BF)
        second_ref[at] = jnp.where(even, pair[-1], pair[1]).astype(BF)
    up_ref[3:, :] = jnp.zeros((5, depth), F32)
    down_ref[3:, :] = jnp.zeros((5, depth), F32)


def stream_kernel(
    sub_total, collided_ref, one_ref, two_ref, first_ref, second_ref, read_ref
):
    rows, depth = collided_ref.shape[1:]
    row = iota((rows, depth), 0, jnp.int32)
    place = lax.axis_index("sub")
    slab_even = (lax.axis_index("slab") & 1) == 0
    sub_even = (place & 1) == 0
    low = jnp.where(sub_even, two_ref[...], one_ref[...])
    high = jnp.where(sub_even, one_ref[...], two_ref[...])
    low_wall = jnp.where(place == 0, 1, 0)
    high_wall = jnp.where(place == sub_total - 1, 1, 0)
    for number in range(19):
        step_x, step_y, step_z = lattice_dirs[number]
        if step_x == 1:
            at = forward_x.index(number)
            moved = jnp.where(slab_even, second_ref[at].astype(F32), first_ref[at].astype(F32))
        elif step_x == -1:
            at = backward_x.index(number)
            moved = jnp.where(slab_even, first_ref[at].astype(F32), second_ref[at].astype(F32))
        else:
            moved = collided_ref[number]
        if step_y != 0:
            rolled = pltpu.roll(moved, 1 if step_y == 1 else rows - 1, 0)
            edge_row = 0 if step_y == 1 else rows - 1
            at = (upward_y if step_y == 1 else downward_y).index(number)
            edge = (low if step_y == 1 else high)[at : at + 1]
            moved = jnp.where(row == edge_row, edge, rolled)
        if step_z != 0:
            moved = pltpu.roll(moved, 1 if step_z == 1 else depth - 1, 1)
        if step_y != 0:
            wall = low_wall if step_y == 1 else high_wall
            at_wall = (row == edge_row) & (wall == 1)
            moved = jnp.where(at_wall, collided_ref[opposite_of[number]], moved)
        read_ref[number] = moved


def whole(memory=pltpu.VMEM):
    return pl.BlockSpec(memory_space=memory)


def swap(value, axis, odd):
    count = lax.axis_size(axis)
    pairs = [(i, (i + 1 if i % 2 == odd else i - 1) % count) for i in range(count)]
    return lax.ppermute(value, axis, pairs)


def per_device(
    populations,
    marker_cell,
    marker_count,
    particle_count,
    particle_id,
    owner_table,
    particle_velocity,
    pair_list,
    pair_gap,
    self_coupling,
    pair_coupling,
):
    slab_count = lax.axis_size("slab")
    slots, width = marker_cell.shape[2:]
    planes, rows, depth = populations.shape[1:]
    assert planes == 1 and slots <= 256 and slots % slab_count == 0
    assert slab_count % 2 == 0 and lax.axis_size("sub") % 2 == 0
    capacity = slots // slab_count
    assert capacity <= width
    packed = capacity % 16 == 0 and width % capacity == 0
    pops = populations.reshape(19, rows, depth)
    cells = marker_cell.reshape(slots, width)
    shape = jax.ShapeDtypeStruct
    limits = pltpu.CompilerParams(vmem_limit_bytes=kernel_memory)

    if packed:
        sample_out = [shape((slab_count, 3 * capacity + mark_rows, width), BF)]
    else:
        sample_out = [shape((3, slots, width), BF), shape((slab_count, width), BF)]
    sample_out += [shape((slots, 8), F32)] * 2 + [shape((slots, width), F32)] * 2
    results = pl.pallas_call(
        functools.partial(sample_kernel, slab_count, packed),
        out_shape=sample_out,
        in_specs=[whole()] + [whole(pltpu.HBM)] * 6,
        out_specs=[whole()] * len(sample_out),
        scratch_shapes=[
            pltpu.SMEM((slab_count,), jnp.int32),
            pltpu.VMEM((1, slots), jnp.int32),
            pltpu.VMEM((1, slots), jnp.int32),
            pltpu.VMEM((3, 1, slots), F32),
            pltpu.VMEM((slots, width), jnp.int32),
            pltpu.VMEM((19, rows, depth), F32),
            pltpu.SemaphoreType.DMA((6,)),
        ],
        compiler_params=limits,
        name="sample",
    )(
        particle_count - lax.broadcasted_iota(jnp.int32, (1, slots), 1),
        *[
            pltpu.with_memory_space_constraint(value, pltpu.HBM)
            for value in (
                owner_table.reshape(slab_count),
                marker_count.reshape(1, slots),
                particle_id.reshape(1, slots),
                particle_velocity.reshape(3, 1, slots),
                cells,
                pops,
            )
        ],
    )
    send, ordered, z_cells, y_cells = results[-4:]

    def exchange(value):
        return lax.all_to_all(value, "slab", split_axis=0, concat_axis=0, tiled=True)

    def by_owner(value):
        value = value.reshape(3, slab_count, capacity, width)
        return jnp.transpose(value, (1, 0, 2, 3)).reshape(slab_count, 3 * capacity, width)

    def by_component(value):
        value = value.reshape(slab_count, 3, capacity, width)
        return jnp.transpose(value, (1, 0, 2, 3)).reshape(3, slots, width)

    if packed:
        arrived = [exchange(results[0])]
        reply_shape = shape((slab_count, 3 * capacity, width), BF)
    else:
        slip = jnp.concatenate([by_owner(results[0]), results[1][:, None, :]], axis=1)
        got = exchange(slip)
        arrived = [
            by_component(got[:, : 3 * capacity]),
            got[:, 3 * capacity, :capacity].reshape(1, slots),
        ]
        reply_shape = shape((3, slots, width), BF)
    reply = pl.pallas_call(
        functools.partial(owner_kernel, slab_count, packed),
        out_shape=reply_shape,
        in_specs=[whole()] * (len(arrived) + 4),
        out_specs=whole(),
        compiler_params=limits,
        name="owner",
    )(
        *arrived,
        jnp.transpose(pair_list.reshape(slots, -1)),
        jnp.transpose(pair_gap.reshape(slots, -1)),
        self_coupling,
        pair_coupling,
    )
    back = exchange(reply) if packed else by_component(exchange(by_owner(reply)))

    collided, up, down, first, second = pl.pallas_call(
        functools.partial(spread_kernel, slab_count, packed),
        out_shape=[
            shape((19, rows, depth), F32),
            shape((8, depth), F32),
            shape((8, depth), F32),
            shape((5, rows, depth), BF),
            shape((5, rows, depth), BF),
        ],
        in_specs=[whole()] * 5,
        out_specs=[whole()] * 5,
        compiler_params=limits,
        name="spread",
    )(back, ordered, z_cells, y_cells, pops)
    marker_force = pl.pallas_call(
        functools.partial(finish_kernel, slab_count, packed),
        out_shape=shape((3, slots, width), BF),
        in_specs=[whole()] * 3,
        out_specs=whole(),
        compiler_params=limits,
        cost_estimate=pl.CostEstimate(flops=50_000_000, bytes_accessed=400_000, transcendentals=0),
        name="finish",
    )(back, ordered, send)

    slab_even = (lax.axis_index("slab") & 1) == 0
    sub_even = (lax.axis_index("sub") & 1) == 0
    first, second = swap(first, "slab", 0), swap(second, "slab", 1)
    top, bottom = slice(rows - 1, rows), slice(0, 1)
    one_up = jnp.where(slab_even, second[1, top], first[1, top])
    two_up = jnp.where(slab_even, first[2, top], second[2, top])
    one_down = jnp.where(slab_even, second[2, bottom], first[2, bottom])
    two_down = jnp.where(slab_even, first[1, bottom], second[1, bottom])
    up = jnp.concatenate([up[:3], one_up.astype(F32), two_up.astype(F32)])
    down = jnp.concatenate([down[:3], one_down.astype(F32), two_down.astype(F32)])
    low_high = (
        swap(jnp.where(sub_even, up, down), "sub", 0),
        swap(jnp.where(sub_even, down, up), "sub", 1),
    )
    read = pl.pallas_call(
        functools.partial(stream_kernel, lax.axis_size("sub")),
        out_shape=shape((19, rows, depth), F32),
        in_specs=[whole()] * 5,
        out_specs=whole(),
        compiler_params=limits,
        name="stream",
    )(collided, *low_high, first, second)
    marker_force = jnp.transpose(marker_force, (1, 0, 2))[None, None]
    return (read.reshape(19, 1, rows, depth), marker_force)


def solution(mesh):
    placed = (
        P(None, "slab", "sub", None),
        P("slab", "sub", None, None),
        P("slab", "sub", None),
        P("slab", "sub"),
        P("slab", "sub", None),
        P("sub", None),
        P("slab", "sub", None, None),
        P("slab", "sub", None, None),
        P("slab", "sub", None, None),
        P(),
        P(),
    )
    return jax.shard_map(
        per_device,
        mesh=mesh,
        in_specs=placed,
        out_specs=(P(None, "slab", "sub", None), P("slab", "sub", None, None, None)),
        check_vma=False,
    )
```

```python
import functools
import math

import jax
import jax.numpy as jnp
from jax import lax
from jax.experimental import pallas as pl
from jax.experimental.pallas import tpu as pltpu
from jax.sharding import PartitionSpec as P

lattice_dirs = [
    (0, 0, 0),
    (1, 0, 0),
    (-1, 0, 0),
    (0, 1, 0),
    (0, -1, 0),
    (0, 0, 1),
    (0, 0, -1),
    (1, 1, 0),
    (-1, -1, 0),
    (1, -1, 0),
    (-1, 1, 0),
    (1, 0, 1),
    (-1, 0, -1),
    (1, 0, -1),
    (-1, 0, 1),
    (0, 1, 1),
    (0, -1, -1),
    (0, 1, -1),
    (0, -1, 1),
]
lattice_weights = [1.0 / 3.0] + [1.0 / 18.0] * 6 + [1.0 / 36.0] * 12
opposite_of = [0, 2, 1, 4, 3, 6, 5, 8, 7, 10, 9, 12, 11, 14, 13, 16, 15, 18, 17]
relax_rate = 1.25
forward_x = [1, 7, 9, 11, 13]
backward_x = [2, 8, 10, 12, 14]
upward_y = [3, 15, 17, 7, 10]
downward_y = [4, 16, 18, 9, 8]
mark_rows = 8
kernel_memory = 16 << 20
BF = jnp.bfloat16
F32 = jnp.float32
PICK = jnp.float8_e4m3fn


def iota(shape, dim, dtype=F32):
    value = lax.broadcasted_iota(jnp.int32, shape, dim)
    return value if dtype == jnp.int32 else value.astype(F32).astype(dtype)


def dot_nt(a, b):
    return lax.dot_general(a, b, (((1,), (1,)), ((), ())), preferred_element_type=F32)


def dot_nn(a, b):
    return jnp.dot(a, b, preferred_element_type=F32)


def moments_of(pops):
    density = pops[0]
    moment = [None, None, None]
    for number in range(19):
        if number:
            density = density + pops[number]
        for axis in range(3):
            step = lattice_dirs[number][axis]
            if step == 0:
                continue
            if moment[axis] is None:
                moment[axis] = pops[number] if step == 1 else -pops[number]
            elif step == 1:
                moment[axis] = moment[axis] + pops[number]
            else:
                moment[axis] = moment[axis] - pops[number]
    return density, moment


def one_hot_rows(row, count):
    tile = (32, row.shape[1])
    tall = jnp.broadcast_to(row, tile).astype(BF)
    one, zero = jnp.ones(tile, F32).astype(PICK), jnp.zeros(tile, F32).astype(PICK)
    parts = []
    for start in range(0, count, 32):
        number = (iota(tile, 0) + float(start)).astype(BF)
        parts.append(jnp.where(number == tall, one, zero))
    return jnp.concatenate(parts, axis=0)


def fold_rows(blocks):
    row = iota(blocks[0].shape, 0, jnp.int32)
    half = 4
    while half:
        merged = []
        for s in range(half):
            a, b = blocks[s], blocks[s + half]
            merged.append(
                jnp.where(
                    (row & half) == 0,
                    a + pltpu.roll(a, 8 - half, 0),
                    b + pltpu.roll(b, half, 0),
                )
            )
        blocks = merged
        half //= 2
    return blocks[0]


def pair_weights(list_ref, gap_ref):
    pairs, slots = list_ref.shape
    row = iota((slots, slots), 0, jnp.int32)
    inverse = 1.0 / gap_ref[...]
    weight = jnp.zeros((slots, slots), F32)
    for k in range(pairs):
        weight = weight + jnp.where(row == list_ref[k : k + 1, :], inverse[k : k + 1], 0.0)
    high = weight.astype(BF)
    return high, (weight - high.astype(F32)).astype(BF)


def sample_kernel(slab_count, packed, *refs):
    left_ref, sources, refs = refs[0], refs[1:7], refs[7:]
    slip_ref, refs = refs[0], refs[1:]
    if not packed:
        spot_ref, refs = refs[0], refs[1:]
    send_ref, sorted_ref, z_ref, y_ref = refs[:4]
    targets, (sems,) = refs[4:10], refs[10:]
    copies = [
        pltpu.make_async_copy(source, target, sems.at[number])
        for number, (source, target) in enumerate(zip(sources, targets))
    ]
    for copy in copies:
        copy.start()
    table_ref, marker_count_ref, id_ref, velocity_ref, cell_ref, pops_ref = targets
    slots, width = cell_ref.shape
    rows, depth = pops_ref.shape[1:]
    capacity = slots // slab_count
    for copy in copies[:4]:
        copy.wait()

    alive = left_ref[...] > 0
    identity = id_ref[...]
    block = identity // slots
    spot = (identity % slots).astype(F32)

    def look_up(b, owner):
        return jnp.where(block == b, table_ref[b], owner)

    owner = lax.fori_loop(
        0, slab_count, look_up, jnp.zeros((1, slots), jnp.int32), unroll=slab_count <= 16
    )
    owner = jnp.where(alive, owner, -1)
    owner_f = owner.astype(F32)
    chosen = jnp.where(iota((slab_count, slots), 0) == owner_f, 1.0, 0.0)
    before = jnp.where(
        iota((slots, slots), 0) < iota((slots, slots), 1), 1.0, 0.0
    ).astype(BF)
    earlier = dot_nn(chosen.astype(BF), before)
    position = jnp.sum(chosen * earlier, axis=0, keepdims=True)
    send_row = jnp.where(alive, owner_f * float(capacity) + position, -1.0)
    place = jnp.where(iota((slots, slots), 0) == send_row, 1.0, 0.0).astype(BF)

    where_to = jnp.where(iota((width, slots), 0) == position, 1.0, 0.0).astype(BF)
    if packed:
        taken = (iota((slab_count * mark_rows, slots), 0, jnp.int32) // mark_rows).astype(
            F32
        ) == owner_f
        marks = dot_nt(jnp.where(taken, spot + 1.0, 0.0).astype(BF), where_to)
        slip_ref[:, 3 * capacity :, :] = marks.reshape(slab_count, mark_rows, width).astype(BF)
    else:
        spot_ref[...] = dot_nt((chosen * (spot + 1.0)).astype(BF), where_to).astype(BF)

    count = jnp.where(alive, marker_count_ref[...], 0).astype(F32)
    stack = jnp.concatenate(
        [velocity_ref[c] for c in range(3)] + [count, send_row, jnp.zeros((3, slots), F32)], axis=0
    )
    own = jnp.transpose(stack)
    send_ref[...] = own
    sorted_ref[...] = dot_nn(place, own.astype(BF))

    for copy in copies[4:]:
        copy.wait()
    cells = cell_ref[...]
    z_all, y_all = (cells % depth).astype(F32), (cells // depth).astype(F32)
    moved = dot_nn(place, jnp.concatenate([z_all, y_all], axis=1).astype(BF))
    z_ref[...] = moved[:, :width]
    y_ref[...] = moved[:, width:]

    density, moment = moments_of([pops_ref[number] for number in range(19)])
    flow = jnp.concatenate([part / density for part in moment], axis=0)
    high = flow.astype(BF)
    low = (flow - high.astype(F32)).astype(BF)
    flow_pair = jnp.concatenate([high, low], axis=1)

    slips = []
    for base in range(0, slots, 16):
        found_rows = []
        for eight in range(base, base + 16, 8):
            z_rows = z_all[eight : eight + 8]
            y_rows = y_all[eight : eight + 8]
            parts = [[], [], []]
            for first in range(0, 8, 2):
                picks = jnp.concatenate(
                    [one_hot_rows(z_rows[s : s + 1], depth) for s in (first, first + 1)], axis=1
                )
                picked = dot_nn(flow_pair, jnp.concatenate([picks, picks], axis=0))
                for s in (first, first + 1):
                    cut = slice((s - first) * width, (s - first + 1) * width)
                    tall = jnp.broadcast_to(y_rows[s : s + 1], (8, width))
                    found = [jnp.zeros((8, width), F32)] * 3
                    for start in range(0, rows, 8):
                        mask = iota((8, width), 0) + float(start) == tall
                        for c in range(3):
                            at = c * rows + start
                            found[c] = jnp.where(mask, picked[at : at + 8, cut], found[c])
                    for c in range(3):
                        parts[c].append(found[c])
            found_rows.append([fold_rows(parts[c]) for c in range(3)])
        live = iota((16, width), 1) < own[base : base + 16, 3:4]
        row = []
        for c in range(3):
            sampled = jnp.concatenate([found_rows[0][c], found_rows[1][c]], axis=0)
            slip = jnp.where(live, own[base : base + 16, c : c + 1] - sampled, 0.0)
            row.append(slip.astype(BF))
        slips.append(jnp.concatenate(row, axis=1))
    sent = dot_nn(place, jnp.concatenate(slips, axis=0)).astype(BF)
    for c in range(3):
        cut = sent[:, c * width : (c + 1) * width]
        if packed:
            slip_ref[:, c * capacity : (c + 1) * capacity, :] = cut.reshape(
                slab_count, capacity, width
            )
        else:
            slip_ref[c] = cut


def owner_kernel(
    slab_count,
    packed,
    *refs,
):
    if packed:
        got_ref, list_ref, gap_ref, self_ref, pair_ref, out_ref = refs
        width = got_ref.shape[2]
        slots = list_ref.shape[1]
        capacity = slots // slab_count
        got = jnp.concatenate(
            [
                got_ref[:, c * capacity : (c + 1) * capacity, :].reshape(slots, width)
                for c in range(3)
            ],
            axis=1,
        )
        per_tile = width // capacity
        lane = iota((8, width), 1, jnp.int32)
        tiles = []
        for start in range(0, slab_count, per_tile):
            total = jnp.zeros((8, width), F32)
            for source in range(start, min(start + per_tile, slab_count)):
                mark = got_ref[source, 3 * capacity : 3 * capacity + mark_rows, :].astype(F32)
                off = (source - start) * capacity
                if off:
                    mark = pltpu.roll(mark, off, 1)
                mine = (lane >= off) & (lane < off + capacity)
                total = jnp.where(mine, mark, total)
            tiles.append(total)
        spots = jnp.concatenate(tiles, axis=1) - 1.0
    else:
        got_ref, spot_ref, list_ref, gap_ref, self_ref, pair_ref, out_ref = refs
        width = got_ref.shape[2]
        slots = list_ref.shape[1]
        got = jnp.concatenate([got_ref[c] for c in range(3)], axis=1)
        spots = jnp.broadcast_to(spot_ref[...].astype(F32), (8, slots)) - 1.0

    spot_row = spots[:1]
    spot_col = jnp.transpose(spots)[:, :1]
    land = jnp.where(iota((slots, slots), 0) == spot_row, 1.0, 0.0).astype(BF)
    reply = jnp.where(iota((slots, slots), 1) == spot_col, 1.0, 0.0).astype(BF)
    chosen = [dot_nt(reply, part).astype(BF) for part in pair_weights(list_ref, gap_ref)]
    owned = dot_nn(land, got).astype(BF)
    near = (dot_nn(chosen[0], owned) + dot_nn(chosen[1], owned)).astype(BF)
    coupling = jnp.concatenate([self_ref[...], pair_ref[...]], axis=0)
    for c in range(3):
        span = slice(c * width, (c + 1) * width)
        both = jnp.concatenate([got[:, span], near[:, span]], axis=1)
        cut = dot_nn(both, coupling).astype(BF)
        if packed:
            out_ref[:, c * capacity : (c + 1) * capacity, :] = cut.reshape(
                slab_count, capacity, width
            )
        else:
            out_ref[c] = cut


def returned_rows(slab_count, packed, back_ref, sorted_ref, base, count):
    if packed:
        capacity = sorted_ref.shape[0] // slab_count
        at, block = base % capacity, slice(base // capacity, (base + count - 1) // capacity + 1)
        take = min(count, capacity)
        parts = [
            back_ref[block, c * capacity + at : c * capacity + at + take, :].reshape(count, -1)
            for c in range(3)
        ]
    else:
        parts = [back_ref[c, base : base + count, :] for c in range(3)]
    live = iota(parts[0].shape, 1) < sorted_ref[base : base + count, 3:4]
    return [jnp.where(live, part.astype(F32), 0.0) for part in parts]


def finish_kernel(slab_count, packed, back_ref, sorted_ref, send_ref, out_ref):
    slots = sorted_ref.shape[0]
    masked = returned_rows(slab_count, packed, back_ref, sorted_ref, 0, slots)
    fetch = jnp.where(iota((slots, slots), 1) == send_ref[:, 4:5], 1.0, 0.0).astype(BF)
    for c in range(3):
        out_ref[c] = dot_nn(fetch, masked[c].astype(BF)).astype(BF)


def spread_kernel(
    slab_count,
    packed,
    back_ref,
    sorted_ref,
    z_ref,
    y_ref,
    pops_ref,
    collided_ref,
    up_ref,
    down_ref,
    first_ref,
    second_ref,
):
    slots, width = z_ref.shape
    rows, depth = pops_ref.shape[1:]
    picks, terms = [], []
    for base in range(0, slots, 16):
        f_rows = returned_rows(slab_count, packed, back_ref, sorted_ref, base, 16)
        z_rows = z_ref[base : base + 16, :]
        y_rows = y_ref[base : base + 16, :]
        for s in range(16):
            picks.append(one_hot_rows(z_rows[s : s + 1], depth))
            tall = jnp.broadcast_to(y_rows[s : s + 1], (16, width)).astype(BF)
            parts = []
            for c in range(3):
                value = jnp.broadcast_to(f_rows[c][s : s + 1], (16, width)).astype(BF)
                for start in range(0, rows, 16):
                    number = (iota((16, width), 0) + float(start)).astype(BF)
                    parts.append(jnp.where(number == tall, value, jnp.zeros((), BF)))
            terms.append(jnp.concatenate(parts, axis=0))
    total = dot_nt(jnp.concatenate(terms, axis=1), jnp.concatenate(picks, axis=1))

    force = [total[c * rows : (c + 1) * rows] for c in range(3)]
    pops = [pops_ref[number] for number in range(19)]
    density, moment = moments_of(pops)
    velocity = [(moment[c] + 0.5 * force[c]) / density for c in range(3)]
    speed_sq = velocity[0] * velocity[0] + velocity[1] * velocity[1] + velocity[2] * velocity[2]
    work_rate = velocity[0] * force[0] + velocity[1] * force[1] + velocity[2] * force[2]
    base_term = 1.0 - 1.5 * speed_sq
    even = (lax.axis_index("slab") & 1) == 0
    sent = {}
    for number in range(19):
        step = lattice_dirs[number]
        along, push = None, None
        for c in range(3):
            if step[c] == 0:
                continue
            v, f = (velocity[c], force[c]) if step[c] == 1 else (-velocity[c], -force[c])
            along = v if along is None else along + v
            push = f if push is None else push + f
        weight = lattice_weights[number]
        if along is None:
            equilibrium = weight * density * base_term
            source = ((1.0 - 0.5 * relax_rate) * weight * -3.0) * work_rate
        else:
            equilibrium = weight * density * (base_term + 3.0 * along + 4.5 * along * along)
            source = ((1.0 - 0.5 * relax_rate) * weight) * (
                3.0 * (push - work_rate) + 9.0 * along * push
            )
        value = pops[number] - relax_rate * (pops[number] - equilibrium) + source
        collided_ref[number] = value
        if step[0] != 0:
            sent.setdefault((forward_x if step[0] == 1 else backward_x).index(number), {})[
                step[0]
            ] = value
        if number in upward_y[:3]:
            at = upward_y.index(number)
            up_ref[at : at + 1, :] = value[rows - 1 :]
        if number in downward_y[:3]:
            at = downward_y.index(number)
            down_ref[at : at + 1, :] = value[:1]
    for at, pair in sent.items():
        first_ref[at] = jnp.where(even, pair[1], pair[-1]).astype(BF)
        second_ref[at] = jnp.where(even, pair[-1], pair[1]).astype(BF)
    up_ref[3:, :] = jnp.zeros((5, depth), F32)
    down_ref[3:, :] = jnp.zeros((5, depth), F32)


def stream_kernel(
    sub_total, collided_ref, one_ref, two_ref, first_ref, second_ref, read_ref
):
    rows, depth = collided_ref.shape[1:]
    row = iota((rows, depth), 0, jnp.int32)
    place = lax.axis_index("sub")
    slab_even = (lax.axis_index("slab") & 1) == 0
    sub_even = (place & 1) == 0
    low = jnp.where(sub_even, two_ref[...], one_ref[...])
    high = jnp.where(sub_even, one_ref[...], two_ref[...])
    low_wall = jnp.where(place == 0, 1, 0)
    high_wall = jnp.where(place == sub_total - 1, 1, 0)
    for number in range(19):
        step_x, step_y, step_z = lattice_dirs[number]
        if step_x == 1:
            at = forward_x.index(number)
            moved = jnp.where(slab_even, second_ref[at].astype(F32), first_ref[at].astype(F32))
        elif step_x == -1:
            at = backward_x.index(number)
            moved = jnp.where(slab_even, first_ref[at].astype(F32), second_ref[at].astype(F32))
        else:
            moved = collided_ref[number]
        if step_y != 0:
            rolled = pltpu.roll(moved, 1 if step_y == 1 else rows - 1, 0)
            edge_row = 0 if step_y == 1 else rows - 1
            at = (upward_y if step_y == 1 else downward_y).index(number)
            edge = (low if step_y == 1 else high)[at : at + 1]
            moved = jnp.where(row == edge_row, edge, rolled)
        if step_z != 0:
            moved = pltpu.roll(moved, 1 if step_z == 1 else depth - 1, 1)
        if step_y != 0:
            wall = low_wall if step_y == 1 else high_wall
            at_wall = (row == edge_row) & (wall == 1)
            moved = jnp.where(at_wall, collided_ref[opposite_of[number]], moved)
        read_ref[number] = moved


def whole(memory=pltpu.VMEM):
    return pl.BlockSpec(memory_space=memory)


def swap(value, axis, odd):
    count = lax.axis_size(axis)
    pairs = [(i, (i + 1 if i % 2 == odd else i - 1) % count) for i in range(count)]
    return lax.ppermute(value, axis, pairs)


def per_device(
    populations,
    marker_cell,
    marker_count,
    particle_count,
    particle_id,
    owner_table,
    particle_velocity,
    pair_list,
    pair_gap,
    self_coupling,
    pair_coupling,
):
    slab_count = lax.axis_size("slab")
    slots, width = marker_cell.shape[2:]
    planes, rows, depth = populations.shape[1:]
    assert planes == 1 and slots <= 256 and slots % slab_count == 0
    assert slab_count % 2 == 0 and lax.axis_size("sub") % 2 == 0
    capacity = slots // slab_count
    assert capacity <= width
    packed = capacity % 16 == 0 and width % capacity == 0
    pops = populations.reshape(19, rows, depth)
    cells = marker_cell.reshape(slots, width)
    shape = jax.ShapeDtypeStruct
    limits = pltpu.CompilerParams(vmem_limit_bytes=kernel_memory)

    if packed:
        sample_out = [shape((slab_count, 3 * capacity + mark_rows, width), BF)]
    else:
        sample_out = [shape((3, slots, width), BF), shape((slab_count, width), BF)]
    sample_out += [shape((slots, 8), F32)] * 2 + [shape((slots, width), F32)] * 2
    results = pl.pallas_call(
        functools.partial(sample_kernel, slab_count, packed),
        out_shape=sample_out,
        in_specs=[whole()] + [whole(pltpu.HBM)] * 6,
        out_specs=[whole()] * len(sample_out),
        scratch_shapes=[
            pltpu.SMEM((slab_count,), jnp.int32),
            pltpu.VMEM((1, slots), jnp.int32),
            pltpu.VMEM((1, slots), jnp.int32),
            pltpu.VMEM((3, 1, slots), F32),
            pltpu.VMEM((slots, width), jnp.int32),
            pltpu.VMEM((19, rows, depth), F32),
            pltpu.SemaphoreType.DMA((6,)),
        ],
        compiler_params=limits,
        name="sample",
    )(
        particle_count - lax.broadcasted_iota(jnp.int32, (1, slots), 1),
        *[
            pltpu.with_memory_space_constraint(value, pltpu.HBM)
            for value in (
                owner_table.reshape(slab_count),
                marker_count.reshape(1, slots),
                particle_id.reshape(1, slots),
                particle_velocity.reshape(3, 1, slots),
                cells,
                pops,
            )
        ],
    )
    send, ordered, z_cells, y_cells = results[-4:]

    def exchange(value):
        return lax.all_to_all(value, "slab", split_axis=0, concat_axis=0, tiled=True)

    def by_owner(value):
        value = value.reshape(3, slab_count, capacity, width)
        return jnp.transpose(value, (1, 0, 2, 3)).reshape(slab_count, 3 * capacity, width)

    def by_component(value):
        value = value.reshape(slab_count, 3, capacity, width)
        return jnp.transpose(value, (1, 0, 2, 3)).reshape(3, slots, width)

    if packed:
        arrived = [exchange(results[0])]
        reply_shape = shape((slab_count, 3 * capacity, width), BF)
    else:
        slip = jnp.concatenate([by_owner(results[0]), results[1][:, None, :]], axis=1)
        got = exchange(slip)
        arrived = [
            by_component(got[:, : 3 * capacity]),
            got[:, 3 * capacity, :capacity].reshape(1, slots),
        ]
        reply_shape = shape((3, slots, width), BF)
    reply = pl.pallas_call(
        functools.partial(owner_kernel, slab_count, packed),
        out_shape=reply_shape,
        in_specs=[whole()] * (len(arrived) + 4),
        out_specs=whole(),
        compiler_params=limits,
        name="owner",
    )(
        *arrived,
        jnp.transpose(pair_list.reshape(slots, -1)),
        jnp.transpose(pair_gap.reshape(slots, -1)),
        self_coupling,
        pair_coupling,
    )
    back = exchange(reply) if packed else by_component(exchange(by_owner(reply)))

    collided, up, down, first, second = pl.pallas_call(
        functools.partial(spread_kernel, slab_count, packed),
        out_shape=[
            shape((19, rows, depth), F32),
            shape((8, depth), F32),
            shape((8, depth), F32),
            shape((5, rows, depth), BF),
            shape((5, rows, depth), BF),
        ],
        in_specs=[whole()] * 5,
        out_specs=[whole()] * 5,
        compiler_params=limits,
        name="spread",
    )(back, ordered, z_cells, y_cells, pops)
    marker_force = pl.pallas_call(
        functools.partial(finish_kernel, slab_count, packed),
        out_shape=shape((3, slots, width), BF),
        in_specs=[whole()] * 3,
        out_specs=whole(),
        compiler_params=limits,
        cost_estimate=pl.CostEstimate(flops=50_000_000, bytes_accessed=400_000, transcendentals=0),
        name="finish",
    )(back, ordered, send)

    slab_even = (lax.axis_index("slab") & 1) == 0
    sub_even = (lax.axis_index("sub") & 1) == 0
    first, second = swap(first, "slab", 0), swap(second, "slab", 1)
    top, bottom = slice(rows - 1, rows), slice(0, 1)
    one_up = jnp.where(slab_even, second[1, top], first[1, top])
    two_up = jnp.where(slab_even, first[2, top], second[2, top])
    one_down = jnp.where(slab_even, second[2, bottom], first[2, bottom])
    two_down = jnp.where(slab_even, first[1, bottom], second[1, bottom])
    up = jnp.concatenate([up[:3], one_up.astype(F32), two_up.astype(F32)])
    down = jnp.concatenate([down[:3], one_down.astype(F32), two_down.astype(F32)])
    up, down, marker_force = lax.optimization_barrier((up, down, marker_force))
    low_high = (
        swap(jnp.where(sub_even, up, down), "sub", 0),
        swap(jnp.where(sub_even, down, up), "sub", 1),
    )
    read = pl.pallas_call(
        functools.partial(stream_kernel, lax.axis_size("sub")),
        out_shape=shape((19, rows, depth), F32),
        in_specs=[whole()] * 5,
        out_specs=whole(),
        compiler_params=limits,
        name="stream",
    )(collided, *low_high, first, second)
    marker_force = jnp.transpose(marker_force, (1, 0, 2))[None, None]
    return (read.reshape(19, 1, rows, depth), marker_force)


def solution(mesh):
    placed = (
        P(None, "slab", "sub", None),
        P("slab", "sub", None, None),
        P("slab", "sub", None),
        P("slab", "sub"),
        P("slab", "sub", None),
        P("sub", None),
        P("slab", "sub", None, None),
        P("slab", "sub", None, None),
        P("slab", "sub", None, None),
        P(),
        P(),
    )
    return jax.shard_map(
        per_device,
        mesh=mesh,
        in_specs=placed,
        out_specs=(P(None, "slab", "sub", None), P("slab", "sub", None, None, None)),
        check_vma=False,
    )
```
